256 devices in a mesh: dp: 32 (over z, y), ep: 8 (over x, core).
Axes of the slice: x: 4, y: 4, z: 8, core: 2. Of those that a mesh axis runs over, the one named last changes fastest.
Arguments:
- hidden: bfloat16 [8192, 2048], P(('dp', 'ep'))
- grad_out: bfloat16 [8192, 2048], P(('dp', 'ep'))
- expert_ids: int32 [8192, 2], P(('dp', 'ep'))
- norm_gain: float32 [2048], replicated
- w_router: float32 [2048, 8], replicated
- w_gate: bfloat16 [8, 2048, 5632], P('ep')
- w_up: bfloat16 [8, 2048, 5632], P('ep')
- w_down: bfloat16 [8, 5632, 2048], P('ep')
Outputs:
- output 1: bfloat16 [8192, 2048], P(('dp', 'ep'))
- output 2: float32 [], replicated
- output 3: bfloat16 [8192, 2048], P(('dp', 'ep'))
- output 4: float32 [2048], replicated
- output 5: float32 [2048, 8], replicated
- output 6: bfloat16 [8, 2048, 5632], P('ep')
- output 7: bfloat16 [8, 2048, 5632], P('ep')
- output 8: bfloat16 [8, 5632, 2048], P('ep')
All inputs are finite; a program needn't handle non-finite values.
Results may differ from the reference program's by a relative error of at most 0.0155116.
Values are sent between devices in bfloat16 or wider.
A program may use at most 768 MiB of HBM per device.

```python
import functools
import jax
import jax.numpy as jnp
from jax import lax

D = 2048
FF = 5632
EXPERTS = 8
TOK = 32
DEVICES = 256
CAP = 4 * TOK // EXPERTS
ROWS_EXP = DEVICES * CAP
S_ALL = TOK * DEVICES
EPS = 1e-6
AUX_COEF = 0.001


def draw_routes(key):
    key_order, key_shift, key_perm, key_swap = jax.random.split(key, 4)
    half_exp = EXPERTS // 2
    mean_load = 2 * TOK // EXPERTS
    shift = jax.random.randint(key_shift, (DEVICES, half_exp), 0, mean_load + 1)
    shift = shift.at[:, 0].set(mean_load)
    order = jax.vmap(lambda sub_key: jax.random.permutation(sub_key, EXPERTS))(jax.random.split(key_order, DEVICES))
    signed = jnp.concatenate([shift, -shift], axis=1)
    expert_range = jnp.arange(EXPERTS, dtype=jnp.int32)
    loads = mean_load + jnp.sum(signed[:, :, None] * (order[:, :, None] == expert_range).astype(jnp.int32), axis=1)
    bounds = jnp.cumsum(loads, axis=1)
    positions = jnp.arange(2 * TOK, dtype=jnp.int32)
    listed = jax.vmap(lambda bound_row: jnp.searchsorted(bound_row, positions, side="right"))(bounds).astype(jnp.int32)
    token_order = jax.vmap(lambda sub_key: jax.random.permutation(sub_key, TOK))(jax.random.split(key_perm, DEVICES))
    first = jnp.take_along_axis(listed[:, :TOK], token_order, axis=1)
    second = jnp.take_along_axis(listed[:, TOK:], token_order, axis=1)
    swap = jax.random.randint(key_swap, (DEVICES, TOK), 0, 2) == 1
    id_first = jnp.where(swap, second, first)
    id_second = jnp.where(swap, first, second)
    return jnp.stack([id_first, id_second], axis=-1).reshape(DEVICES * TOK, 2).astype(jnp.int32)


def setup_inputs(seed: int = 0) -> dict:
    key = jax.random.key(seed)
    keys = jax.random.split(key, 8)
    expert_ids = draw_routes(keys[0])
    w_router = jax.random.normal(keys[1], (D, EXPERTS), jnp.float32) * D ** -0.5
    col_dir = w_router * lax.rsqrt(jnp.mean(w_router * w_router, axis=0, keepdims=True))
    chosen = jnp.sum((expert_ids[:, :, None] == jnp.arange(EXPERTS, dtype=jnp.int32)).astype(jnp.float32), axis=1)
    boost = jnp.dot(chosen, col_dir.T, preferred_element_type=jnp.float32)
    hidden = jax.random.normal(keys[2], (S_ALL, D), jnp.float32) + (2.5 * D ** -0.5) * boost
    grad_out = jax.random.normal(keys[3], (S_ALL, D), jnp.float32)
    norm_gain = 1.0 + 0.3 * jax.random.normal(keys[4], (D,), jnp.float32)
    w_gate = jax.random.normal(keys[5], (EXPERTS, D, FF), jnp.float32) * D ** -0.5
    w_up = jax.random.normal(keys[6], (EXPERTS, D, FF), jnp.float32) * D ** -0.5
    w_down = jax.random.normal(keys[7], (EXPERTS, FF, D), jnp.float32) * (2.0 * FF ** -0.5)
    return {"hidden": hidden.astype(jnp.bfloat16), "grad_out": grad_out.astype(jnp.bfloat16), "expert_ids": expert_ids, "norm_gain": norm_gain, "w_router": w_router, "w_gate": w_gate.astype(jnp.bfloat16), "w_up": w_up.astype(jnp.bfloat16), "w_down": w_down.astype(jnp.bfloat16)}


def bf16_trip(value):
    return value.astype(jnp.bfloat16).astype(jnp.float32)


def route_tables(expert_ids, n_exp, capacity):
    flat_ids = expert_ids.reshape(-1)
    n_choice = flat_ids.shape[0]
    one_hot = (flat_ids[:, None] == jnp.arange(n_exp, dtype=jnp.int32)[None, :]).astype(jnp.int32)
    running = jnp.cumsum(one_hot, axis=0) - 1
    dest_rows = flat_ids * capacity + jnp.sum(running * one_hot, axis=1)
    slot_owner = jnp.full((n_exp * capacity,), n_choice, jnp.int32).at[dest_rows].set(jnp.arange(n_choice, dtype=jnp.int32))
    return dest_rows, slot_owner, jnp.sum(one_hot, axis=0)


def expert_ffn(operands):
    rows, gate_w, up_w, down_w = operands
    h_gate = bf16_trip(jnp.dot(rows, gate_w.astype(jnp.float32), preferred_element_type=jnp.float32))
    h_up = bf16_trip(jnp.dot(rows, up_w.astype(jnp.float32), preferred_element_type=jnp.float32))
    act_rows = bf16_trip(jax.nn.silu(h_gate) * h_up)
    return bf16_trip(jnp.dot(act_rows, down_w.astype(jnp.float32), preferred_element_type=jnp.float32))


def forward_pass(hidden, norm_gain, w_router, w_gate, w_up, w_down, expert_ids):
    dest_rows, slot_owner, loads = route_tables(expert_ids, EXPERTS, ROWS_EXP)
    choice_hot = (expert_ids[:, :, None] == jnp.arange(EXPERTS, dtype=jnp.int32)).astype(jnp.float32)
    x_f32 = hidden.astype(jnp.float32)
    inv_rms = lax.rsqrt(jnp.mean(x_f32 * x_f32, axis=-1, keepdims=True) + EPS)
    x_norm = bf16_trip(x_f32 * inv_rms * norm_gain)
    logits = jnp.dot(x_norm, w_router, preferred_element_type=jnp.float32)
    router_probs = jax.nn.softmax(logits, axis=-1)
    gate_vals = jnp.sum(router_probs[:, None, :] * choice_hot, axis=-1)
    rows = bf16_trip(jnp.take(x_norm, slot_owner // 2, axis=0, mode="fill", fill_value=0))
    exp_out = lax.map(jax.checkpoint(expert_ffn), (rows.reshape(EXPERTS, ROWS_EXP, D), w_gate, w_up, w_down))
    picked = jnp.take(exp_out.reshape(EXPERTS * ROWS_EXP, D), dest_rows, axis=0).reshape(S_ALL, 2, D)
    out_hidden = (x_f32 + jnp.sum(gate_vals[:, :, None] * picked, axis=1)).astype(jnp.bfloat16)
    load_frac = loads.astype(jnp.float32) / (2 * S_ALL)
    aux_loss = AUX_COEF * EXPERTS * jnp.sum(load_frac * jnp.mean(router_probs, axis=0))
    return out_hidden, aux_loss


def reference(hidden, grad_out, expert_ids, norm_gain, w_router, w_gate, w_up, w_down):
    forward_fn = functools.partial(forward_pass, expert_ids=expert_ids)
    (out_hidden, aux_loss), pullback = jax.vjp(forward_fn, hidden, norm_gain, w_router, w_gate, w_up, w_down)
    all_grads = pullback((grad_out, jnp.ones_like(aux_loss)))
    return (out_hidden, aux_loss, all_grads[0], all_grads[1], all_grads[2], all_grads[3], all_grads[4], all_grads[5])
```

```python
import functools
import jax
import jax.numpy as jnp
from jax import lax
from jax.experimental import pallas as pl
from jax.experimental.pallas import tpu as pltpu
from jax.sharding import PartitionSpec as P

EPS = 1e-6
AUX_COEF = 0.001
LANES = 128
GROUP = 256
ALIGN = 16
CAP_SMALL = 256
F32 = jnp.float32
BF16 = jnp.bfloat16


def route_tables(expert_ids, n_exp, capacity):
    flat_ids = expert_ids.reshape(-1)
    n_choice = flat_ids.shape[0]
    one_hot = (flat_ids[:, None] == jnp.arange(n_exp, dtype=jnp.int32)[None, :]).astype(jnp.int32)
    running = jnp.cumsum(one_hot, axis=0) - 1
    dest_rows = flat_ids * capacity + jnp.sum(running * one_hot, axis=1)
    slot_owner = jnp.full((n_exp * capacity,), n_choice, jnp.int32).at[dest_rows].set(jnp.arange(n_choice, dtype=jnp.int32))
    return dest_rows, slot_owner, jnp.sum(one_hot, axis=0)


def peers(n_y, n_z, n_ep):
    dp, ep = lax.axis_index("dp"), lax.axis_index("ep")
    y, z = lax.rem(dp, n_y), lax.div(dp, n_y)
    along_ep = [{"dp": dp, "ep": lax.rem(ep + k, n_ep)} for k in range(1, n_ep)]
    along_y = [{"dp": z * n_y + lax.rem(y + k, n_y), "ep": ep} for k in range(1, n_y)]
    along_z = [{"dp": lax.rem(z + k, n_z) * n_y + y, "ep": ep} for k in range(1, n_z)]
    return dp, ep, y, z, along_ep, along_y, along_z


def enter(all_peers):
    barrier = pltpu.get_barrier_semaphore()
    for peer in all_peers:
        pl.semaphore_signal(barrier, inc=1, device_id=peer, device_id_type=pl.DeviceIdType.MESH)
    pl.semaphore_wait(barrier, len(all_peers))


def exchange(targets, make):
    copies = [make(k, target) for k, target in enumerate(targets)]
    for copy in copies:
        copy.start()
    for copy in copies:
        copy.wait()


def remote(src, dst, send_sem, recv_sem, target):
    return pltpu.make_async_remote_copy(src_ref=src, dst_ref=dst, send_sem=send_sem, recv_sem=recv_sem, device_id=target, device_id_type=pl.DeviceIdType.MESH)


def gather_kernel(n_y, n_z, n_ep, row_ref, out_ref, send_sem, recv_sem):
    dp, ep, y, z, along_ep, along_y, along_z = peers(n_y, n_z, n_ep)
    enter(along_ep + along_y + along_z)
    mine = out_ref.at[pl.ds(dp * n_ep + ep, 1)]
    local = pltpu.make_async_copy(row_ref, mine, send_sem.at[0])
    local.start()
    local.wait()
    base = 0
    exchange(along_ep, lambda k, t: remote(row_ref, mine, send_sem.at[base + k], recv_sem.at[base + k], t))
    base = len(along_ep)
    rows_y = out_ref.at[pl.ds(dp * n_ep, n_ep)]
    exchange(along_y, lambda k, t: remote(rows_y, rows_y, send_sem.at[base + k], recv_sem.at[base + k], t))
    base += len(along_y)
    rows_z = out_ref.at[pl.ds(z * n_y * n_ep, n_y * n_ep)]
    exchange(along_z, lambda k, t: remote(rows_z, rows_z, send_sem.at[base + k], recv_sem.at[base + k], t))


def gather_rows(row, n_y, n_z, n_ep):
    n_dev = n_y * n_z * n_ep
    n_sem = n_ep + n_y + n_z - 3
    return pl.pallas_call(
        functools.partial(gather_kernel, n_y, n_z, n_ep),
        out_shape=jax.ShapeDtypeStruct((n_dev, 1, LANES), F32),
        in_specs=[pl.BlockSpec(memory_space=pltpu.VMEM)],
        out_specs=pl.BlockSpec(memory_space=pltpu.VMEM),
        scratch_shapes=[pltpu.SemaphoreType.DMA((n_sem,)), pltpu.SemaphoreType.DMA((n_sem,))],
        compiler_params=pltpu.CompilerParams(collective_id=1, has_side_effects=True),
        name="gather_rows",
    )(row)


def reduce_kernel(n_y, n_z, n_ep, in_ref, out_ref, got_ep, got_y, got_z, send_sem, recv_sem):
    dp, ep, y, z, along_ep, along_y, along_z = peers(n_y, n_z, n_ep)
    enter(along_ep + along_y + along_z)
    base = 0
    got_ep[ep] = in_ref[ep]
    exchange(along_ep, lambda k, t: remote(in_ref.at[t["ep"]], got_ep.at[ep], send_sem.at[base + k], recv_sem.at[base + k], t))
    total = got_ep[0]
    for k in range(1, n_ep):
        total = total + got_ep[k]
    got_y[y] = total
    base = len(along_ep)
    exchange(along_y, lambda k, t: remote(got_y.at[y], got_y.at[y], send_sem.at[base + k], recv_sem.at[base + k], t))
    total = got_y[0]
    for k in range(1, n_y):
        total = total + got_y[k]
    got_z[z] = total
    base += len(along_y)
    exchange(along_z, lambda k, t: remote(got_z.at[z], got_z.at[z], send_sem.at[base + k], recv_sem.at[base + k], t))
    total = got_z[0]
    for k in range(1, n_z):
        total = total + got_z[k]
    out_ref[ep] = total
    base += len(along_z)
    exchange(along_ep, lambda k, t: remote(out_ref.at[ep], out_ref.at[ep], send_sem.at[base + k], recv_sem.at[base + k], t))


def reduce_rows(parts, n_y, n_z, n_ep):
    n_sem = 2 * n_ep + n_y + n_z - 4
    chunk = parts.shape[1:]
    return pl.pallas_call(
        functools.partial(reduce_kernel, n_y, n_z, n_ep),
        out_shape=jax.ShapeDtypeStruct(parts.shape, F32),
        in_specs=[pl.BlockSpec(memory_space=pltpu.VMEM)],
        out_specs=pl.BlockSpec(memory_space=pltpu.VMEM),
        scratch_shapes=[pltpu.VMEM((n_ep, *chunk), F32), pltpu.VMEM((n_y, *chunk), F32), pltpu.VMEM((n_z, *chunk), F32), pltpu.SemaphoreType.DMA((n_sem,)), pltpu.SemaphoreType.DMA((n_sem,))],
        compiler_params=pltpu.CompilerParams(collective_id=2, has_side_effects=True),
        name="reduce_rows",
    )(parts)


def dot(a, b, dims):
    return lax.dot_general(a, b, (dims, ((), ())), preferred_element_type=F32)


def expert_math(hg, hu, da):
    gate = hg.astype(BF16).astype(F32)
    up = hu.astype(BF16).astype(F32)
    d_act = da.astype(BF16).astype(F32)
    sig = jax.nn.sigmoid(gate)
    silu = gate * sig
    act = (silu * up).astype(BF16)
    d_up = (d_act * silu).astype(BF16)
    d_gate = (d_act * up * sig * (1.0 + gate * (1.0 - sig))).astype(BF16)
    return act, d_gate, d_up


def ffn_kernel(rows_ref, wg_ref, wu_ref, wd_ref, out_ref, o_acc, d_acc):
    step = pl.program_id(0)
    width = wg_ref.shape[0]
    xn, dp = rows_ref[:, :width], rows_ref[:, width:]
    wg, wu, wd = wg_ref[...], wu_ref[...], wd_ref[...]
    act, d_gate, d_up = expert_math(dot(xn, wg, ((1,), (0,))), dot(xn, wu, ((1,), (0,))), dot(dp, wd, ((1,), (1,))))

    @pl.when(step == 0)
    def _():
        o_acc[...] = jnp.zeros_like(o_acc)
        d_acc[...] = jnp.zeros_like(d_acc)

    o_acc[...] += dot(act, wd, ((1,), (0,)))
    d_acc[...] += dot(d_gate, wg, ((1,), (1,))) + dot(d_up, wu, ((1,), (1,)))

    @pl.when(step == pl.num_programs(0) - 1)
    def _():
        out_ref[:, :width] = o_acc[...].astype(BF16)
        out_ref[:, width:] = d_acc[...].astype(BF16)


def local_ffn(rows, wg, wu, wd, block):
    n, width = rows.shape[0], wg.shape[0]
    ff = wg.shape[1]
    whole = pl.BlockSpec((n, 2 * width), lambda j: (0, 0))
    col = pl.BlockSpec((width, block), lambda j: (0, j))
    row = pl.BlockSpec((block, width), lambda j: (j, 0))
    return pl.pallas_call(
        ffn_kernel,
        grid=(ff // block,),
        out_shape=jax.ShapeDtypeStruct((n, 2 * width), BF16),
        in_specs=[whole, col, col, row],
        out_specs=whole,
        scratch_shapes=[pltpu.VMEM((n, width), F32), pltpu.VMEM((n, width), F32)],
        compiler_params=pltpu.CompilerParams(dimension_semantics=("arbitrary",), vmem_limit_bytes=40 * 2**20),
        cost_estimate=pl.CostEstimate(flops=12 * n * width * ff, bytes_accessed=6 * width * ff, transcendentals=0),
        name="local_ffn",
    )(rows, wg, wu, wd)


def pack_kernel(cap, off_ref, first_ref, rows_ref, pos_ref, gate_ref, xn_out, dp_out, xn_buf, dp_buf, sem):
    g = pl.program_id(0)
    width = xn_buf.shape[1]
    tile = xn_buf.shape[0] - cap
    off = off_ref[g] - first_ref[0]
    base = pl.multiple_of(jnp.clip(lax.div(off, ALIGN) * ALIGN, 0, cap), ALIGN)

    @pl.when(g == 0)
    def _():
        xn_buf[...] = jnp.zeros_like(xn_buf)
        dp_buf[...] = jnp.zeros_like(dp_buf)

    row_id = lax.broadcasted_iota(jnp.int32, (tile, GROUP), 0) + base
    hit = row_id == pos_ref[0] - first_ref[0]
    pick = hit.astype(F32).astype(BF16)
    gate = jnp.sum(jnp.where(hit, gate_ref[0], 0.0), axis=1, keepdims=True)
    xn = dot(pick, rows_ref[:, :width], ((1,), (0,))).astype(BF16)
    dp = (dot(pick, rows_ref[:, width:], ((1,), (0,))) * gate).astype(BF16)
    keep = lax.broadcasted_iota(jnp.int32, (ALIGN, width), 0) + base < off
    for buf, new in ((xn_buf, xn), (dp_buf, dp)):
        head = pl.ds(base, ALIGN)
        buf[head, :] = jnp.where(keep, buf[head, :].astype(F32), new[:ALIGN].astype(F32)).astype(BF16)
        buf[pl.ds(pl.multiple_of(base + ALIGN, ALIGN), tile - ALIGN), :] = new[ALIGN:]

    @pl.when(g == pl.num_programs(0) - 1)
    def _():
        copies = [pltpu.make_async_copy(xn_buf.at[pl.ds(0, cap)], xn_out, sem.at[0]), pltpu.make_async_copy(dp_buf.at[pl.ds(0, cap)], dp_out, sem.at[1])]
        for copy in copies:
            copy.start()
        for copy in copies:
            copy.wait()


def pack_rows(rows, offsets, first, pos, gates, cap, most):
    total, width = rows.shape[0], rows.shape[1] // 2
    n_group = total // GROUP
    tile = most + ALIGN
    small = pl.BlockSpec((1, 1, GROUP), lambda g, *_: (g, 0, 0))
    return pl.pallas_call(
        functools.partial(pack_kernel, cap),
        grid_spec=pltpu.PrefetchScalarGridSpec(
            num_scalar_prefetch=2,
            grid=(n_group,),
            in_specs=[pl.BlockSpec((GROUP, 2 * width), lambda g, *_: (g, 0)), small, small],
            out_specs=[pl.BlockSpec(memory_space=pl.ANY), pl.BlockSpec(memory_space=pl.ANY)],
            scratch_shapes=[pltpu.VMEM((cap + tile, width), BF16), pltpu.VMEM((cap + tile, width), BF16), pltpu.SemaphoreType.DMA((2,))],
        ),
        out_shape=[jax.ShapeDtypeStruct((cap, width), BF16)] * 2,
        compiler_params=pltpu.CompilerParams(dimension_semantics=("arbitrary",), vmem_limit_bytes=50 * 2**20),
        cost_estimate=pl.CostEstimate(flops=4 * tile * total * width, bytes_accessed=4 * total * width, transcendentals=0),
        name="pack_rows",
    )(offsets, first, rows, pos, gates)


def solution(mesh):
    n_ep = mesh.shape["ep"]
    n_dp = mesh.shape["dp"]
    n_y = 4 if n_dp == 32 else 2
    n_z = n_dp // n_y
    n_dev = n_dp * n_ep
    all_axes = ("dp", "ep")

    def local_step(hidden, grad_out, expert_ids, norm_gain, w_router, w_gate, w_up, w_down):
        n_tok, width = hidden.shape
        n_exp = w_router.shape[1]
        capacity = 4 * n_tok // n_exp
        total_tok = n_tok * n_dev
        cap = min(2432, total_tok) if n_dp == 32 else CAP_SMALL
        dest_rows, slot_owner, loads = route_tables(expert_ids, n_exp, capacity)
        choice_hot = (expert_ids[:, :, None] == jnp.arange(n_exp, dtype=jnp.int32)).astype(F32)

        x_f32 = hidden.astype(F32)
        inv_rms = lax.rsqrt(jnp.mean(x_f32 * x_f32, axis=-1, keepdims=True) + EPS)
        x_hat = x_f32 * inv_rms
        x_norm = (x_hat * norm_gain).astype(BF16)
        rows_all = lax.all_gather(jnp.concatenate([x_norm, grad_out], axis=1), all_axes, axis=0, tiled=True)
        xn_f32 = x_norm.astype(F32)
        router_probs = jax.nn.softmax(jnp.dot(xn_f32, w_router, preferred_element_type=F32), axis=-1)
        gate_vals = jnp.sum(router_probs[:, None, :] * choice_hot, axis=-1)

        meta = jnp.concatenate([gate_vals.T.reshape(1, -1), expert_ids.T.astype(F32).reshape(1, -1)], axis=1)
        meta = jnp.pad(meta, ((0, 0), (0, LANES - meta.shape[1])))
        meta_all = gather_rows(meta[None], n_y, n_z, n_ep).reshape(n_dev, LANES)
        ids_all = meta_all[:, 2 * n_tok:4 * n_tok].astype(jnp.int32).reshape(n_dev, 2, n_tok)
        gates_all = meta_all[:, :2 * n_tok].reshape(n_dev, 2, n_tok)
        all_loads = jnp.sum((ids_all[..., None] == jnp.arange(n_exp, dtype=jnp.int32)).astype(F32), axis=(0, 1, 2))
        load_frac = all_loads / (2 * total_tok)

        dy_f32 = grad_out.astype(F32)
        d_picked = (dy_f32[:, None, :] * gate_vals[:, :, None]).astype(BF16).reshape(n_tok * 2, width)
        send = jnp.concatenate([
            jnp.take(x_norm, slot_owner // 2, axis=0, mode="fill", fill_value=0),
            jnp.take(d_picked, slot_owner, axis=0, mode="fill", fill_value=0)], axis=1)
        recv = lax.all_to_all(send.reshape(n_exp, capacity, 2 * width), "ep", 0, 0, tiled=True).reshape(n_exp * capacity, 2 * width)
        wg, wu, wd = w_gate[0], w_up[0], w_down[0]
        done = local_ffn(recv, wg, wu, wd, 256)
        back = lax.all_to_all(done.reshape(n_exp, capacity, 2 * width), "ep", 0, 0, tiled=True).reshape(n_exp * capacity, 2 * width)
        both = jnp.take(back, dest_rows, axis=0).reshape(n_tok, 2, 2 * width)
        picked, d_xn_exp = both[..., :width], both[..., width:]
        out_hidden = (x_f32 + jnp.sum(gate_vals[:, :, None] * picked, axis=1)).astype(BF16)
        d_gates = jnp.sum(dy_f32[:, None, :] * picked, axis=-1)

        d_probs = jnp.sum(d_gates[:, :, None] * choice_hot, axis=1) + (AUX_COEF * n_exp / total_tok) * load_frac
        d_logits = router_probs * (d_probs - jnp.sum(router_probs * d_probs, axis=-1, keepdims=True))
        d_xnorm = jnp.einsum("te,de->td", d_logits, w_router) + d_xn_exp[:, 0].astype(F32) + d_xn_exp[:, 1].astype(F32)
        d_xnorm = d_xnorm.astype(BF16).astype(F32)
        value_a6 = d_xnorm * norm_gain
        grad_hidden = (inv_rms * (value_a6 - x_hat * jnp.mean(value_a6 * x_hat, axis=-1, keepdims=True)) + dy_f32).astype(BF16)

        part_router = jnp.einsum("te,td->ed", d_logits, xn_f32).reshape(-1)
        part_gain = jnp.sum(d_xnorm * x_hat, axis=0)
        flat = jnp.concatenate([part_router, part_gain, jnp.sum(router_probs, axis=0)])
        unit = n_ep * 8 * LANES
        size = -(-flat.shape[0] // unit) * unit
        summed = reduce_rows(jnp.pad(flat, (0, size - flat.shape[0])).reshape(n_ep, -1, LANES), n_y, n_z, n_ep).reshape(-1)
        grad_router = summed[:n_exp * width].reshape(n_exp, width).T
        grad_gain = summed[n_exp * width:(n_exp + 1) * width]
        prob_sum = summed[(n_exp + 1) * width:(n_exp + 1) * width + n_exp]
        aux_loss = AUX_COEF * n_exp * jnp.sum(load_frac * prob_sum / total_tok)

        me = lax.axis_index("ep")
        mine = ids_all == me
        member = jnp.any(mine, axis=1).reshape(-1, GROUP)
        gate_me = jnp.sum(jnp.where(mine, gates_all, 0.0), axis=1).reshape(-1, 1, GROUP)
        rank = jnp.cumsum(member.astype(jnp.int32), axis=1)
        counts = rank[:, -1]
        offsets = jnp.cumsum(counts) - counts
        n_rows = offsets[-1] + counts[-1]
        pos = jnp.where(member, offsets[:, None] + rank - 1, -(2**24)).reshape(-1, 1, GROUP)

        def one_pass(first):
            xn, dp = pack_rows(rows_all, offsets, jnp.full((1,), first, jnp.int32), pos, gate_me, cap, GROUP // n_tok * capacity)
            act, d_gate, d_up = expert_math(dot(xn, wg, ((1,), (0,))), dot(xn, wu, ((1,), (0,))), dot(dp, wd, ((1,), (1,))))
            return dot(xn, d_gate, ((0,), (0,))), dot(xn, d_up, ((0,), (0,))), dot(act, dp, ((0,), (0,)))

        def few():
            return tuple(g.astype(BF16)[None] for g in one_pass(0))

        def many():
            return tuple((a + b).astype(BF16)[None] for a, b in zip(one_pass(0), one_pass(cap)))

        g_gate, g_up, g_down = lax.cond(n_rows <= cap, few, many)
        return out_hidden, aux_loss, grad_hidden, grad_gain, grad_router, g_gate, g_up, g_down

    tok_spec = P(all_axes, None)
    w_spec = P("ep", None, None)
    return jax.shard_map(local_step, mesh=mesh, in_specs=(tok_spec, tok_spec, tok_spec, P(), P(), w_spec, w_spec, w_spec), out_specs=(tok_spec, P(), tok_spec, P(), P(), w_spec, w_spec, w_spec), check_vma=False)
```

```python
import functools
import jax
import jax.numpy as jnp
from jax import lax
from jax.experimental import pallas as pl
from jax.experimental.pallas import tpu as pltpu
from jax.sharding import PartitionSpec as P

EPS = 1e-6
AUX_COEF = 0.001
LANES = 128
GROUP = 256
ALIGN = 16
TILE = 256
FIRST_ROWS = 1024
LAST_ROWS = 1280
F32 = jnp.float32
BF16 = jnp.bfloat16


def route_tables(expert_ids, n_exp, capacity):
    flat_ids = expert_ids.reshape(-1)
    n_choice = flat_ids.shape[0]
    one_hot = (flat_ids[:, None] == jnp.arange(n_exp, dtype=jnp.int32)[None, :]).astype(jnp.int32)
    running = jnp.cumsum(one_hot, axis=0) - 1
    dest_rows = flat_ids * capacity + jnp.sum(running * one_hot, axis=1)
    slot_owner = jnp.full((n_exp * capacity,), n_choice, jnp.int32).at[dest_rows].set(jnp.arange(n_choice, dtype=jnp.int32))
    return dest_rows, slot_owner, jnp.sum(one_hot, axis=0)


def peers(n_y, n_z, n_ep):
    dp, ep = lax.axis_index("dp"), lax.axis_index("ep")
    y, z = lax.rem(dp, n_y), lax.div(dp, n_y)
    along_ep = [{"dp": dp, "ep": lax.rem(ep + k, n_ep)} for k in range(1, n_ep)]
    along_y = [{"dp": z * n_y + lax.rem(y + k, n_y), "ep": ep} for k in range(1, n_y)]
    along_z = [{"dp": lax.rem(z + k, n_z) * n_y + y, "ep": ep} for k in range(1, n_z)]
    return dp, ep, y, z, along_ep, along_y, along_z


def enter(all_peers):
    barrier = pltpu.get_barrier_semaphore()
    for peer in all_peers:
        pl.semaphore_signal(barrier, inc=1, device_id=peer, device_id_type=pl.DeviceIdType.MESH)
    pl.semaphore_wait(barrier, len(all_peers))


def exchange(targets, make):
    copies = [make(k, target) for k, target in enumerate(targets)]
    for copy in copies:
        copy.start()
    for copy in copies:
        copy.wait()


def remote(src, dst, send_sem, recv_sem, target):
    return pltpu.make_async_remote_copy(src_ref=src, dst_ref=dst, send_sem=send_sem, recv_sem=recv_sem, device_id=target, device_id_type=pl.DeviceIdType.MESH)


def gather_kernel(n_y, n_z, n_ep, row_ref, out_ref, send_sem, recv_sem):
    dp, ep, y, z, along_ep, along_y, along_z = peers(n_y, n_z, n_ep)
    enter(along_ep + along_y + along_z)
    mine = out_ref.at[pl.ds(dp * n_ep + ep, 1)]
    local = pltpu.make_async_copy(row_ref, mine, send_sem.at[0])
    local.start()
    local.wait()
    base = 0
    exchange(along_ep, lambda k, t: remote(row_ref, mine, send_sem.at[base + k], recv_sem.at[base + k], t))
    base = len(along_ep)
    rows_y = out_ref.at[pl.ds(dp * n_ep, n_ep)]
    exchange(along_y, lambda k, t: remote(rows_y, rows_y, send_sem.at[base + k], recv_sem.at[base + k], t))
    base += len(along_y)
    rows_z = out_ref.at[pl.ds(z * n_y * n_ep, n_y * n_ep)]
    exchange(along_z, lambda k, t: remote(rows_z, rows_z, send_sem.at[base + k], recv_sem.at[base + k], t))


def gather_rows(row, n_y, n_z, n_ep):
    n_dev = n_y * n_z * n_ep
    n_sem = n_ep + n_y + n_z - 3
    return pl.pallas_call(
        functools.partial(gather_kernel, n_y, n_z, n_ep),
        out_shape=jax.ShapeDtypeStruct((n_dev, 1, LANES), F32),
        in_specs=[pl.BlockSpec(memory_space=pltpu.VMEM)],
        out_specs=pl.BlockSpec(memory_space=pltpu.VMEM),
        scratch_shapes=[pltpu.SemaphoreType.DMA((n_sem,)), pltpu.SemaphoreType.DMA((n_sem,))],
        compiler_params=pltpu.CompilerParams(collective_id=1, has_side_effects=True),
        name="gather_rows",
    )(row)


def reduce_kernel(n_y, n_z, n_ep, in_ref, out_ref, got_ep, got_y, got_z, send_sem, recv_sem):
    dp, ep, y, z, along_ep, along_y, along_z = peers(n_y, n_z, n_ep)
    enter(along_ep + along_y + along_z)
    base = 0
    got_ep[ep] = in_ref[ep]
    exchange(along_ep, lambda k, t: remote(in_ref.at[t["ep"]], got_ep.at[ep], send_sem.at[base + k], recv_sem.at[base + k], t))
    total = got_ep[0]
    for k in range(1, n_ep):
        total = total + got_ep[k]
    got_y[y] = total
    base = len(along_ep)
    exchange(along_y, lambda k, t: remote(got_y.at[y], got_y.at[y], send_sem.at[base + k], recv_sem.at[base + k], t))
    total = got_y[0]
    for k in range(1, n_y):
        total = total + got_y[k]
    got_z[z] = total
    base += len(along_y)
    exchange(along_z, lambda k, t: remote(got_z.at[z], got_z.at[z], send_sem.at[base + k], recv_sem.at[base + k], t))
    total = got_z[0]
    for k in range(1, n_z):
        total = total + got_z[k]
    out_ref[ep] = total
    base += len(along_z)
    exchange(along_ep, lambda k, t: remote(out_ref.at[ep], out_ref.at[ep], send_sem.at[base + k], recv_sem.at[base + k], t))


def reduce_rows(parts, n_y, n_z, n_ep):
    n_sem = 2 * n_ep + n_y + n_z - 4
    chunk = parts.shape[1:]
    return pl.pallas_call(
        functools.partial(reduce_kernel, n_y, n_z, n_ep),
        out_shape=jax.ShapeDtypeStruct(parts.shape, F32),
        in_specs=[pl.BlockSpec(memory_space=pltpu.VMEM)],
        out_specs=pl.BlockSpec(memory_space=pltpu.VMEM),
        scratch_shapes=[pltpu.VMEM((n_ep, *chunk), F32), pltpu.VMEM((n_y, *chunk), F32), pltpu.VMEM((n_z, *chunk), F32), pltpu.SemaphoreType.DMA((n_sem,)), pltpu.SemaphoreType.DMA((n_sem,))],
        compiler_params=pltpu.CompilerParams(collective_id=2, has_side_effects=True),
        name="reduce_rows",
    )(parts)


def dot(a, b, dims):
    return lax.dot_general(a, b, (dims, ((), ())), preferred_element_type=F32)


def expert_math(hg, hu, da):
    gate = hg.astype(BF16).astype(F32)
    up = hu.astype(BF16).astype(F32)
    d_act = da.astype(BF16).astype(F32)
    sig = jax.nn.sigmoid(gate)
    silu = gate * sig
    act = (silu * up).astype(BF16)
    d_up = (d_act * silu).astype(BF16)
    d_gate = (d_act * up * sig * (1.0 + gate * (1.0 - sig))).astype(BF16)
    return act, d_gate, d_up


def ffn_kernel(rows_ref, wg_ref, wu_ref, wd_ref, out_ref, o_acc, d_acc):
    step = pl.program_id(0)
    width = wg_ref.shape[0]
    half = wg_ref.shape[1] // 2
    xn, dp = rows_ref[:, :width], rows_ref[:, width:]

    @pl.when(step == 0)
    def _():
        o_acc[...] = jnp.zeros_like(o_acc)
        d_acc[...] = jnp.zeros_like(d_acc)

    cols = [slice(0, half), slice(half, 2 * half)]
    mid = [expert_math(dot(xn, wg_ref[:, c], ((1,), (0,))), dot(xn, wu_ref[:, c], ((1,), (0,))), dot(dp, wd_ref[c, :], ((1,), (1,)))) for c in cols]
    act, d_gate, d_up = (jnp.concatenate(parts, axis=1) for parts in zip(*mid))
    o_acc[...] += dot(act, wd_ref[...], ((1,), (0,)))
    d_acc[...] += dot(d_gate, wg_ref[...], ((1,), (1,))) + dot(d_up, wu_ref[...], ((1,), (1,)))

    @pl.when(step == pl.num_programs(0) - 1)
    def _():
        out_ref[:, :width] = o_acc[...].astype(BF16)
        out_ref[:, width:] = d_acc[...].astype(BF16)


def local_ffn(rows, wg, wu, wd, block):
    n, width = rows.shape[0], wg.shape[0]
    ff = wg.shape[1]
    whole = pl.BlockSpec((n, 2 * width), lambda j: (0, 0))
    col = pl.BlockSpec((width, block), lambda j: (0, j))
    row = pl.BlockSpec((block, width), lambda j: (j, 0))
    return pl.pallas_call(
        ffn_kernel,
        grid=(ff // block,),
        out_shape=jax.ShapeDtypeStruct((n, 2 * width), BF16),
        in_specs=[whole, col, col, row],
        out_specs=whole,
        scratch_shapes=[pltpu.VMEM((n, width), F32), pltpu.VMEM((n, width), F32)],
        compiler_params=pltpu.CompilerParams(dimension_semantics=("arbitrary",), vmem_limit_bytes=40 * 2**20),
        cost_estimate=pl.CostEstimate(flops=12 * n * width * ff, bytes_accessed=6 * width * ff, transcendentals=0),
        name="local_ffn",
    )(rows, wg, wu, wd)


def pack_kernel(cap, n_early, info_ref, off_ref, early_ref, late_ref, pos_ref, gate_ref, xn_out, dp_out, xn_buf, dp_buf, sem):
    g = pl.program_id(0)
    first = info_ref[0]
    width = xn_buf.shape[1]
    tile = xn_buf.shape[0] - cap
    off = off_ref[g] - first
    base = pl.multiple_of(jnp.clip(lax.div(off, ALIGN) * ALIGN, 0, cap), ALIGN)

    @pl.when(g == 0)
    def _():
        xn_buf[...] = jnp.zeros_like(xn_buf)
        dp_buf[...] = jnp.zeros_like(dp_buf)

    def add(rows_ref):
        row_id = lax.broadcasted_iota(jnp.int32, (tile, GROUP), 0) + base
        hit = row_id == pos_ref[0] - first
        pick = hit.astype(F32).astype(BF16)
        gate = jnp.sum(jnp.where(hit, gate_ref[0], 0.0), axis=1, keepdims=True)
        xn = dot(pick, rows_ref[:, :width], ((1,), (0,))).astype(BF16)
        dp = (dot(pick, rows_ref[:, width:], ((1,), (0,))) * gate).astype(BF16)
        keep = lax.broadcasted_iota(jnp.int32, (ALIGN, width), 0) + base < off
        for buf, new in ((xn_buf, xn), (dp_buf, dp)):
            head = pl.ds(base, ALIGN)
            buf[head, :] = jnp.where(keep, buf[head, :].astype(F32), new[:ALIGN].astype(F32)).astype(BF16)
            buf[pl.ds(pl.multiple_of(base + ALIGN, ALIGN), tile - ALIGN), :] = new[ALIGN:]

    @pl.when(jnp.logical_and(g >= info_ref[1], g < n_early))
    def _():
        add(early_ref)

    @pl.when(jnp.logical_and(g >= info_ref[1], g >= n_early))
    def _():
        add(late_ref)

    @pl.when(g == pl.num_programs(0) - 1)
    def _():
        copies = [pltpu.make_async_copy(xn_buf.at[pl.ds(0, cap)], xn_out, sem.at[0]), pltpu.make_async_copy(dp_buf.at[pl.ds(0, cap)], dp_out, sem.at[1])]
        for copy in copies:
            copy.start()
        for copy in copies:
            copy.wait()


def pack_rows(early, late, offsets, first, start, n_group, pos, gates, cap):
    width = early.shape[1] // 2
    n_early, n_late = early.shape[0] // GROUP, late.shape[0] // GROUP
    tile = GROUP + ALIGN
    small = pl.BlockSpec((1, 1, GROUP), lambda g, info, off: (jnp.maximum(g, info[1]), 0, 0))
    return pl.pallas_call(
        functools.partial(pack_kernel, cap, n_early),
        grid_spec=pltpu.PrefetchScalarGridSpec(
            num_scalar_prefetch=2,
            grid=(n_group,),
            in_specs=[
                pl.BlockSpec((GROUP, 2 * width), lambda g, info, off: (jnp.minimum(jnp.maximum(g, info[1]), n_early - 1), 0)),
                pl.BlockSpec((GROUP, 2 * width), lambda g, info, off: (jnp.clip(g - n_early, 0, n_late - 1), 0)),
                small, small],
            out_specs=[pl.BlockSpec(memory_space=pl.ANY), pl.BlockSpec(memory_space=pl.ANY)],
            scratch_shapes=[pltpu.VMEM((cap + tile, width), BF16), pltpu.VMEM((cap + tile, width), BF16), pltpu.SemaphoreType.DMA((2,))],
        ),
        out_shape=[jax.ShapeDtypeStruct((cap, width), BF16)] * 2,
        compiler_params=pltpu.CompilerParams(dimension_semantics=("arbitrary",), vmem_limit_bytes=50 * 2**20),
        cost_estimate=pl.CostEstimate(flops=64 * tile * GROUP * width, bytes_accessed=64 * GROUP * width, transcendentals=0),
        name="pack_rows",
    )(jnp.stack([jnp.asarray(first, jnp.int32), jnp.asarray(start, jnp.int32)]), offsets, early, late, pos, gates)


def grads_kernel(n_part, xn_hbm, dp_hbm, wg_ref, wu_ref, wd_ref, *refs):
    parts, (gg_ref, gu_ref, gd_ref, xn, xt, dp, act_t, d_gate, d_up, sem) = refs[:n_part], refs[n_part:]
    rows, width = xn.shape
    tiles = [slice(r, r + TILE) for r in range(0, rows, TILE)]

    @pl.when(pl.program_id(0) == 0)
    def _():
        copies = [[pltpu.make_async_copy(src.at[pl.ds(t.start, TILE)], dst.at[pl.ds(t.start, TILE)], sem.at[k, i]) for i, t in enumerate(tiles)] for k, (src, dst) in enumerate(((xn_hbm, xn), (dp_hbm, dp)))]
        for copy in copies[0] + copies[1]:
            copy.start()
        for copy, t in zip(copies[0], tiles):
            copy.wait()
            xt[:, t] = xn[t, :].T
        for copy in copies[1]:
            copy.wait()

    wg, wu, wd = wg_ref[...], wu_ref[...], wd_ref[...]
    for t in tiles:
        act, d_gate[t, :], d_up[t, :] = expert_math(dot(xn[t, :], wg, ((1,), (0,))), dot(xn[t, :], wu, ((1,), (0,))), dot(dp[t, :], wd, ((1,), (1,))))
        act_t[:, t] = act.T

    def put(out, index, k, value):
        if n_part:
            value = value + parts[k][(0, *index)]
        if out.dtype == F32:
            out[(0, *index)] = value
        else:
            out[index] = value.astype(out.dtype)

    wide = 2 * TILE if width % (2 * TILE) == 0 else TILE
    for c in range(0, width, wide):
        cut = slice(c, c + wide)
        put(gg_ref, (cut, slice(None)), 0, dot(xt[cut, :], d_gate[...], ((1,), (0,))))
        put(gu_ref, (cut, slice(None)), 1, dot(xt[cut, :], d_up[...], ((1,), (0,))))
    for c in range(0, width, wide):
        cut = slice(c, c + wide)
        put(gd_ref, (slice(None), cut), 2, dot(act_t[...], dp[:, cut], ((1,), (0,))))


def expert_grads(xn, dp, wg, wu, wd, parts, last):
    rows, width = xn.shape
    ff = wg.shape[1]
    n_block = ff // TILE
    hbm = pl.BlockSpec(memory_space=pl.ANY)
    col = pl.BlockSpec((width, TILE), lambda j: (0, j))
    row = pl.BlockSpec((TILE, width), lambda j: (j, 0))
    col_part = pl.BlockSpec((1, width, TILE), lambda j: (j, 0, 0))
    row_part = pl.BlockSpec((1, TILE, width), lambda j: (j, 0, 0))
    part_specs = [col_part, col_part, row_part]
    if last:
        outs = [jax.ShapeDtypeStruct((width, ff), BF16)] * 2 + [jax.ShapeDtypeStruct((ff, width), BF16)]
    else:
        outs = [jax.ShapeDtypeStruct((n_block, width, TILE), F32)] * 2 + [jax.ShapeDtypeStruct((n_block, TILE, width), F32)]
    return pl.pallas_call(
        functools.partial(grads_kernel, len(parts)),
        grid=(n_block,),
        in_specs=[hbm, hbm, col, col, row] + part_specs[:len(parts)],
        out_specs=[col, col, row] if last else part_specs,
        out_shape=outs,
        scratch_shapes=[pltpu.VMEM((rows, width), BF16), pltpu.VMEM((width, rows), BF16), pltpu.VMEM((rows, width), BF16), pltpu.VMEM((TILE, rows), BF16), pltpu.VMEM((rows, TILE), BF16), pltpu.VMEM((rows, TILE), BF16), pltpu.SemaphoreType.DMA((2, rows // TILE))],
        input_output_aliases={} if last or not parts else {5: 0, 6: 1, 7: 2},
        compiler_params=pltpu.CompilerParams(dimension_semantics=("arbitrary",), vmem_limit_bytes=62 * 2**20),
        cost_estimate=pl.CostEstimate(flops=12 * rows * width * ff, bytes_accessed=12 * width * ff, transcendentals=0),
        name="expert_grads",
    )(xn, dp, wg, wu, wd, *parts)


def solution(mesh):
    n_ep = mesh.shape["ep"]
    n_dp = mesh.shape["dp"]
    n_y = 4 if n_dp == 32 else 2
    n_z = n_dp // n_y
    n_dev = n_dp * n_ep
    all_axes = ("dp", "ep")

    def local_step(hidden, grad_out, expert_ids, norm_gain, w_router, w_gate, w_up, w_down):
        n_tok, width = hidden.shape
        n_exp = w_router.shape[1]
        capacity = 4 * n_tok // n_exp
        total_tok = n_tok * n_dev
        dest_rows, slot_owner, loads = route_tables(expert_ids, n_exp, capacity)
        choice_hot = (expert_ids[:, :, None] == jnp.arange(n_exp, dtype=jnp.int32)).astype(F32)

        x_f32 = hidden.astype(F32)
        inv_rms = lax.rsqrt(jnp.mean(x_f32 * x_f32, axis=-1, keepdims=True) + EPS)
        x_hat = x_f32 * inv_rms
        x_norm = (x_hat * norm_gain).astype(BF16)
        rows = jnp.concatenate([x_norm, grad_out], axis=1)
        half = n_tok // 2
        early = lax.all_gather(rows[:half], all_axes, axis=0, tiled=True)
        late = lax.all_gather(rows[half:], all_axes, axis=0, tiled=True)
        xn_f32 = x_norm.astype(F32)
        router_probs = jax.nn.softmax(jnp.dot(xn_f32, w_router, preferred_element_type=F32), axis=-1)
        gate_vals = jnp.sum(router_probs[:, None, :] * choice_hot, axis=-1)

        meta = jnp.concatenate([gate_vals.T.reshape(1, -1), expert_ids.T.astype(F32).reshape(1, -1)], axis=1)
        meta = jnp.pad(meta, ((0, 0), (0, LANES - meta.shape[1])))
        meta_all = gather_rows(meta[None], n_y, n_z, n_ep).reshape(n_dev, LANES)
        ids_all = meta_all[:, 2 * n_tok:4 * n_tok].astype(jnp.int32).reshape(n_dev, 2, n_tok)
        gates_all = meta_all[:, :2 * n_tok].reshape(n_dev, 2, n_tok)
        all_loads = jnp.sum((ids_all[..., None] == jnp.arange(n_exp, dtype=jnp.int32)).astype(F32), axis=(0, 1, 2))
        load_frac = all_loads / (2 * total_tok)

        dy_f32 = grad_out.astype(F32)
        d_picked = (dy_f32[:, None, :] * gate_vals[:, :, None]).astype(BF16).reshape(n_tok * 2, width)
        send = jnp.concatenate([
            jnp.take(x_norm, slot_owner // 2, axis=0, mode="fill", fill_value=0),
            jnp.take(d_picked, slot_owner, axis=0, mode="fill", fill_value=0)], axis=1)
        recv = lax.all_to_all(send.reshape(n_exp, capacity, 2 * width), "ep", 0, 0, tiled=True).reshape(n_exp * capacity, 2 * width)
        wg, wu, wd = w_gate[0], w_up[0], w_down[0]
        done = local_ffn(recv, wg, wu, wd, 2 * TILE)
        back = lax.all_to_all(done.reshape(n_exp, capacity, 2 * width), "ep", 0, 0, tiled=True).reshape(n_exp * capacity, 2 * width)
        both = jnp.take(back, dest_rows, axis=0).reshape(n_tok, 2, 2 * width)
        picked, d_xn_exp = both[..., :width], both[..., width:]
        out_hidden = (x_f32 + jnp.sum(gate_vals[:, :, None] * picked, axis=1)).astype(BF16)
        d_gates = jnp.sum(dy_f32[:, None, :] * picked, axis=-1)

        d_probs = jnp.sum(d_gates[:, :, None] * choice_hot, axis=1) + (AUX_COEF * n_exp / total_tok) * load_frac
        d_logits = router_probs * (d_probs - jnp.sum(router_probs * d_probs, axis=-1, keepdims=True))
        d_xnorm = jnp.einsum("te,de->td", d_logits, w_router) + d_xn_exp[:, 0].astype(F32) + d_xn_exp[:, 1].astype(F32)
        d_xnorm = d_xnorm.astype(BF16).astype(F32)
        value_a6 = d_xnorm * norm_gain
        grad_hidden = (inv_rms * (value_a6 - x_hat * jnp.mean(value_a6 * x_hat, axis=-1, keepdims=True)) + dy_f32).astype(BF16)

        part_router = jnp.einsum("te,td->ed", d_logits, xn_f32).reshape(-1)
        part_gain = jnp.sum(d_xnorm * x_hat, axis=0)
        flat = jnp.concatenate([part_router, part_gain, jnp.sum(router_probs, axis=0)])
        unit = n_ep * 8 * LANES
        size = -(-flat.shape[0] // unit) * unit
        summed = reduce_rows(jnp.pad(flat, (0, size - flat.shape[0])).reshape(n_ep, -1, LANES), n_y, n_z, n_ep).reshape(-1)
        grad_router = summed[:n_exp * width].reshape(n_exp, width).T
        grad_gain = summed[n_exp * width:(n_exp + 1) * width]
        prob_sum = summed[(n_exp + 1) * width:(n_exp + 1) * width + n_exp]
        aux_loss = AUX_COEF * n_exp * jnp.sum(load_frac * prob_sum / total_tok)

        me = lax.axis_index("ep")
        mine = ids_all == me
        member = jnp.any(mine, axis=1)
        gate_me = jnp.sum(jnp.where(mine, gates_all, 0.0), axis=1)

        def by_group(a):
            return jnp.concatenate([a[:, :half].reshape(-1, GROUP), a[:, half:].reshape(-1, GROUP)], axis=0)

        rank = jnp.cumsum(by_group(member.astype(jnp.int32)), axis=1)
        counts = rank[:, -1]
        offsets = jnp.cumsum(counts) - counts
        n_rows = offsets[-1] + counts[-1]
        pos = jnp.where(by_group(member), offsets[:, None] + rank - 1, -(2**24))[:, None]
        gate_me = by_group(gate_me)[:, None]
        n_group, n_early = pos.shape[0], n_dev * half // GROUP
        in_early = jnp.sum(counts[:n_early])
        split = jnp.minimum(in_early, FIRST_ROWS)
        extra = jnp.maximum(n_rows - split - LAST_ROWS + FIRST_ROWS - 1, 0) // FIRST_ROWS
        pos, gate_me, offsets, split, grad_router = lax.optimization_barrier((pos, gate_me, offsets, split, grad_router))

        parts = expert_grads(*pack_rows(early, early, offsets[:n_early], 0, 0, n_early, pos, gate_me, FIRST_ROWS), wg, wu, wd, (), False)

        def more(k, parts):
            xn, dp = pack_rows(early, late, offsets, split + k * FIRST_ROWS, 0, n_group, pos, gate_me, FIRST_ROWS)
            return tuple(expert_grads(xn, dp, wg, wu, wd, tuple(parts), False))

        parts = lax.fori_loop(0, extra, more, tuple(parts))
        split = split + extra * FIRST_ROWS
        start = jnp.minimum(jnp.sum((offsets + counts <= split).astype(jnp.int32)), n_group - 1)
        grads = expert_grads(*pack_rows(early, late, offsets, split, start, n_group, pos, gate_me, LAST_ROWS), wg, wu, wd, parts, True)
        g_gate, g_up, g_down = (g[None] for g in grads)
        return out_hidden, aux_loss, grad_hidden, grad_gain, grad_router, g_gate, g_up, g_down

    tok_spec = P(all_axes, None)
    w_spec = P("ep", None, None)
    return jax.shard_map(local_step, mesh=mesh, in_specs=(tok_spec, tok_spec, tok_spec, P(), P(), w_spec, w_spec, w_spec), out_specs=(tok_spec, P(), tok_spec, P(), P(), w_spec, w_spec, w_spec), check_vma=False)
```

```python
import functools
import jax
import jax.numpy as jnp
from jax import lax
from jax.experimental import pallas as pl
from jax.experimental.pallas import tpu as pltpu
from jax.sharding import PartitionSpec as P

EPS = 1e-6
AUX_COEF = 0.001
LANES = 128
GROUP = 256
MOST_PER_GROUP = 128
ALIGN = 16
TILE = 256
USUAL_ROWS = 2304
QUARTERS = 4
F32 = jnp.float32
BF16 = jnp.bfloat16


def route_tables(expert_ids, n_exp, capacity):
    flat_ids = expert_ids.reshape(-1)
    n_choice = flat_ids.shape[0]
    one_hot = (flat_ids[:, None] == jnp.arange(n_exp, dtype=jnp.int32)[None, :]).astype(jnp.int32)
    running = jnp.cumsum(one_hot, axis=0) - 1
    dest_rows = flat_ids * capacity + jnp.sum(running * one_hot, axis=1)
    slot_owner = jnp.full((n_exp * capacity,), n_choice, jnp.int32).at[dest_rows].set(jnp.arange(n_choice, dtype=jnp.int32))
    return dest_rows, slot_owner, jnp.sum(one_hot, axis=0)


def peers(n_y, n_z, n_ep):
    dp, ep = lax.axis_index("dp"), lax.axis_index("ep")
    y, z = lax.rem(dp, n_y), lax.div(dp, n_y)
    along_ep = [{"dp": dp, "ep": lax.rem(ep + k, n_ep)} for k in range(1, n_ep)]
    along_y = [{"dp": z * n_y + lax.rem(y + k, n_y), "ep": ep} for k in range(1, n_y)]
    along_z = [{"dp": lax.rem(z + k, n_z) * n_y + y, "ep": ep} for k in range(1, n_z)]
    return dp, ep, y, z, along_ep, along_y, along_z


def enter(all_peers):
    barrier = pltpu.get_barrier_semaphore()
    for peer in all_peers:
        pl.semaphore_signal(barrier, inc=1, device_id=peer, device_id_type=pl.DeviceIdType.MESH)
    pl.semaphore_wait(barrier, len(all_peers))


def exchange(targets, make):
    copies = [make(k, target) for k, target in enumerate(targets)]
    for copy in copies:
        copy.start()
    for copy in copies:
        copy.wait()


def remote(src, dst, send_sem, recv_sem, target):
    return pltpu.make_async_remote_copy(src_ref=src, dst_ref=dst, send_sem=send_sem, recv_sem=recv_sem, device_id=target, device_id_type=pl.DeviceIdType.MESH)


def gather_kernel(n_y, n_z, n_ep, row_ref, out_ref, send_sem, recv_sem):
    dp, ep, y, z, along_ep, along_y, along_z = peers(n_y, n_z, n_ep)
    enter(along_ep + along_y + along_z)
    mine = out_ref.at[pl.ds(dp * n_ep + ep, 1)]
    local = pltpu.make_async_copy(row_ref, mine, send_sem.at[0])
    local.start()
    local.wait()
    base = 0
    exchange(along_ep, lambda k, t: remote(row_ref, mine, send_sem.at[base + k], recv_sem.at[base + k], t))
    base = len(along_ep)
    rows_y = out_ref.at[pl.ds(dp * n_ep, n_ep)]
    exchange(along_y, lambda k, t: remote(rows_y, rows_y, send_sem.at[base + k], recv_sem.at[base + k], t))
    base += len(along_y)
    rows_z = out_ref.at[pl.ds(z * n_y * n_ep, n_y * n_ep)]
    exchange(along_z, lambda k, t: remote(rows_z, rows_z, send_sem.at[base + k], recv_sem.at[base + k], t))


def gather_rows(row, n_y, n_z, n_ep):
    n_dev = n_y * n_z * n_ep
    n_sem = n_ep + n_y + n_z - 3
    return pl.pallas_call(
        functools.partial(gather_kernel, n_y, n_z, n_ep),
        out_shape=jax.ShapeDtypeStruct((n_dev, 1, LANES), F32),
        in_specs=[pl.BlockSpec(memory_space=pltpu.VMEM)],
        out_specs=pl.BlockSpec(memory_space=pltpu.VMEM),
        scratch_shapes=[pltpu.SemaphoreType.DMA((n_sem,)), pltpu.SemaphoreType.DMA((n_sem,))],
        compiler_params=pltpu.CompilerParams(collective_id=1, has_side_effects=True),
        name="gather_rows",
    )(row)


def reduce_kernel(n_y, n_z, n_ep, in_ref, out_ref, got_ep, got_y, got_z, send_sem, recv_sem):
    dp, ep, y, z, along_ep, along_y, along_z = peers(n_y, n_z, n_ep)
    enter(along_ep + along_y + along_z)
    base = 0
    got_ep[ep] = in_ref[ep]
    exchange(along_ep, lambda k, t: remote(in_ref.at[t["ep"]], got_ep.at[ep], send_sem.at[base + k], recv_sem.at[base + k], t))
    total = got_ep[0]
    for k in range(1, n_ep):
        total = total + got_ep[k]
    got_y[y] = total
    base = len(along_ep)
    exchange(along_y, lambda k, t: remote(got_y.at[y], got_y.at[y], send_sem.at[base + k], recv_sem.at[base + k], t))
    total = got_y[0]
    for k in range(1, n_y):
        total = total + got_y[k]
    got_z[z] = total
    base += len(along_y)
    exchange(along_z, lambda k, t: remote(got_z.at[z], got_z.at[z], send_sem.at[base + k], recv_sem.at[base + k], t))
    total = got_z[0]
    for k in range(1, n_z):
        total = total + got_z[k]
    out_ref[ep] = total
    base += len(along_z)
    exchange(along_ep, lambda k, t: remote(out_ref.at[ep], out_ref.at[ep], send_sem.at[base + k], recv_sem.at[base + k], t))


def reduce_rows(parts, n_y, n_z, n_ep):
    n_sem = 2 * n_ep + n_y + n_z - 4
    chunk = parts.shape[1:]
    return pl.pallas_call(
        functools.partial(reduce_kernel, n_y, n_z, n_ep),
        out_shape=jax.ShapeDtypeStruct(parts.shape, F32),
        in_specs=[pl.BlockSpec(memory_space=pltpu.VMEM)],
        out_specs=pl.BlockSpec(memory_space=pltpu.VMEM),
        scratch_shapes=[pltpu.VMEM((n_ep, *chunk), F32), pltpu.VMEM((n_y, *chunk), F32), pltpu.VMEM((n_z, *chunk), F32), pltpu.SemaphoreType.DMA((n_sem,)), pltpu.SemaphoreType.DMA((n_sem,))],
        compiler_params=pltpu.CompilerParams(collective_id=2, has_side_effects=True),
        name="reduce_rows",
    )(parts)


def dot(a, b, dims):
    return lax.dot_general(a, b, (dims, ((), ())), preferred_element_type=F32)


def expert_math(hg, hu, da):
    gate = hg.astype(BF16).astype(F32)
    up = hu.astype(BF16).astype(F32)
    d_act = da.astype(BF16).astype(F32)
    sig = jax.nn.sigmoid(gate)
    silu = gate * sig
    act = (silu * up).astype(BF16)
    d_up = (d_act * silu).astype(BF16)
    d_gate = (d_act * up * sig * (1.0 + gate * (1.0 - sig))).astype(BF16)
    return act, d_gate, d_up


def ffn_kernel(rows_ref, wg_ref, wu_ref, wd_ref, out_ref, o_acc, d_acc):
    step = pl.program_id(0)
    width = wg_ref.shape[0]
    half = wg_ref.shape[1] // 2
    xn, dp = rows_ref[:, :width], rows_ref[:, width:]

    @pl.when(step == 0)
    def _():
        o_acc[...] = jnp.zeros_like(o_acc)
        d_acc[...] = jnp.zeros_like(d_acc)

    cols = [slice(0, half), slice(half, 2 * half)]
    mid = [expert_math(dot(xn, wg_ref[:, c], ((1,), (0,))), dot(xn, wu_ref[:, c], ((1,), (0,))), dot(dp, wd_ref[c, :], ((1,), (1,)))) for c in cols]
    act, d_gate, d_up = (jnp.concatenate(parts, axis=1) for parts in zip(*mid))
    o_acc[...] += dot(act, wd_ref[...], ((1,), (0,)))
    d_acc[...] += dot(d_gate, wg_ref[...], ((1,), (1,))) + dot(d_up, wu_ref[...], ((1,), (1,)))

    @pl.when(step == pl.num_programs(0) - 1)
    def _():
        out_ref[:, :width] = o_acc[...].astype(BF16)
        out_ref[:, width:] = d_acc[...].astype(BF16)


def local_ffn(rows, wg, wu, wd, block):
    n, width = rows.shape[0], wg.shape[0]
    ff = wg.shape[1]
    whole = pl.BlockSpec((n, 2 * width), lambda j: (0, 0))
    col = pl.BlockSpec((width, block), lambda j: (0, j))
    row = pl.BlockSpec((block, width), lambda j: (j, 0))
    return pl.pallas_call(
        ffn_kernel,
        grid=(ff // block,),
        out_shape=jax.ShapeDtypeStruct((n, 2 * width), BF16),
        in_specs=[whole, col, col, row],
        out_specs=whole,
        scratch_shapes=[pltpu.VMEM((n, width), F32), pltpu.VMEM((n, width), F32)],
        compiler_params=pltpu.CompilerParams(dimension_semantics=("arbitrary",), vmem_limit_bytes=40 * 2**20),
        cost_estimate=pl.CostEstimate(flops=12 * n * width * ff, bytes_accessed=6 * width * ff, transcendentals=0),
        name="local_ffn",
    )(rows, wg, wu, wd)


def pack_kernel(off_ref, rows_ref, pos_ref, gate_ref, xn_out, dp_out, xn_buf, dp_buf, sem):
    g = pl.program_id(0)
    n_group = pl.num_programs(0)
    width = xn_buf.shape[1]
    tile = MOST_PER_GROUP + ALIGN
    off = off_ref[g]
    base = pl.multiple_of(lax.div(off, ALIGN) * ALIGN, ALIGN)
    row_id = lax.broadcasted_iota(jnp.int32, (tile, GROUP), 0) + base
    hit = row_id == pos_ref[0]
    pick = hit.astype(F32).astype(BF16)
    gate = jnp.sum(jnp.where(hit, gate_ref[0], 0.0), axis=1, keepdims=True)
    xn = dot(pick, rows_ref[:, :width], ((1,), (0,))).astype(BF16)
    dp = (dot(pick, rows_ref[:, width:], ((1,), (0,))) * gate).astype(BF16)
    keep = lax.broadcasted_iota(jnp.int32, (ALIGN, width), 0) + base < off
    for buf, new in ((xn_buf, xn), (dp_buf, dp)):
        head = pl.ds(base, ALIGN)
        buf[head, :] = jnp.where(keep, buf[head, :].astype(F32), new[:ALIGN].astype(F32)).astype(BF16)
        buf[pl.ds(pl.multiple_of(base + ALIGN, ALIGN), tile - ALIGN), :] = new[ALIGN:]

    @pl.when(g == n_group - 1)
    def _():
        usual = USUAL_ROWS // TILE
        zeros = jnp.zeros((TILE, width), BF16)
        tail = pl.ds(pl.multiple_of(base + tile, ALIGN), TILE)
        xn_buf[tail, :] = zeros
        dp_buf[tail, :] = zeros
        used = lax.div(off_ref[n_group] + TILE - 1, TILE)

        def clear(t, carry):
            rows = pl.ds(pl.multiple_of(t * TILE, TILE), TILE)
            xn_buf[rows, :] = zeros
            dp_buf[rows, :] = zeros
            return carry

        lax.fori_loop(used, usual, clear, 0)

        def copies(t):
            rows = pl.ds(pl.multiple_of(t * TILE, TILE), TILE)
            return [pltpu.make_async_copy(buf.at[rows], out.at[rows], sem.at[k]) for k, (buf, out) in enumerate(((xn_buf, xn_out), (dp_buf, dp_out)))]

        def begin(t, carry):
            for copy in copies(t):
                copy.start()
            return carry

        def end(t, carry):
            for copy in copies(t):
                copy.wait()
            return carry

        lax.fori_loop(0, jnp.maximum(used, usual), begin, 0)
        lax.fori_loop(0, jnp.maximum(used, usual), end, 0)


def pack_rows(rows, offsets, pos, gates, most):
    total, width = rows.shape[0], rows.shape[1] // 2
    n_group = total // GROUP
    small = pl.BlockSpec((1, 1, GROUP), lambda g, off: (g, 0, 0))
    whole = pl.BlockSpec(memory_space=pl.ANY)
    buf = pltpu.VMEM((max(most, USUAL_ROWS) + 2 * TILE + ALIGN, width), BF16)
    out = jax.ShapeDtypeStruct((max(most, USUAL_ROWS), width), BF16)
    return pl.pallas_call(
        pack_kernel,
        grid_spec=pltpu.PrefetchScalarGridSpec(
            num_scalar_prefetch=1,
            grid=(n_group,),
            in_specs=[pl.BlockSpec((GROUP, 2 * width), lambda g, off: (g, 0)), small, small],
            out_specs=[whole, whole],
            scratch_shapes=[buf, buf, pltpu.SemaphoreType.DMA((2,))],
        ),
        out_shape=[out, out],
        compiler_params=pltpu.CompilerParams(dimension_semantics=("arbitrary",), vmem_limit_bytes=60 * 2**20),
        cost_estimate=pl.CostEstimate(flops=4 * GROUP * total * width, bytes_accessed=4 * total * width, transcendentals=0),
        name="pack_rows",
    )(offsets, rows, pos, gates)


def grads_kernel(n_quarter, info_ref, xn_hbm, dp_hbm, wg_ref, wu_ref, wd_ref, *refs):
    if n_quarter > 1:
        out_ref, xn, xt, dp, act_t, d_gate, d_up, acc_g, acc_u, acc_d, tile_x, tile_p, sem = refs
    else:
        gg_ref, gu_ref, gd_ref, xn, xt, dp, act_t, d_gate, d_up, acc_g, acc_u, acc_d, tile_x, tile_p, sem = refs
    rows, width = xn.shape
    part = width // n_quarter
    low = pl.multiple_of(info_ref[2] * part, part)
    tiles = [slice(r, r + TILE) for r in range(0, rows, TILE)]

    @pl.when(pl.program_id(0) == 0)
    def _():
        copies = [[pltpu.make_async_copy(src.at[pl.ds(t.start, TILE)], dst.at[pl.ds(t.start, TILE)], sem.at[k, i]) for i, t in enumerate(tiles)] for k, (src, dst) in enumerate(((xn_hbm, xn), (dp_hbm, dp)))]
        for copy in copies[0] + copies[1]:
            copy.start()
        for acc in (acc_g, acc_u, acc_d):
            acc[...] = jnp.zeros_like(acc)
        for copy, t in zip(copies[0], tiles):
            copy.wait()
            xt[:, t] = xn[t, pl.ds(low, part)].T
        for copy in copies[1]:
            copy.wait()

    wg, wu, wd = wg_ref[...], wu_ref[...], wd_ref[...]

    def hidden_rows(x, p):
        return expert_math(dot(x, wg, ((1,), (0,))), dot(x, wu, ((1,), (0,))), dot(p, wd, ((1,), (1,))))

    @pl.when(info_ref[0] > rows // TILE)
    def _():
        for acc in (acc_g, acc_u, acc_d):
            acc[...] = jnp.zeros_like(acc)

        def more(t, carry):
            at = pl.ds(pl.multiple_of(t * TILE, TILE), TILE)
            copies = [pltpu.make_async_copy(xn_hbm.at[at], tile_x, sem.at[0, 0]), pltpu.make_async_copy(dp_hbm.at[at], tile_p, sem.at[1, 0])]
            for copy in copies:
                copy.start()
            for copy in copies:
                copy.wait()
            act, dg, du = hidden_rows(tile_x[...], tile_p[...])
            x, p = tile_x[:, pl.ds(low, part)], tile_p[:, pl.ds(low, part)]
            acc_g[...] += dot(x, dg, ((0,), (0,)))
            acc_u[...] += dot(x, du, ((0,), (0,)))
            acc_d[...] += dot(act, p, ((0,), (0,)))
            return carry

        lax.fori_loop(rows // TILE, info_ref[0], more, 0)

    for t in tiles:
        act, d_gate[t, :], d_up[t, :] = hidden_rows(xn[t, :], dp[t, :])
        act_t[:, t] = act.T

    wide = 2 * TILE if part % (2 * TILE) == 0 else TILE
    for c in range(0, part, wide):
        cut = slice(c, c + wide)
        new_g = (dot(xt[cut, :], d_gate[...], ((1,), (0,))) + acc_g[cut, :]).astype(BF16)
        new_u = (dot(xt[cut, :], d_up[...], ((1,), (0,))) + acc_u[cut, :]).astype(BF16)
        if n_quarter > 1:
            out_ref[0, cut, :], out_ref[1, cut, :] = new_g, new_u
        else:
            gg_ref[cut, :], gu_ref[cut, :] = new_g, new_u
    for c in range(0, part, wide):
        cut = slice(c, c + wide)
        if n_quarter > 1:
            new_d = (dot(act_t[...], dp[:, pl.ds(pl.multiple_of(low + c, wide), wide)], ((1,), (0,))) + acc_d[:, cut]).astype(BF16)
            for k in range(0, wide, TILE):
                out_ref[2, slice(c + k, c + k + TILE), :] = new_d[:, k:k + TILE]
        else:
            gd_ref[:, cut] = (dot(act_t[...], dp[:, cut], ((1,), (0,))) + acc_d[:, cut]).astype(BF16)


def expert_grads(info, xn, dp, wg, wu, wd, n_block, n_quarter):
    width, ff = wg.shape
    rows = USUAL_ROWS
    part = width // n_quarter
    hbm = pl.BlockSpec(memory_space=pl.ANY)
    if n_quarter > 1:
        col = pl.BlockSpec((width, TILE), lambda j, info: (0, info[1]))
        row = pl.BlockSpec((TILE, width), lambda j, info: (info[1], 0))
        out_specs = [pl.BlockSpec((3, part, TILE), lambda j, info: (0, 0, 0))]
        outs = [jax.ShapeDtypeStruct((3, part, TILE), BF16)]
    else:
        col = pl.BlockSpec((width, TILE), lambda j, info: (0, j))
        row = pl.BlockSpec((TILE, width), lambda j, info: (j, 0))
        out_specs = [col, col, row]
        outs = [jax.ShapeDtypeStruct((width, ff), BF16)] * 2 + [jax.ShapeDtypeStruct((ff, width), BF16)]
    return pl.pallas_call(
        functools.partial(grads_kernel, n_quarter),
        grid_spec=pltpu.PrefetchScalarGridSpec(
            num_scalar_prefetch=1,
            grid=(n_block,),
            in_specs=[hbm, hbm, col, col, row],
            out_specs=out_specs,
            scratch_shapes=[
                pltpu.VMEM((rows, width), BF16), pltpu.VMEM((part, rows), BF16), pltpu.VMEM((rows, width), BF16),
                pltpu.VMEM((TILE, rows), BF16), pltpu.VMEM((rows, TILE), BF16), pltpu.VMEM((rows, TILE), BF16),
                pltpu.VMEM((part, TILE), F32), pltpu.VMEM((part, TILE), F32), pltpu.VMEM((TILE, part), F32),
                pltpu.VMEM((TILE, width), BF16), pltpu.VMEM((TILE, width), BF16), pltpu.SemaphoreType.DMA((2, rows // TILE))],
        ),
        out_shape=outs,
        compiler_params=pltpu.CompilerParams(dimension_semantics=("arbitrary",), vmem_limit_bytes=63 * 2**20),
        cost_estimate=pl.CostEstimate(flops=12 * rows * width * TILE * n_block, bytes_accessed=12 * width * TILE * n_block, transcendentals=0),
        name="expert_grads" if n_quarter == 1 else "expert_slices",
    )(info, xn, dp, wg, wu, wd)


def place_kernel(slices_ref, gg_in, gu_in, gd_in, gg_ref, gu_ref, gd_ref):
    gg_ref[...] = slices_ref[0]
    gu_ref[...] = slices_ref[1]
    part = gg_ref.shape[0]
    for k in range(0, part, TILE):
        gd_ref[:, k:k + TILE] = slices_ref[2, k:k + TILE, :]


def place_slices(slices, grads, first, n_quarter):
    width, ff = grads[0].shape
    part = width // n_quarter
    hbm = pl.BlockSpec(memory_space=pl.ANY)
    col = pl.BlockSpec((part, TILE), lambda i: (i % n_quarter, first + i // n_quarter))
    row = pl.BlockSpec((TILE, part), lambda i: (first + i // n_quarter, i % n_quarter))
    return pl.pallas_call(
        place_kernel,
        grid=(slices.shape[0] // 3,),
        in_specs=[pl.BlockSpec((3, part, TILE), lambda i: (i, 0, 0)), hbm, hbm, hbm],
        out_specs=[col, col, row],
        out_shape=[jax.ShapeDtypeStruct(g.shape, g.dtype) for g in grads],
        input_output_aliases={1: 0, 2: 1, 3: 2},
        compiler_params=pltpu.CompilerParams(dimension_semantics=("arbitrary",)),
        cost_estimate=pl.CostEstimate(flops=0, bytes_accessed=4 * slices.size, transcendentals=0),
        name="place_slices",
    )(slices, *grads)


def solution(mesh):
    n_ep = mesh.shape["ep"]
    n_dp = mesh.shape["dp"]
    n_y = 4 if n_dp == 32 else 2
    n_z = n_dp // n_y
    n_dev = n_dp * n_ep
    all_axes = ("dp", "ep")

    def local_step(hidden, grad_out, expert_ids, norm_gain, w_router, w_gate, w_up, w_down):
        n_tok, width = hidden.shape
        n_exp = w_router.shape[1]
        capacity = 4 * n_tok // n_exp
        total_tok = n_tok * n_dev
        dest_rows, slot_owner, loads = route_tables(expert_ids, n_exp, capacity)
        choice_hot = (expert_ids[:, :, None] == jnp.arange(n_exp, dtype=jnp.int32)).astype(F32)

        x_f32 = hidden.astype(F32)
        inv_rms = lax.rsqrt(jnp.mean(x_f32 * x_f32, axis=-1, keepdims=True) + EPS)
        x_hat = x_f32 * inv_rms
        x_norm = (x_hat * norm_gain).astype(BF16)
        rows_all = lax.all_gather(jnp.concatenate([x_norm, grad_out], axis=1), all_axes, axis=0, tiled=True)
        xn_f32 = x_norm.astype(F32)
        router_probs = jax.nn.softmax(jnp.dot(xn_f32, w_router, preferred_element_type=F32), axis=-1)
        gate_vals = jnp.sum(router_probs[:, None, :] * choice_hot, axis=-1)

        meta = jnp.concatenate([gate_vals.T.reshape(1, -1), expert_ids.T.astype(F32).reshape(1, -1)], axis=1)
        meta = jnp.pad(meta, ((0, 0), (0, LANES - meta.shape[1])))
        meta_all = gather_rows(meta[None], n_y, n_z, n_ep).reshape(n_dev, LANES)
        ids_all = meta_all[:, 2 * n_tok:4 * n_tok].astype(jnp.int32).reshape(n_dev, 2, n_tok)
        gates_all = meta_all[:, :2 * n_tok].reshape(n_dev, 2, n_tok)
        all_loads = jnp.sum((ids_all[..., None] == jnp.arange(n_exp, dtype=jnp.int32)).astype(F32), axis=(0, 1, 2))
        load_frac = all_loads / (2 * total_tok)

        dy_f32 = grad_out.astype(F32)
        d_picked = (dy_f32[:, None, :] * gate_vals[:, :, None]).astype(BF16).reshape(n_tok * 2, width)
        send = jnp.concatenate([
            jnp.take(x_norm, slot_owner // 2, axis=0, mode="fill", fill_value=0),
            jnp.take(d_picked, slot_owner, axis=0, mode="fill", fill_value=0)], axis=1)
        recv = lax.all_to_all(send.reshape(n_exp, capacity, 2 * width), "ep", 0, 0, tiled=True).reshape(n_exp * capacity, 2 * width)
        wg, wu, wd = w_gate[0], w_up[0], w_down[0]
        done = local_ffn(recv, wg, wu, wd, 2 * TILE)
        back = lax.all_to_all(done.reshape(n_exp, capacity, 2 * width), "ep", 0, 0, tiled=True).reshape(n_exp * capacity, 2 * width)
        both = jnp.take(back, dest_rows, axis=0).reshape(n_tok, 2, 2 * width)
        picked, d_xn_exp = both[..., :width], both[..., width:]
        out_hidden = (x_f32 + jnp.sum(gate_vals[:, :, None] * picked, axis=1)).astype(BF16)
        d_gates = jnp.sum(dy_f32[:, None, :] * picked, axis=-1)

        d_probs = jnp.sum(d_gates[:, :, None] * choice_hot, axis=1) + (AUX_COEF * n_exp / total_tok) * load_frac
        d_logits = router_probs * (d_probs - jnp.sum(router_probs * d_probs, axis=-1, keepdims=True))
        d_xnorm = jnp.einsum("te,de->td", d_logits, w_router) + d_xn_exp[:, 0].astype(F32) + d_xn_exp[:, 1].astype(F32)
        d_xnorm = d_xnorm.astype(BF16).astype(F32)
        value_a6 = d_xnorm * norm_gain
        grad_hidden = (inv_rms * (value_a6 - x_hat * jnp.mean(value_a6 * x_hat, axis=-1, keepdims=True)) + dy_f32).astype(BF16)

        part_router = jnp.einsum("te,td->ed", d_logits, xn_f32).reshape(-1)
        part_gain = jnp.sum(d_xnorm * x_hat, axis=0)
        flat = jnp.concatenate([part_router, part_gain, jnp.sum(router_probs, axis=0)])
        unit = n_ep * 8 * LANES
        size = -(-flat.shape[0] // unit) * unit
        summed = reduce_rows(jnp.pad(flat, (0, size - flat.shape[0])).reshape(n_ep, -1, LANES), n_y, n_z, n_ep).reshape(-1)
        grad_router = summed[:n_exp * width].reshape(n_exp, width).T
        grad_gain = summed[n_exp * width:(n_exp + 1) * width]
        prob_sum = summed[(n_exp + 1) * width:(n_exp + 1) * width + n_exp]
        aux_loss = AUX_COEF * n_exp * jnp.sum(load_frac * prob_sum / total_tok)

        me = lax.axis_index("ep")
        mine = ids_all == me
        member = jnp.any(mine, axis=1).reshape(-1, GROUP)
        gate_me = jnp.sum(jnp.where(mine, gates_all, 0.0), axis=1).reshape(-1, 1, GROUP)
        rank = jnp.cumsum(member.astype(jnp.int32), axis=1)
        counts = rank[:, -1]
        ends = jnp.cumsum(counts)
        offsets = jnp.concatenate([jnp.zeros((1,), jnp.int32), ends])
        pos = jnp.where(member, offsets[:-1, None] + rank - 1, -(2**24))[:, None]
        pos, gate_me, offsets, grad_router = lax.optimization_barrier((pos, gate_me, offsets, grad_router))
        xn, dp = pack_rows(rows_all, offsets, pos, gate_me, capacity * n_dev)
        n_block = w_gate.shape[2] // TILE
        own = n_block - n_dp // QUARTERS
        place = lax.axis_index("dp")
        info = jnp.stack([(offsets[-1] + TILE - 1) // TILE, own + place // QUARTERS, place % QUARTERS]).astype(jnp.int32)
        slices = expert_grads(info, xn, dp, wg, wu, wd, 1, QUARTERS)[0]
        whole_info = info * jnp.array([1, 0, 0], jnp.int32)
        slices_all = lax.all_gather(slices, "dp", axis=0, tiled=True)
        grads = expert_grads(whole_info, xn, dp, wg, wu, wd, own, 1)
        g_gate, g_up, g_down = (g[None] for g in place_slices(slices_all, grads, own, QUARTERS))
        return out_hidden, aux_loss, grad_hidden, grad_gain, grad_router, g_gate, g_up, g_down

    tok_spec = P(all_axes, None)
    w_spec = P("ep", None, None)
    return jax.shard_map(local_step, mesh=mesh, in_specs=(tok_spec, tok_spec, tok_spec, P(), P(), w_spec, w_spec, w_spec), out_specs=(tok_spec, P(), tok_spec, P(), P(), w_spec, w_spec, w_spec), check_vma=False)
```

```python
import functools
import jax
import jax.numpy as jnp
from jax import lax
from jax.experimental import pallas as pl
from jax.experimental.pallas import tpu as pltpu
from jax.sharding import PartitionSpec as P

EPS = 1e-6
AUX_COEF = 0.001
LANES = 128
GROUP = 256
MOST_PER_GROUP = 128
ALIGN = 16
TILE = 256
USUAL_ROWS = 2304
QUARTERS = 4
F32 = jnp.float32
BF16 = jnp.bfloat16


def route_tables(expert_ids, n_exp, capacity):
    flat_ids = expert_ids.reshape(-1)
    n_choice = flat_ids.shape[0]
    one_hot = (flat_ids[:, None] == jnp.arange(n_exp, dtype=jnp.int32)[None, :]).astype(jnp.int32)
    running = jnp.cumsum(one_hot, axis=0) - 1
    dest_rows = flat_ids * capacity + jnp.sum(running * one_hot, axis=1)
    slot_owner = jnp.full((n_exp * capacity,), n_choice, jnp.int32).at[dest_rows].set(jnp.arange(n_choice, dtype=jnp.int32))
    return dest_rows, slot_owner, jnp.sum(one_hot, axis=0)


def peers(n_y, n_z, n_ep):
    dp, ep = lax.axis_index("dp"), lax.axis_index("ep")
    y, z = lax.rem(dp, n_y), lax.div(dp, n_y)
    along_ep = [{"dp": dp, "ep": lax.rem(ep + k, n_ep)} for k in range(1, n_ep)]
    along_y = [{"dp": z * n_y + lax.rem(y + k, n_y), "ep": ep} for k in range(1, n_y)]
    along_z = [{"dp": lax.rem(z + k, n_z) * n_y + y, "ep": ep} for k in range(1, n_z)]
    return dp, ep, y, z, along_ep, along_y, along_z


def enter(all_peers):
    barrier = pltpu.get_barrier_semaphore()
    for peer in all_peers:
        pl.semaphore_signal(barrier, inc=1, device_id=peer, device_id_type=pl.DeviceIdType.MESH)
    pl.semaphore_wait(barrier, len(all_peers))


def exchange(targets, make):
    copies = [make(k, target) for k, target in enumerate(targets)]
    for copy in copies:
        copy.start()
    for copy in copies:
        copy.wait()


def remote(src, dst, send_sem, recv_sem, target):
    return pltpu.make_async_remote_copy(src_ref=src, dst_ref=dst, send_sem=send_sem, recv_sem=recv_sem, device_id=target, device_id_type=pl.DeviceIdType.MESH)


def dot(a, b, dims):
    return lax.dot_general(a, b, (dims, ((), ())), preferred_element_type=F32)


def expert_math(hg, hu, da):
    gate = hg.astype(BF16).astype(F32)
    up = hu.astype(BF16).astype(F32)
    d_act = da.astype(BF16).astype(F32)
    sig = jax.nn.sigmoid(gate)
    silu = gate * sig
    act = (silu * up).astype(BF16)
    d_up = (d_act * silu).astype(BF16)
    d_gate = (d_act * up * sig * (1.0 + gate * (1.0 - sig))).astype(BF16)
    return act, d_gate, d_up


LINK_RATE, HOP_US, FFN_US, FFN_FROM_US = 46e3, 3.0, 3.5, 24.0
PIECES = (
    (0, None, "xyz"), (3, 0, "zxy"), (3, 1, "zyx"), (1, None, "yzx"), (2, None, "xzy"))


def due(left, sizes):
    ready = []
    for piece in range(len(PIECES)):
        for phase in (1, 2):
            if (piece, phase) not in left and left.get((piece, phase - 1)) == 0:
                if (piece, phase) != (0, 2) or all(left.get((other, 1)) == 0 for other in (3, 4)):
                    ready.append((piece, phase))
    return ready


def plan(sizes, tile_bytes, n_ffn):
    free, arrive, order, left = {}, [], [], {}
    ffn, now = 0, 8.0

    def issue(hop, when):
        piece, phase, sign, step = hop
        _, half, axes = PIECES[piece]
        size = tile_bytes // (1 if half is None else 2)
        for axis in axes[:phase]:
            size *= sizes[axis]
        size //= 2 if step == sizes[axes[phase]] // 2 else 1
        link = (axes[phase], sign)
        free[link] = max(when, free.get(link, 0.0)) + size / LINK_RATE
        arrive.append((free[link] + HOP_US, hop))

    def begin(piece, phase, when):
        left[piece, phase] = 2 * (sizes[PIECES[piece][2][phase]] // 2)
        for sign in (1, -1):
            issue((piece, phase, sign, 1), when)

    for piece in range(len(PIECES)):
        begin(piece, 0, now)
    while arrive:
        arrive.sort()
        when, hop = arrive[0]
        if ffn < n_ffn and now >= FFN_FROM_US and when > now + 0.4 * FFN_US:
            order.append("ffn")
            ffn, now = ffn + 1, now + FFN_US
            continue
        arrive.pop(0)
        now = max(now, when)
        order.append(hop)
        piece, phase, sign, step = hop
        if step < sizes[PIECES[piece][2][phase]] // 2:
            issue((piece, phase, sign, step + 1), now)
        left[piece, phase] -= 1
        for other in due(left, sizes):
            begin(*other, now)
    return order + ["ffn"] * (n_ffn - ffn), now


class Copies:
    def __init__(self, send_sem, recv_sem):
        self.sems, self.made = (send_sem, recv_sem), {}

    def start(self, name, ends):
        k = len(self.made)
        self.made[name] = lambda: remote(*ends()[:2], self.sems[0].at[k], self.sems[1].at[k], ends()[2])
        self.made[name]().start()

    def wait_recv(self, name):
        self.made[name]().wait_recv()


def gather_kernel(n_y, n_z, n_ep, order, rows_in, send_in, meta_in, wg_ref, wu_ref, wd_ref, rows_out, back_out, meta_out, got, result, o_acc, d_acc, send_sem, recv_sem, own_sem):
    step = pl.program_id(0)
    n_x = n_ep // 2
    dp, ep = lax.axis_index("dp"), lax.axis_index("ep")
    at = {"x": lax.div(ep, 2), "y": lax.rem(dp, n_y), "z": lax.div(dp, n_y)}
    core = lax.rem(ep, 2)
    sizes = {"x": n_x, "y": n_y, "z": n_z}
    width = wg_ref.shape[0]
    wide = rows_in.shape[2]

    def shifted(axis, by):
        return lax.rem(at[axis] + by + 2 * sizes[axis], sizes[axis])

    def neighbour(axis, by):
        place = {**at, axis: shifted(axis, by)}
        return {"dp": place["z"] * n_y + place["y"], "ep": place["x"] * 2 + core}

    partner = {"dp": dp, "ep": at["x"] * 2 + (1 - core)}
    along_ep = [{"dp": dp, "ep": lax.rem(ep + k, n_ep)} for k in range(1, n_ep)]
    along_y = [{"dp": at["z"] * n_y + lax.rem(at["y"] + k, n_y), "ep": ep} for k in range(1, n_y)]
    along_z = [{"dp": lax.rem(at["z"] + k, n_z) * n_y + at["y"], "ep": ep} for k in range(1, n_z)]
    copies = Copies(send_sem, recv_sem)

    def columns(piece, half):
        low, high = 0, wide
        for part in (PIECES[piece][1], half):
            if part is not None:
                middle = (low + high) // 2
                low, high = ((low, middle), (middle, high))[part]
        return pl.ds(low, high - low)

    def region(piece, phase, index, half):
        tile, _, axes = PIECES[piece]
        pick = {axis: slice(None) if k < phase else index if k == phase else at[axis] for k, axis in enumerate(axes)}
        return rows_out.at[pick["z"], pick["y"], pick["x"], core, tile, :, columns(piece, half)]

    def send(piece, phase, sign, hop):
        axis = PIECES[piece][2][phase]
        half = None if hop < sizes[axis] // 2 else (0 if sign == 1 else 1)

        def ends():
            dst = region(piece, phase, shifted(axis, -sign * (hop - 1)), half)
            src = rows_in.at[PIECES[piece][0], :, columns(piece, half)] if (phase, hop) == (0, 1) else dst
            return src, dst, neighbour(axis, sign)

        copies.start((piece, phase, sign, hop), ends)

    def to_partner(name, block):
        copies.start(("pair", *name), lambda: (block(), block(), partner))

    left = {}

    def arrived(piece, phase, sign, hop):
        axes = PIECES[piece][2]
        copies.wait_recv((piece, phase, sign, hop))
        last = sizes[axes[phase]] // 2
        if hop < last:
            send(piece, phase, sign, hop + 1)
        if phase == 2:
            half = None if hop < last else (0 if sign == 1 else 1)
            to_partner((piece, phase, sign, hop), lambda: region(piece, phase, shifted(axes[phase], -sign * hop), half))
        left[piece, phase] = left.get((piece, phase), 2 * last) - 1
        if not left[piece, phase] and phase == 1:
            to_partner((piece, phase), lambda: region(piece, 2, at[axes[2]], None))
        for other, later in due(left, sizes):
            left[other, later] = 2 * (sizes[PIECES[other][2][later]] // 2)
            for way in (1, -1):
                send(other, later, way, 1)

    def exchange_results(name, src, dst):
        for k, target in enumerate(along_ep):
            copies.start((name, k), lambda target=target: (src.at[target["ep"]], dst.at[ep], target))

    def spread(name, targets, block):
        for k, target in enumerate(targets):
            copies.start((name, k), lambda target=target: (block(), block(), target))

    def all_in(name, n):
        for k in range(n):
            copies.wait_recv((name, k))

    def own_copies():
        return [
            pltpu.make_async_copy(rows_in, rows_out.at[at["z"], at["y"], at["x"], core], own_sem.at[0]),
            pltpu.make_async_copy(send_in.at[ep], got.at[ep], own_sem.at[1]),
            pltpu.make_async_copy(meta_in, meta_out.at[pl.ds(dp * n_ep + ep, 1)], own_sem.at[2])]

    def prologue():
        enter(along_ep + [neighbour("y", 1), neighbour("y", -1), neighbour("z", 1), neighbour("z", -1)] + along_y + along_z)
        mine = own_copies()
        for copy in mine:
            copy.start()
        for piece in range(len(PIECES)):
            left[piece, 0] = 2 * (sizes[PIECES[piece][2][0]] // 2)
            for sign in (1, -1):
                send(piece, 0, sign, 1)
        exchange_results("dispatch", send_in, got)
        for copy in mine:
            copy.wait()
        spread("meta_ep", along_ep, lambda: meta_out.at[pl.ds(dp * n_ep + ep, 1)])

    def ready():
        all_in("dispatch", n_ep - 1)
        all_in("meta_ep", n_ep - 1)
        spread("meta_y", along_y, lambda: meta_out.at[pl.ds(dp * n_ep, n_ep)])

    runs, current = [], []
    for entry in order:
        if entry == "ffn":
            runs.append(current)
            current = []
        else:
            current.append(entry)
    runs.append(current)
    n_ffn = len(runs) - 1

    @pl.when(step == 0)
    def _():
        prologue()
        for hop in runs[0]:
            arrived(*hop)
        ready()
        o_acc[...] = jnp.zeros_like(o_acc)
        d_acc[...] = jnp.zeros_like(d_acc)

    @pl.when(step < n_ffn)
    def _():
        n_row = got.shape[0] * got.shape[1]
        half = wg_ref.shape[1] // 2
        xn = got[:, :, :width].reshape(n_row, width)
        dy = got[:, :, width:].reshape(n_row, width)
        cuts = [slice(0, half), slice(half, 2 * half)]
        mid = [expert_math(dot(xn, wg_ref[:, c], ((1,), (0,))), dot(xn, wu_ref[:, c], ((1,), (0,))), dot(dy, wd_ref[c, :], ((1,), (1,)))) for c in cuts]
        act, d_gate, d_up = (jnp.concatenate(parts, axis=1) for parts in zip(*mid))
        o_acc[...] += dot(act, wd_ref[...], ((1,), (0,)))
        d_acc[...] += dot(d_gate, wg_ref[...], ((1,), (1,))) + dot(d_up, wu_ref[...], ((1,), (1,)))

    @pl.when(step == n_ffn - 1)
    def _():
        result[:, :, :width] = o_acc[...].astype(BF16).reshape(*result.shape[:2], width)
        result[:, :, width:] = d_acc[...].astype(BF16).reshape(*result.shape[:2], width)

    for k in range(1, n_ffn + 1):
        @pl.when(step == (k - 1 if k < n_ffn else n_ffn))
        def _():
            if k == 2:
                all_in("meta_y", n_y - 1)
                spread("meta_z", along_z, lambda: meta_out.at[pl.ds(at["z"] * n_y * n_ep, n_y * n_ep)])
            if k == n_ffn:
                own = pltpu.make_async_copy(result.at[ep], back_out.at[ep], own_sem.at[1])
                own.start()
                own.wait()
                exchange_results("back", result, back_out)
            for hop in runs[k]:
                arrived(*hop)
            if k == n_ffn:
                all_in("meta_z", n_z - 1)
                all_in("back", n_ep - 1)
                for name in copies.made:
                    if name[0] == "pair":
                        copies.wait_recv(name)
                for copy in copies.made.values():
                    copy().wait_send()


def gather_rows(rows, send, meta, wg, wu, wd, n_y, n_z, n_ep, block):
    n_tok, wide = rows.shape
    n_dev = n_y * n_z * n_ep
    capacity = send.shape[1]
    width, ff = wg.shape
    n_ffn = ff // block
    tiles = n_tok // 8
    order, _ = plan({"x": n_ep // 2, "y": n_y, "z": n_z}, 8 * wide * 2, n_ffn)
    n_sem = len([e for e in order if e != "ffn"])
    n_sem += sum(1 for e in order if e != "ffn" and e[1] == 2) + len(PIECES) + 2 * (n_ep - 1) + n_ep + n_y + n_z - 3
    vmem, hbm = pl.BlockSpec(memory_space=pltpu.VMEM), pl.BlockSpec(memory_space=pl.ANY)
    col = pl.BlockSpec((width, block), lambda j: (0, jnp.minimum(j, n_ffn - 1)))
    row = pl.BlockSpec((block, width), lambda j: (jnp.minimum(j, n_ffn - 1), 0))
    slots = pltpu.VMEM((n_ep, capacity, wide), BF16)
    out, back, meta_all = pl.pallas_call(
        functools.partial(gather_kernel, n_y, n_z, n_ep, order),
        grid=(n_ffn + 1,),
        in_specs=[vmem, vmem, vmem, col, col, row],
        out_specs=[hbm, hbm, hbm],
        out_shape=[
            jax.ShapeDtypeStruct((n_z, n_y, n_ep // 2, 2, tiles, 8, wide), BF16),
            jax.ShapeDtypeStruct((n_ep, capacity, wide), BF16),
            jax.ShapeDtypeStruct((n_dev, 1, LANES), F32)],
        scratch_shapes=[slots, slots, pltpu.VMEM((n_ep * capacity, width), F32), pltpu.VMEM((n_ep * capacity, width), F32),
                        pltpu.SemaphoreType.DMA((n_sem,)), pltpu.SemaphoreType.DMA((n_sem,)), pltpu.SemaphoreType.DMA((3,))],
        compiler_params=pltpu.CompilerParams(collective_id=1, has_side_effects=True, dimension_semantics=("arbitrary",), vmem_limit_bytes=50 * 2**20),
        cost_estimate=pl.CostEstimate(flops=12 * n_ep * capacity * width * ff, bytes_accessed=6 * width * ff, transcendentals=0),
        name="gather_rows",
    )(rows.reshape(tiles, 8, wide), send, meta, wg, wu, wd)
    return out.reshape(n_dev * n_tok, wide), back.reshape(n_ep * capacity, wide), meta_all


def reduce_kernel(n_y, n_z, n_ep, in_ref, out_ref, got_ep, got_y, got_z, send_sem, recv_sem):
    dp, ep, y, z, along_ep, along_y, along_z = peers(n_y, n_z, n_ep)
    enter(along_ep + along_y + along_z)
    base = 0
    got_ep[ep] = in_ref[ep]
    exchange(along_ep, lambda k, t: remote(in_ref.at[t["ep"]], got_ep.at[ep], send_sem.at[base + k], recv_sem.at[base + k], t))
    total = got_ep[0]
    for k in range(1, n_ep):
        total = total + got_ep[k]
    got_y[y] = total
    base = len(along_ep)
    exchange(along_y, lambda k, t: remote(got_y.at[y], got_y.at[y], send_sem.at[base + k], recv_sem.at[base + k], t))
    total = got_y[0]
    for k in range(1, n_y):
        total = total + got_y[k]
    got_z[z] = total
    base += len(along_y)
    exchange(along_z, lambda k, t: remote(got_z.at[z], got_z.at[z], send_sem.at[base + k], recv_sem.at[base + k], t))
    total = got_z[0]
    for k in range(1, n_z):
        total = total + got_z[k]
    out_ref[ep] = total
    base += len(along_z)
    exchange(along_ep, lambda k, t: remote(out_ref.at[ep], out_ref.at[ep], send_sem.at[base + k], recv_sem.at[base + k], t))


def reduce_rows(parts, n_y, n_z, n_ep):
    n_sem = 2 * n_ep + n_y + n_z - 4
    chunk = parts.shape[1:]
    return pl.pallas_call(
        functools.partial(reduce_kernel, n_y, n_z, n_ep),
        out_shape=jax.ShapeDtypeStruct(parts.shape, F32),
        in_specs=[pl.BlockSpec(memory_space=pltpu.VMEM)],
        out_specs=pl.BlockSpec(memory_space=pltpu.VMEM),
        scratch_shapes=[pltpu.VMEM((n_ep, *chunk), F32), pltpu.VMEM((n_y, *chunk), F32), pltpu.VMEM((n_z, *chunk), F32), pltpu.SemaphoreType.DMA((n_sem,)), pltpu.SemaphoreType.DMA((n_sem,))],
        compiler_params=pltpu.CompilerParams(collective_id=2, has_side_effects=True),
        name="reduce_rows",
    )(parts)


def pack_kernel(off_ref, rows_ref, pos_ref, gate_ref, xn_out, dp_out, xn_buf, dp_buf, sem):
    g = pl.program_id(0)
    n_group = pl.num_programs(0)
    width = xn_buf.shape[1]
    tile = MOST_PER_GROUP + ALIGN
    off = off_ref[g]
    base = pl.multiple_of(lax.div(off, ALIGN) * ALIGN, ALIGN)
    row_id = lax.broadcasted_iota(jnp.int32, (tile, GROUP), 0) + base
    hit = row_id == pos_ref[0]
    pick = hit.astype(F32).astype(BF16)
    gate = jnp.sum(jnp.where(hit, gate_ref[0], 0.0), axis=1, keepdims=True)
    xn = dot(pick, rows_ref[:, :width], ((1,), (0,))).astype(BF16)
    dp = (dot(pick, rows_ref[:, width:], ((1,), (0,))) * gate).astype(BF16)
    keep = lax.broadcasted_iota(jnp.int32, (ALIGN, width), 0) + base < off
    for buf, new in ((xn_buf, xn), (dp_buf, dp)):
        head = pl.ds(base, ALIGN)
        buf[head, :] = jnp.where(keep, buf[head, :].astype(F32), new[:ALIGN].astype(F32)).astype(BF16)
        buf[pl.ds(pl.multiple_of(base + ALIGN, ALIGN), tile - ALIGN), :] = new[ALIGN:]

    @pl.when(g == n_group - 1)
    def _():
        usual = USUAL_ROWS // TILE
        zeros = jnp.zeros((TILE, width), BF16)
        tail = pl.ds(pl.multiple_of(base + tile, ALIGN), TILE)
        xn_buf[tail, :] = zeros
        dp_buf[tail, :] = zeros
        used = lax.div(off_ref[n_group] + TILE - 1, TILE)

        def clear(t, carry):
            rows = pl.ds(pl.multiple_of(t * TILE, TILE), TILE)
            xn_buf[rows, :] = zeros
            dp_buf[rows, :] = zeros
            return carry

        lax.fori_loop(used, usual, clear, 0)

        def copies(t):
            rows = pl.ds(pl.multiple_of(t * TILE, TILE), TILE)
            return [pltpu.make_async_copy(buf.at[rows], out.at[rows], sem.at[k]) for k, (buf, out) in enumerate(((xn_buf, xn_out), (dp_buf, dp_out)))]

        def begin(t, carry):
            for copy in copies(t):
                copy.start()
            return carry

        def end(t, carry):
            for copy in copies(t):
                copy.wait()
            return carry

        lax.fori_loop(0, jnp.maximum(used, usual), begin, 0)
        lax.fori_loop(0, jnp.maximum(used, usual), end, 0)


def pack_rows(rows, offsets, pos, gates, most):
    total, width = rows.shape[0], rows.shape[1] // 2
    n_group = total // GROUP
    small = pl.BlockSpec((1, 1, GROUP), lambda g, off: (g, 0, 0))
    whole = pl.BlockSpec(memory_space=pl.ANY)
    buf = pltpu.VMEM((max(most, USUAL_ROWS) + 2 * TILE + ALIGN, width), BF16)
    out = jax.ShapeDtypeStruct((max(most, USUAL_ROWS), width), BF16)
    return pl.pallas_call(
        pack_kernel,
        grid_spec=pltpu.PrefetchScalarGridSpec(
            num_scalar_prefetch=1,
            grid=(n_group,),
            in_specs=[pl.BlockSpec((GROUP, 2 * width), lambda g, off: (g, 0)), small, small],
            out_specs=[whole, whole],
            scratch_shapes=[buf, buf, pltpu.SemaphoreType.DMA((2,))],
        ),
        out_shape=[out, out],
        compiler_params=pltpu.CompilerParams(dimension_semantics=("arbitrary",), vmem_limit_bytes=60 * 2**20),
        cost_estimate=pl.CostEstimate(flops=4 * GROUP * total * width, bytes_accessed=4 * total * width, transcendentals=0),
        name="pack_rows",
    )(offsets, rows, pos, gates)


def grads_kernel(n_quarter, info_ref, xn_hbm, dp_hbm, wg_ref, wu_ref, wd_ref, *refs):
    if n_quarter > 1:
        out_ref, xn, xt, dp, act_t, d_gate, d_up, acc_g, acc_u, acc_d, tile_x, tile_p, sem = refs
    else:
        gg_ref, gu_ref, gd_ref, xn, xt, dp, act_t, d_gate, d_up, acc_g, acc_u, acc_d, tile_x, tile_p, sem = refs
    rows, width = xn.shape
    part = width // n_quarter
    low = pl.multiple_of(info_ref[2] * part, part)
    tiles = [slice(r, r + TILE) for r in range(0, rows, TILE)]

    @pl.when(pl.program_id(0) == 0)
    def _():
        copies = [[pltpu.make_async_copy(src.at[pl.ds(t.start, TILE)], dst.at[pl.ds(t.start, TILE)], sem.at[k, i]) for i, t in enumerate(tiles)] for k, (src, dst) in enumerate(((xn_hbm, xn), (dp_hbm, dp)))]
        for copy in copies[0] + copies[1]:
            copy.start()
        for acc in (acc_g, acc_u, acc_d):
            acc[...] = jnp.zeros_like(acc)
        for copy, t in zip(copies[0], tiles):
            copy.wait()
            xt[:, t] = xn[t, pl.ds(low, part)].T
        for copy in copies[1]:
            copy.wait()

    wg, wu, wd = wg_ref[...], wu_ref[...], wd_ref[...]

    def hidden_rows(x, p):
        return expert_math(dot(x, wg, ((1,), (0,))), dot(x, wu, ((1,), (0,))), dot(p, wd, ((1,), (1,))))

    @pl.when(info_ref[0] > rows // TILE)
    def _():
        for acc in (acc_g, acc_u, acc_d):
            acc[...] = jnp.zeros_like(acc)

        def more(t, carry):
            at = pl.ds(pl.multiple_of(t * TILE, TILE), TILE)
            copies = [pltpu.make_async_copy(xn_hbm.at[at], tile_x, sem.at[0, 0]), pltpu.make_async_copy(dp_hbm.at[at], tile_p, sem.at[1, 0])]
            for copy in copies:
                copy.start()
            for copy in copies:
                copy.wait()
            act, dg, du = hidden_rows(tile_x[...], tile_p[...])
            x, p = tile_x[:, pl.ds(low, part)], tile_p[:, pl.ds(low, part)]
            acc_g[...] += dot(x, dg, ((0,), (0,)))
            acc_u[...] += dot(x, du, ((0,), (0,)))
            acc_d[...] += dot(act, p, ((0,), (0,)))
            return carry

        lax.fori_loop(rows // TILE, info_ref[0], more, 0)

    for t in tiles:
        act, d_gate[t, :], d_up[t, :] = hidden_rows(xn[t, :], dp[t, :])
        act_t[:, t] = act.T

    wide = 2 * TILE if part % (2 * TILE) == 0 else TILE
    for c in range(0, part, wide):
        cut = slice(c, c + wide)
        new_g = (dot(xt[cut, :], d_gate[...], ((1,), (0,))) + acc_g[cut, :]).astype(BF16)
        new_u = (dot(xt[cut, :], d_up[...], ((1,), (0,))) + acc_u[cut, :]).astype(BF16)
        if n_quarter > 1:
            out_ref[0, cut, :], out_ref[1, cut, :] = new_g, new_u
        else:
            gg_ref[cut, :], gu_ref[cut, :] = new_g, new_u
    for c in range(0, part, wide):
        cut = slice(c, c + wide)
        if n_quarter > 1:
            new_d = (dot(act_t[...], dp[:, pl.ds(pl.multiple_of(low + c, wide), wide)], ((1,), (0,))) + acc_d[:, cut]).astype(BF16)
            for k in range(0, wide, TILE):
                out_ref[2, slice(c + k, c + k + TILE), :] = new_d[:, k:k + TILE]
        else:
            gd_ref[:, cut] = (dot(act_t[...], dp[:, cut], ((1,), (0,))) + acc_d[:, cut]).astype(BF16)


def expert_grads(info, xn, dp, wg, wu, wd, n_block, n_quarter):
    width, ff = wg.shape
    rows = USUAL_ROWS
    part = width // n_quarter
    hbm = pl.BlockSpec(memory_space=pl.ANY)
    if n_quarter > 1:
        col = pl.BlockSpec((width, TILE), lambda j, info: (0, info[1]))
        row = pl.BlockSpec((TILE, width), lambda j, info: (info[1], 0))
        out_specs = [pl.BlockSpec((3, part, TILE), lambda j, info: (0, 0, 0))]
        outs = [jax.ShapeDtypeStruct((3, part, TILE), BF16)]
    else:
        col = pl.BlockSpec((width, TILE), lambda j, info: (0, j))
        row = pl.BlockSpec((TILE, width), lambda j, info: (j, 0))
        out_specs = [col, col, row]
        outs = [jax.ShapeDtypeStruct((width, ff), BF16)] * 2 + [jax.ShapeDtypeStruct((ff, width), BF16)]
    return pl.pallas_call(
        functools.partial(grads_kernel, n_quarter),
        grid_spec=pltpu.PrefetchScalarGridSpec(
            num_scalar_prefetch=1,
            grid=(n_block,),
            in_specs=[hbm, hbm, col, col, row],
            out_specs=out_specs,
            scratch_shapes=[
                pltpu.VMEM((rows, width), BF16), pltpu.VMEM((part, rows), BF16), pltpu.VMEM((rows, width), BF16),
                pltpu.VMEM((TILE, rows), BF16), pltpu.VMEM((rows, TILE), BF16), pltpu.VMEM((rows, TILE), BF16),
                pltpu.VMEM((part, TILE), F32), pltpu.VMEM((part, TILE), F32), pltpu.VMEM((TILE, part), F32),
                pltpu.VMEM((TILE, width), BF16), pltpu.VMEM((TILE, width), BF16), pltpu.SemaphoreType.DMA((2, rows // TILE))],
        ),
        out_shape=outs,
        compiler_params=pltpu.CompilerParams(dimension_semantics=("arbitrary",), vmem_limit_bytes=63 * 2**20),
        cost_estimate=pl.CostEstimate(flops=12 * rows * width * TILE * n_block, bytes_accessed=12 * width * TILE * n_block, transcendentals=0),
        name="expert_grads" if n_quarter == 1 else "expert_slices",
    )(info, xn, dp, wg, wu, wd)


def place_kernel(slices_ref, gg_in, gu_in, gd_in, gg_ref, gu_ref, gd_ref):
    part = slices_ref.shape[1]
    for q in range(slices_ref.shape[0] // 3):
        rows = slice(q * part, (q + 1) * part)
        gg_ref[rows, :] = slices_ref[3 * q]
        gu_ref[rows, :] = slices_ref[3 * q + 1]
        for k in range(0, part, TILE):
            gd_ref[:, q * part + k:q * part + k + TILE] = slices_ref[3 * q + 2, k:k + TILE, :]


def place_slices(slices, grads, first, n_quarter):
    width, ff = grads[0].shape
    part = width // n_quarter
    hbm = pl.BlockSpec(memory_space=pl.ANY)
    col = pl.BlockSpec((width, TILE), lambda i: (0, first + i))
    row = pl.BlockSpec((TILE, width), lambda i: (first + i, 0))
    return pl.pallas_call(
        place_kernel,
        grid=(slices.shape[0] // (3 * n_quarter),),
        in_specs=[pl.BlockSpec((3 * n_quarter, part, TILE), lambda i: (i, 0, 0)), hbm, hbm, hbm],
        out_specs=[col, col, row],
        out_shape=[jax.ShapeDtypeStruct(g.shape, g.dtype) for g in grads],
        input_output_aliases={1: 0, 2: 1, 3: 2},
        compiler_params=pltpu.CompilerParams(dimension_semantics=("arbitrary",)),
        cost_estimate=pl.CostEstimate(flops=0, bytes_accessed=4 * slices.size, transcendentals=0),
        name="place_slices",
    )(slices, *grads)


def solution(mesh):
    n_ep = mesh.shape["ep"]
    n_dp = mesh.shape["dp"]
    n_y = 4 if n_dp == 32 else 2
    n_z = n_dp // n_y
    n_dev = n_dp * n_ep
    all_axes = ("dp", "ep")

    def local_step(hidden, grad_out, expert_ids, norm_gain, w_router, w_gate, w_up, w_down):
        n_tok, width = hidden.shape
        n_exp = w_router.shape[1]
        capacity = 4 * n_tok // n_exp
        total_tok = n_tok * n_dev
        dest_rows, slot_owner, loads = route_tables(expert_ids, n_exp, capacity)
        choice_hot = (expert_ids[:, :, None] == jnp.arange(n_exp, dtype=jnp.int32)).astype(F32)

        x_f32 = hidden.astype(F32)
        inv_rms = lax.rsqrt(jnp.mean(x_f32 * x_f32, axis=-1, keepdims=True) + EPS)
        x_hat = x_f32 * inv_rms
        x_norm = (x_hat * norm_gain).astype(BF16)
        xn_f32 = x_norm.astype(F32)
        router_probs = jax.nn.softmax(jnp.dot(xn_f32, w_router, preferred_element_type=F32), axis=-1)
        gate_vals = jnp.sum(router_probs[:, None, :] * choice_hot, axis=-1)

        meta = jnp.concatenate([gate_vals.T.reshape(1, -1), expert_ids.T.astype(F32).reshape(1, -1)], axis=1)
        meta = jnp.pad(meta, ((0, 0), (0, LANES - meta.shape[1])))
        dy_f32 = grad_out.astype(F32)
        d_picked = (dy_f32[:, None, :] * gate_vals[:, :, None]).astype(BF16).reshape(n_tok * 2, width)
        send = jnp.concatenate([
            jnp.take(x_norm, slot_owner // 2, axis=0, mode="fill", fill_value=0),
            jnp.take(d_picked, slot_owner, axis=0, mode="fill", fill_value=0)], axis=1)
        wg, wu, wd = w_gate[0], w_up[0], w_down[0]
        rows_all, back, meta_all = gather_rows(jnp.concatenate([x_norm, grad_out], axis=1), send.reshape(n_exp, capacity, 2 * width), meta[None], wg, wu, wd, n_y, n_z, n_ep, 2 * TILE)
        meta_all = meta_all.reshape(n_dev, LANES)
        ids_all = meta_all[:, 2 * n_tok:4 * n_tok].astype(jnp.int32).reshape(n_dev, 2, n_tok)
        gates_all = meta_all[:, :2 * n_tok].reshape(n_dev, 2, n_tok)
        all_loads = jnp.sum((ids_all[..., None] == jnp.arange(n_exp, dtype=jnp.int32)).astype(F32), axis=(0, 1, 2))
        load_frac = all_loads / (2 * total_tok)

        both = jnp.take(back, dest_rows, axis=0).reshape(n_tok, 2, 2 * width)
        picked, d_xn_exp = both[..., :width], both[..., width:]
        out_hidden = (x_f32 + jnp.sum(gate_vals[:, :, None] * picked, axis=1)).astype(BF16)
        d_gates = jnp.sum(dy_f32[:, None, :] * picked, axis=-1)

        d_probs = jnp.sum(d_gates[:, :, None] * choice_hot, axis=1) + (AUX_COEF * n_exp / total_tok) * load_frac
        d_logits = router_probs * (d_probs - jnp.sum(router_probs * d_probs, axis=-1, keepdims=True))
        d_xnorm = jnp.einsum("te,de->td", d_logits, w_router) + d_xn_exp[:, 0].astype(F32) + d_xn_exp[:, 1].astype(F32)
        d_xnorm = d_xnorm.astype(BF16).astype(F32)
        value_a6 = d_xnorm * norm_gain
        grad_hidden = (inv_rms * (value_a6 - x_hat * jnp.mean(value_a6 * x_hat, axis=-1, keepdims=True)) + dy_f32).astype(BF16)

        part_router = jnp.einsum("te,td->ed", d_logits, xn_f32).reshape(-1)
        part_gain = jnp.sum(d_xnorm * x_hat, axis=0)
        flat = jnp.concatenate([part_router, part_gain, jnp.sum(router_probs, axis=0)])
        unit = n_ep * 8 * LANES
        size = -(-flat.shape[0] // unit) * unit
        summed = reduce_rows(jnp.pad(flat, (0, size - flat.shape[0])).reshape(n_ep, -1, LANES), n_y, n_z, n_ep).reshape(-1)
        grad_router = summed[:n_exp * width].reshape(n_exp, width).T
        grad_gain = summed[n_exp * width:(n_exp + 1) * width]
        prob_sum = summed[(n_exp + 1) * width:(n_exp + 1) * width + n_exp]
        aux_loss = AUX_COEF * n_exp * jnp.sum(load_frac * prob_sum / total_tok)

        me = lax.axis_index("ep")
        mine = ids_all == me
        member = jnp.any(mine, axis=1).reshape(-1, GROUP)
        gate_me = jnp.sum(jnp.where(mine, gates_all, 0.0), axis=1).reshape(-1, 1, GROUP)
        rank = jnp.cumsum(member.astype(jnp.int32), axis=1)
        counts = rank[:, -1]
        ends = jnp.cumsum(counts)
        offsets = jnp.concatenate([jnp.zeros((1,), jnp.int32), ends])
        pos = jnp.where(member, offsets[:-1, None] + rank - 1, -(2**24))[:, None]
        pos, gate_me, offsets, grad_router = lax.optimization_barrier((pos, gate_me, offsets, grad_router))
        xn, dp = pack_rows(rows_all, offsets, pos, gate_me, capacity * n_dev)
        n_block = w_gate.shape[2] // TILE
        own = n_block - n_dp // QUARTERS
        place = lax.axis_index("dp")
        info = jnp.stack([(offsets[-1] + TILE - 1) // TILE, own + place // QUARTERS, place % QUARTERS]).astype(jnp.int32)
        slices = expert_grads(info, xn, dp, wg, wu, wd, 1, QUARTERS)[0]
        whole_info = info * jnp.array([1, 0, 0], jnp.int32)
        slices_all = lax.all_gather(slices, "dp", axis=0, tiled=True)
        grads = expert_grads(whole_info, xn, dp, wg, wu, wd, own, 1)
        g_gate, g_up, g_down = (g[None] for g in place_slices(slices_all, grads, own, QUARTERS))
        return out_hidden, aux_loss, grad_hidden, grad_gain, grad_router, g_gate, g_up, g_down

    tok_spec = P(all_axes, None)
    w_spec = P("ep", None, None)
    return jax.shard_map(local_step, mesh=mesh, in_specs=(tok_spec, tok_spec, tok_spec, P(), P(), w_spec, w_spec, w_spec), out_specs=(tok_spec, P(), tok_spec, P(), P(), w_spec, w_spec, w_spec), check_vma=False)
```

```python
import functools
import jax
import jax.numpy as jnp
from jax import lax
from jax.experimental import pallas as pl
from jax.experimental.pallas import tpu as pltpu
from jax.sharding import PartitionSpec as P

EPS = 1e-6
AUX_COEF = 0.001
LANES = 128
GROUP = 256
ALIGN = 16
TILE = 256
FIRST_ROWS = 768
USUAL_ROWS = 2304
QUARTERS = 4
F32 = jnp.float32
BF16 = jnp.bfloat16


def route_tables(expert_ids, n_exp, capacity):
    flat_ids = expert_ids.reshape(-1)
    n_choice = flat_ids.shape[0]
    one_hot = (flat_ids[:, None] == jnp.arange(n_exp, dtype=jnp.int32)[None, :]).astype(jnp.int32)
    running = jnp.cumsum(one_hot, axis=0) - 1
    dest_rows = flat_ids * capacity + jnp.sum(running * one_hot, axis=1)
    slot_owner = jnp.full((n_exp * capacity,), n_choice, jnp.int32).at[dest_rows].set(jnp.arange(n_choice, dtype=jnp.int32))
    return dest_rows, slot_owner, jnp.sum(one_hot, axis=0)


def peers(n_y, n_z, n_ep):
    dp, ep = lax.axis_index("dp"), lax.axis_index("ep")
    y, z = lax.rem(dp, n_y), lax.div(dp, n_y)
    along_ep = [{"dp": dp, "ep": lax.rem(ep + k, n_ep)} for k in range(1, n_ep)]
    along_y = [{"dp": z * n_y + lax.rem(y + k, n_y), "ep": ep} for k in range(1, n_y)]
    along_z = [{"dp": lax.rem(z + k, n_z) * n_y + y, "ep": ep} for k in range(1, n_z)]
    return dp, ep, y, z, along_ep, along_y, along_z


def enter(all_peers):
    barrier = pltpu.get_barrier_semaphore()
    for peer in all_peers:
        pl.semaphore_signal(barrier, inc=1, device_id=peer, device_id_type=pl.DeviceIdType.MESH)
    pl.semaphore_wait(barrier, len(all_peers))


def exchange(targets, make):
    copies = [make(k, target) for k, target in enumerate(targets)]
    for copy in copies:
        copy.start()
    for copy in copies:
        copy.wait()


def remote(src, dst, send_sem, recv_sem, target):
    return pltpu.make_async_remote_copy(src_ref=src, dst_ref=dst, send_sem=send_sem, recv_sem=recv_sem, device_id=target, device_id_type=pl.DeviceIdType.MESH)


def dot(a, b, dims):
    return lax.dot_general(a, b, (dims, ((), ())), preferred_element_type=F32)


def expert_math(hg, hu, da):
    gate = hg.astype(BF16).astype(F32)
    up = hu.astype(BF16).astype(F32)
    d_act = da.astype(BF16).astype(F32)
    sig = jax.nn.sigmoid(gate)
    silu = gate * sig
    act = (silu * up).astype(BF16)
    d_up = (d_act * silu).astype(BF16)
    d_gate = (d_act * up * sig * (1.0 + gate * (1.0 - sig))).astype(BF16)
    return act, d_gate, d_up


LINK_RATE, HOP_US, FFN_US, FFN_FROM_US, STEP_US = 46e3, 3.0, 3.5, 24.0, 5.6
PIECES = (
    (1, 0, None, "xyz"), (0, 0, 0, "zxy"), (0, 0, 1, "zyx"), (0, 1, None, "yzx"), (1, 1, None, "xzy"))
LATE = (0, 4)


def due(left):
    steps = [(piece, phase) for piece in range(len(PIECES)) for phase in (1, 2) if phase == 1 or piece not in LATE]
    return [(piece, phase) for piece, phase in steps if (piece, phase) not in left and left.get((piece, phase - 1)) == 0]


def plan(sizes, tile_bytes, n_ffn):
    free, arrive, order, left = {}, [], [], {}
    tasks = [("ffn", 0.0, FFN_US)] * n_ffn + [("back", 0.0, 0.5), ("final", 12.0, 6.0)] + [(f"sum{k}", 5.0, 0.5) for k in range(4)]
    now, next_at = 8.0, FFN_FROM_US

    def issue(hop, when):
        piece, phase, sign, step = hop
        _, _, half, axes = PIECES[piece]
        size = tile_bytes // (1 if half is None else 2)
        for axis in axes[:phase]:
            size *= sizes[axis]
        size //= 2 if step == sizes[axes[phase]] // 2 else 1
        link = (axes[phase], sign)
        free[link] = max(when, free.get(link, 0.0)) + size / LINK_RATE
        arrive.append((free[link] + HOP_US, hop))

    def begin(piece, phase, when):
        left[piece, phase] = 2 * (sizes[PIECES[piece][3][phase]] // 2)
        for sign in (1, -1):
            issue((piece, phase, sign, 1), when)

    for piece in range(len(PIECES)):
        begin(piece, 0, now)
    while arrive or tasks:
        arrive.sort()
        when, hop = arrive[0] if arrive else (1e9, None)
        if tasks and max(now, next_at) + 0.6 * tasks[0][2] < max(now, when) + (0.0 if arrive else 1e9):
            name, _, lasts = tasks.pop(0)
            order.append(name)
            now = max(now, next_at) + lasts
            next_at = now + (tasks[0][1] if tasks else 0.0)
            continue
        arrive.pop(0)
        now = max(now, when)
        order.append(hop)
        piece, phase, sign, step = hop
        if step < sizes[PIECES[piece][3][phase]] // 2:
            issue((piece, phase, sign, step + 1), now)
        left[piece, phase] -= 1
        for other in due(left):
            begin(*other, now)
    return order, now


class Copies:
    def __init__(self, send_sem, recv_sem):
        self.sems, self.made = (send_sem, recv_sem), {}

    def start(self, name, ends):
        k = len(self.made)
        self.made[name] = lambda: remote(*ends()[:2], self.sems[0].at[k], self.sems[1].at[k], ends()[2])
        self.made[name]().start()

    def wait_recv(self, name):
        self.made[name]().wait_recv()


class Rings:
    def __init__(self, n_y, n_z, n_ep, rows, own, copies):
        self.sizes = {"x": n_ep // 2, "y": n_y, "z": n_z}
        self.dp, self.ep = lax.axis_index("dp"), lax.axis_index("ep")
        self.at = {"x": lax.div(self.ep, 2), "y": lax.rem(self.dp, n_y), "z": lax.div(self.dp, n_y)}
        self.core = lax.rem(self.ep, 2)
        self.rows, self.own, self.copies, self.left = rows, own, copies, {}
        self.partner = {"dp": self.dp, "ep": self.at["x"] * 2 + (1 - self.core)}

    def shifted(self, axis, by):
        return lax.rem(self.at[axis] + by + 2 * self.sizes[axis], self.sizes[axis])

    def neighbour(self, axis, by):
        place = {**self.at, axis: self.shifted(axis, by)}
        return {"dp": place["z"] * self.sizes["y"] + place["y"], "ep": place["x"] * 2 + self.core}

    def columns(self, piece, half):
        low, high = 0, self.rows[1].shape[-1]
        for part in (PIECES[piece][2], half):
            if part is not None:
                middle = (low + high) // 2
                low, high = ((low, middle), (middle, high))[part]
        return pl.ds(low, high - low)

    def region(self, piece, phase, index, half, core=None):
        late, tile, _, axes = PIECES[piece]
        pick = {axis: slice(None) if k < phase else index if k == phase else self.at[axis] for k, axis in enumerate(axes)}
        core = self.core if core is None else core
        return self.rows[late].at[pick["z"], pick["y"], pick["x"], core, tile, :, self.columns(piece, half)]

    def half(self, axis, sign, hop):
        return None if hop < self.sizes[axis] // 2 else (0 if sign == 1 else 1)

    def send(self, piece, phase, sign, hop, before=None):
        late, tile, _, axes = PIECES[piece]
        axis = axes[phase]
        half = self.half(axis, sign, hop)

        def ends():
            dst = self.region(piece, phase, self.shifted(axis, -sign * (hop - 1)), half)
            src = dst
            if (phase, hop) == (0, 1):
                src = self.own.at[2 * late + tile, :, self.columns(piece, half)]
            elif before is not None:
                src = before.region(piece, phase, self.at[axis], half)
            return src, dst, self.neighbour(axis, sign)

        self.copies.start((piece, phase, sign, hop), ends)

    def begin(self, piece, phase, before=None):
        self.left[piece, phase] = 2 * (self.sizes[PIECES[piece][3][phase]] // 2)
        for sign in (1, -1):
            self.send(piece, phase, sign, 1, before)

    def to_partner(self, name, block):
        self.copies.start(("pair", *name), lambda: (block(), block(), self.partner))

    def arrived(self, piece, phase, sign, hop):
        axes = PIECES[piece][3]
        axis = axes[phase]
        self.copies.wait_recv((piece, phase, sign, hop))
        if hop < self.sizes[axis] // 2:
            self.send(piece, phase, sign, hop + 1)
        if phase == 2:
            self.to_partner((piece, phase, sign, hop), lambda: self.region(piece, phase, self.shifted(axis, -sign * hop), self.half(axis, sign, hop)))
        self.left[piece, phase] -= 1
        if not self.left[piece, phase] and phase == 1:
            self.to_partner((piece, phase), lambda: self.region(piece, 2, self.at[axes[2]], None))
        for other, later in due(self.left):
            self.begin(other, later)

    def finish(self):
        for name in self.copies.made:
            if name[0] == "pair":
                self.copies.wait_recv(name)
        for copy in self.copies.made.values():
            copy().wait_send()


def gather_kernel(n_y, n_z, n_ep, order, rows_in, send_in, meta_in, x_ref, tok_ref, gain_ref, router_ref, wg_ref, wu_ref, wd_ref, early_out, late_out, meta_res, y_ref, gh_ref, sum_ref,
                  got, result, back_out, meta_out, parts, got_ep, got_y, got_z, total, o_acc, d_acc, send_sem, recv_sem, own_sem):
    step = pl.program_id(0)
    copies = Copies(send_sem, recv_sem)
    rings = Rings(n_y, n_z, n_ep, (early_out, late_out), rows_in, copies)
    dp, ep, at = rings.dp, rings.ep, rings.at
    width = wg_ref.shape[0]
    wide = rows_in.shape[2]
    along_ep = [{"dp": dp, "ep": lax.rem(ep + k, n_ep)} for k in range(1, n_ep)]
    along_y = [{"dp": at["z"] * n_y + lax.rem(at["y"] + k, n_y), "ep": ep} for k in range(1, n_y)]
    along_z = [{"dp": lax.rem(at["z"] + k, n_z) * n_y + at["y"], "ep": ep} for k in range(1, n_z)]

    def exchange_results(name, src, dst):
        for k, target in enumerate(along_ep):
            copies.start((name, k), lambda target=target: (src.at[target["ep"]], dst.at[ep], target))

    def spread(name, targets, block):
        for k, target in enumerate(targets):
            copies.start((name, k), lambda target=target: (block(), block(), target))

    def all_in(name, n):
        for k in range(n):
            copies.wait_recv((name, k))

    def own_copies():
        return [
            pltpu.make_async_copy(rows_in.at[pl.ds(0, 2)], early_out.at[at["z"], at["y"], at["x"], rings.core], own_sem.at[0]),
            pltpu.make_async_copy(rows_in.at[pl.ds(2, 2)], late_out.at[at["z"], at["y"], at["x"], rings.core], own_sem.at[3]),
            pltpu.make_async_copy(send_in.at[ep], got.at[ep], own_sem.at[1]),
            pltpu.make_async_copy(meta_in, meta_out.at[pl.ds(dp * n_ep + ep, 1)], own_sem.at[2])]

    def prologue():
        enter(along_ep + along_y + along_z)
        mine = own_copies()
        for copy in mine:
            copy.start()
        for piece in range(len(PIECES)):
            rings.begin(piece, 0)
        exchange_results("dispatch", send_in, got)
        for copy in mine:
            copy.wait()
        spread("meta_ep", along_ep, lambda: meta_out.at[pl.ds(dp * n_ep + ep, 1)])

    def ready():
        all_in("dispatch", n_ep - 1)
        all_in("meta_ep", n_ep - 1)
        spread("meta_y", along_y, lambda: meta_out.at[pl.ds(dp * n_ep, n_ep)])

    def finish_tokens():
        all_in("back", n_ep - 1)
        all_in("meta_z", n_z - 1)
        n_tok = x_ref.shape[0]
        n_slot = got.shape[0] * got.shape[1]
        tok = tok_ref[...]
        probs, inv = tok[:, :n_ep], tok[:, n_ep:n_ep + 1]
        gates, slots, experts = ([tok[:, n_ep + k:n_ep + k + 1] for k in (first, first + 1)] for first in (1, 3, 5))
        slot_id = lax.broadcasted_iota(jnp.int32, (n_tok, n_slot), 1).astype(F32)
        expert_id = lax.broadcasted_iota(jnp.int32, (n_tok, n_ep), 1).astype(F32)
        picks = [(slot_id == slot).astype(F32).astype(BF16) for slot in slots]
        hots = [(expert_id == expert).astype(F32) for expert in experts]
        back = back_out[...].reshape(n_slot, wide)
        picked = [dot(pick, back[:, :width], ((1,), (0,))) for pick in picks]
        d_picks = [dot(pick, back[:, width:], ((1,), (0,))) for pick in picks]
        x = x_ref[...].astype(F32)
        x_hat = x * inv
        xn = rows_in[:, :, :width].reshape(n_tok, width).astype(F32)
        dy = rows_in[:, :, width:].reshape(n_tok, width).astype(F32)
        ids = meta_out[...]
        lane = lax.broadcasted_iota(jnp.int32, (1, 1, LANES), 2)
        is_id = jnp.logical_and(lane >= 2 * n_tok, lane < 4 * n_tok)
        expert_lane = lax.broadcasted_iota(jnp.int32, (1, n_ep), 1)
        load_frac = jnp.zeros((1, n_ep), F32)
        for e in range(n_ep):
            named = jnp.sum(jnp.where(jnp.logical_and(is_id, ids == float(e)), 1.0, 0.0), axis=0)
            load_frac += jnp.where(expert_lane == e, jnp.sum(named, axis=1, keepdims=True), 0.0)
        total_tok = n_tok * ids.shape[0]
        load_frac = load_frac / (2 * total_tok)
        d_probs = (AUX_COEF * n_ep / total_tok) * load_frac
        for hot, pick in zip(hots, picked):
            d_probs = d_probs + hot * jnp.sum(dy * pick, axis=1, keepdims=True)
        d_logits = probs * (d_probs - jnp.sum(probs * d_probs, axis=1, keepdims=True))
        d_xn = d_picks[0] + d_picks[1]
        for e in range(n_ep):
            d_xn = d_xn + d_logits[:, e:e + 1] * router_ref[e:e + 1, :]
        d_xn = d_xn.astype(BF16).astype(F32)
        d_gain = jnp.sum(d_xn * x_hat, axis=0, keepdims=True)
        d_probs_sum = jnp.sum(tok, axis=0, keepdims=True)
        share = width // n_ep
        for e in range(n_ep):
            parts[e, :, :width] = jnp.sum(d_logits[:, e:e + 1] * xn, axis=0, keepdims=True)
            parts[e, :, width:width + share] = d_gain[:, e * share:(e + 1) * share]
            parts[e, :, width + share:] = d_probs_sum
        y_ref[...] = (x + (gates[0] * picked[0] + gates[1] * picked[1])).astype(BF16)
        scaled = d_xn * gain_ref[...]
        gh_ref[...] = (inv * (scaled - x_hat * jnp.mean(scaled * x_hat, axis=1, keepdims=True)) + dy).astype(BF16)
        got_ep[ep] = parts[ep]
        exchange_results("sum0", parts, got_ep)

    def added(ref, n):
        value = ref[0]
        for k in range(1, n):
            value = value + ref[k]
        return value

    def sum_up(stage):
        if stage == 0:
            all_in("sum0", n_ep - 1)
            got_y[at["y"]] = added(got_ep, n_ep)
            spread("sum1", along_y, lambda: got_y.at[at["y"]])
        if stage == 1:
            all_in("sum1", n_y - 1)
            got_z[at["z"]] = added(got_y, n_y)
            spread("sum2", along_z, lambda: got_z.at[at["z"]])
        if stage == 2:
            all_in("sum2", n_z - 1)
            total[ep] = added(got_z, n_z)
            spread("sum3", along_ep, lambda: total.at[ep])
        if stage == 3:
            all_in("sum3", n_ep - 1)
            sum_ref[...] = total[...]

    runs, current = [], []
    for entry in order:
        if entry == "ffn":
            runs.append(current)
            current = []
        else:
            current.append(entry)
    runs.append(current)
    n_ffn = len(runs) - 1

    @pl.when(step == 0)
    def _():
        prologue()
        for hop in runs[0]:
            rings.arrived(*hop)
        ready()
        o_acc[...] = jnp.zeros_like(o_acc)
        d_acc[...] = jnp.zeros_like(d_acc)

    @pl.when(step < n_ffn)
    def _():
        n_row = got.shape[0] * got.shape[1]
        half = wg_ref.shape[1] // 2
        xn = got[:, :, :width].reshape(n_row, width)
        dy = got[:, :, width:].reshape(n_row, width)
        cuts = [slice(0, half), slice(half, 2 * half)]
        mid = [expert_math(dot(xn, wg_ref[:, c], ((1,), (0,))), dot(xn, wu_ref[:, c], ((1,), (0,))), dot(dy, wd_ref[c, :], ((1,), (1,)))) for c in cuts]
        act, d_gate, d_up = (jnp.concatenate(parts, axis=1) for parts in zip(*mid))
        o_acc[...] += dot(act, wd_ref[...], ((1,), (0,)))
        d_acc[...] += dot(d_gate, wg_ref[...], ((1,), (1,))) + dot(d_up, wu_ref[...], ((1,), (1,)))

    @pl.when(step == n_ffn - 1)
    def _():
        result[:, :, :width] = o_acc[...].astype(BF16).reshape(*result.shape[:2], width)
        result[:, :, width:] = d_acc[...].astype(BF16).reshape(*result.shape[:2], width)

    for k in range(1, n_ffn):
        @pl.when(step == k - 1)
        def _():
            if k == 2:
                all_in("meta_y", n_y - 1)
                spread("meta_z", along_z, lambda: meta_out.at[pl.ds(at["z"] * n_y * n_ep, n_y * n_ep)])
            for hop in runs[k]:
                rings.arrived(*hop)

    @pl.when(step == n_ffn)
    def _():
        for entry in runs[n_ffn]:
            if entry == "back":
                back_out[ep] = result[ep]
                exchange_results("back", result, back_out)
            elif entry == "final":
                finish_tokens()
            elif entry[:3] == "sum":
                sum_up(int(entry[3:]))
            else:
                rings.arrived(*entry)
        meta_res[...] = meta_out[...]
        rings.finish()


def gather_rows(rows, send, meta, x, tok, gain, router, wg, wu, wd, n_y, n_z, n_ep, block):
    n_tok, wide = rows.shape
    n_dev = n_y * n_z * n_ep
    capacity = send.shape[1]
    width, ff = wg.shape
    n_ffn = ff // block
    tiles = n_tok // 8
    order, _ = plan({"x": n_ep // 2, "y": n_y, "z": n_z}, 8 * wide * 2, n_ffn)
    hops = [e for e in order if not isinstance(e, str)]
    n_sem = len(hops) + sum(1 for e in hops if e[1] == 2) + len(PIECES)
    n_sem += 5 * (n_ep - 1) + 2 * (n_y - 1) + 2 * (n_z - 1)
    vmem, hbm = pl.BlockSpec(memory_space=pltpu.VMEM), pl.BlockSpec(memory_space=pl.ANY)
    col = pl.BlockSpec((width, block), lambda j: (0, jnp.minimum(j, n_ffn - 1)))
    row = pl.BlockSpec((block, width), lambda j: (jnp.minimum(j, n_ffn - 1), 0))
    slots = pltpu.VMEM((n_ep, capacity, wide), BF16)
    long = width + width // n_ep + LANES
    rows_type = jax.ShapeDtypeStruct((n_z, n_y, n_ep // 2, 2, tiles // 2, 8, wide), BF16)
    early, late, meta_all, y, gh, sums = pl.pallas_call(
        functools.partial(gather_kernel, n_y, n_z, n_ep, order),
        grid=(n_ffn + 1,),
        in_specs=[vmem] * 7 + [col, col, row],
        out_specs=[hbm] * 2 + [vmem] * 4,
        out_shape=[
            rows_type, rows_type,
            jax.ShapeDtypeStruct((n_dev, 1, LANES), F32),
            jax.ShapeDtypeStruct((n_tok, width), BF16),
            jax.ShapeDtypeStruct((n_tok, width), BF16),
            jax.ShapeDtypeStruct((n_ep, 1, long), F32)],
        scratch_shapes=[
            slots, slots, slots, pltpu.VMEM((n_dev, 1, LANES), F32),
            *(pltpu.VMEM((n, 1, long), F32) for n in (n_ep, n_ep, n_y, n_z, n_ep)),
            pltpu.VMEM((n_ep * capacity, width), F32), pltpu.VMEM((n_ep * capacity, width), F32),
            pltpu.SemaphoreType.DMA((n_sem,)), pltpu.SemaphoreType.DMA((n_sem,)), pltpu.SemaphoreType.DMA((4,))],
        compiler_params=pltpu.CompilerParams(collective_id=1, has_side_effects=True, dimension_semantics=("arbitrary",), vmem_limit_bytes=56 * 2**20),
        cost_estimate=pl.CostEstimate(flops=12 * n_ep * capacity * width * ff, bytes_accessed=6 * width * ff, transcendentals=0),
        name="gather_rows",
    )(rows.reshape(tiles, 8, wide), send, meta, x, tok, gain, router, wg, wu, wd)
    return early.reshape(-1, wide), late, meta_all, y, gh, sums


def at_tile(t):
    return pl.ds(pl.multiple_of(t * TILE, TILE), TILE)


def each(low, high, do):
    def body(t, carry):
        do(t)
        return carry

    lax.fori_loop(low, high, body, 0)


def select_rows(off, rows_ref, pos_ref, gate_ref, xn_buf, dp_buf):
    width = xn_buf.shape[1]
    tile = GROUP + ALIGN
    base = pl.multiple_of(lax.div(off, ALIGN) * ALIGN, ALIGN)
    hit = lax.broadcasted_iota(jnp.int32, (tile, GROUP), 0) + base == pos_ref[0]
    pick = hit.astype(F32).astype(BF16)
    gate = jnp.sum(jnp.where(hit, gate_ref[0], 0.0), axis=1, keepdims=True)
    head, rest = pl.ds(base, ALIGN), pl.ds(pl.multiple_of(base + ALIGN, ALIGN), GROUP)
    wide = min(2 * TILE, width)
    keep = lax.broadcasted_iota(jnp.int32, (ALIGN, wide), 0) + base < off
    for buf, low, scale in ((xn_buf, 0, None), (dp_buf, width, gate)):
        for c in range(0, width, wide):
            cut = slice(c, c + wide)
            new = dot(pick, rows_ref[:, low + c:low + c + wide], ((1,), (0,)))
            new = (new if scale is None else new * scale).astype(BF16)
            buf[head, cut] = jnp.where(keep, buf[head, cut].astype(F32), new[:ALIGN].astype(F32)).astype(BF16)
            buf[rest, cut] = new[ALIGN:]
    return pl.multiple_of(base + tile, ALIGN)


def fill_tiles(end, used, least, xn_buf, dp_buf):
    zeros = jnp.zeros((TILE, xn_buf.shape[1]), BF16)
    for buf in (xn_buf, dp_buf):
        buf[pl.ds(end, TILE), :] = zeros

    def clear(t):
        for buf in (xn_buf, dp_buf):
            buf[at_tile(t), :] = zeros

    each(used, least, clear)


def tile_copies(pairs, sem):
    return lambda t: [pltpu.make_async_copy(src.at[at_tile(t)], dst.at[at_tile(t)], sem.at[k]) for k, (src, dst) in enumerate(pairs)]


def start_all(copies):
    return lambda t: [copy.start() for copy in copies(t)] and None


def wait_all(copies):
    return lambda t: [copy.wait() for copy in copies(t)] and None


def hidden_rows(x, p, wg, wu, wd):
    return expert_math(dot(x, wg, ((1,), (0,))), dot(x, wu, ((1,), (0,))), dot(p, wd, ((1,), (1,))))


def early_kernel(info_ref, off_ref, rows_ref, pos_ref, gate_ref, xn_out, dp_out, xt_out, pt_out, xn_buf, dp_buf, xt, pt, sem):
    g = pl.program_id(0)
    end = select_rows(off_ref[g], rows_ref, pos_ref, gate_ref, xn_buf, dp_buf)

    @pl.when(g == pl.num_programs(0) - 1)
    def _():
        first = FIRST_ROWS // TILE
        fill_tiles(end, info_ref[0], first, xn_buf, dp_buf)

        def turn(t):
            xt[:, at_tile(t)] = xn_buf[at_tile(t), :].T
            pt[:, at_tile(t)] = dp_buf[at_tile(t), :].T

        each(0, first, turn)
        copies = tile_copies(((xn_buf, xn_out), (dp_buf, dp_out)), sem)
        each(0, jnp.maximum(info_ref[0], first), start_all(copies))
        turned = [pltpu.make_async_copy(xt, xt_out, sem.at[2]), pltpu.make_async_copy(pt, pt_out, sem.at[3])]
        for copy in turned:
            copy.start()
        each(0, jnp.maximum(info_ref[0], first), wait_all(copies))
        for copy in turned:
            copy.wait()


def late_kernel(n_quarter, info_ref, off_ref, rows_ref, pos_ref, gate_ref, wg_ref, wu_ref, wd_ref, xn_in, dp_in, xn_out, dp_out, slice_ref, xn_buf, dp_buf, acc_g, acc_u, acc_d, sem):
    g = pl.program_id(0)
    first = FIRST_ROWS // TILE

    @pl.when(g == 0)
    def _():
        copies = tile_copies(((xn_in, xn_buf), (dp_in, dp_buf)), sem)
        each(0, jnp.maximum(info_ref[3], first), start_all(copies))
        each(0, jnp.maximum(info_ref[3], first), wait_all(copies))

    end = select_rows(off_ref[g], rows_ref, pos_ref, gate_ref, xn_buf, dp_buf)

    @pl.when(g == pl.num_programs(0) - 1)
    def _():
        width = xn_buf.shape[1]
        usual, used = USUAL_ROWS // TILE, info_ref[0]
        fill_tiles(end, used, usual, xn_buf, dp_buf)
        part = width // n_quarter
        quarter = pl.ds(pl.multiple_of(info_ref[2] * part, part), part)
        wg, wu, wd = wg_ref[...], wu_ref[...], wd_ref[...]
        for acc in (acc_g, acc_u, acc_d):
            acc[...] = jnp.zeros_like(acc)

        copies = tile_copies(((xn_buf, xn_out), (dp_buf, dp_out)), sem)

        def add(t):
            act, dg, du = hidden_rows(xn_buf[at_tile(t), :], dp_buf[at_tile(t), :], wg, wu, wd)
            acc_g[...] += dot(xn_buf[at_tile(t), quarter], dg, ((0,), (0,)))
            acc_u[...] += dot(xn_buf[at_tile(t), quarter], du, ((0,), (0,)))
            acc_d[...] += dot(act, dp_buf[at_tile(t), quarter], ((0,), (0,)))

            @pl.when(t == 1)
            def _():
                each(first, jnp.maximum(used, usual), start_all(copies))

        each(0, jnp.maximum(used, 2), add)
        slice_ref[0] = acc_g[...].astype(BF16)
        slice_ref[1] = acc_u[...].astype(BF16)
        for k in range(0, part, TILE):
            slice_ref[2, k:k + TILE, :] = acc_d[:, k:k + TILE].astype(BF16)
        each(first, jnp.maximum(used, usual), wait_all(copies))


def pack_early(info, rows, offsets, pos, gates, most):
    total, width = rows.shape[0], rows.shape[1] // 2
    small = pl.BlockSpec((1, 1, GROUP), lambda g, info, off: (g, 0, 0))
    whole = pl.BlockSpec(memory_space=pl.ANY)
    buf = pltpu.VMEM((max(most, FIRST_ROWS) + 2 * TILE + ALIGN, width), BF16)
    return pl.pallas_call(
        early_kernel,
        grid_spec=pltpu.PrefetchScalarGridSpec(
            num_scalar_prefetch=2,
            grid=(total // GROUP,),
            in_specs=[pl.BlockSpec((GROUP, 2 * width), lambda g, info, off: (g, 0)), small, small],
            out_specs=[whole] * 4,
            scratch_shapes=[buf, buf, pltpu.VMEM((width, FIRST_ROWS), BF16), pltpu.VMEM((width, FIRST_ROWS), BF16), pltpu.SemaphoreType.DMA((4,))],
        ),
        out_shape=[jax.ShapeDtypeStruct((max(most, FIRST_ROWS), width), BF16)] * 2 + [jax.ShapeDtypeStruct((width, FIRST_ROWS), BF16)] * 2,
        compiler_params=pltpu.CompilerParams(dimension_semantics=("arbitrary",), vmem_limit_bytes=63 * 2**20),
        cost_estimate=pl.CostEstimate(flops=4 * GROUP * total * width, bytes_accessed=4 * total * width, transcendentals=0),
        name="pack_early",
    )(info, offsets, rows, pos, gates)


def pack_late(info, rows, offsets, pos, gates, wg, wu, wd, xn, dp, most, n_quarter):
    total, width = rows.shape[0], rows.shape[1] // 2
    usual, part = USUAL_ROWS, width // n_quarter
    small = pl.BlockSpec((1, 1, GROUP), lambda g, info, off: (g, 0, 0))
    once = pl.Buffered(1)
    col = pl.BlockSpec((width, TILE), lambda g, info, off: (0, info[1]), pipeline_mode=once)
    row = pl.BlockSpec((TILE, width), lambda g, info, off: (info[1], 0), pipeline_mode=once)
    whole = pl.BlockSpec(memory_space=pl.ANY)
    buf = pltpu.VMEM((max(most, usual) + 2 * TILE + ALIGN, width), BF16)
    out = jax.ShapeDtypeStruct((max(most, usual), width), BF16)
    return pl.pallas_call(
        functools.partial(late_kernel, n_quarter),
        grid_spec=pltpu.PrefetchScalarGridSpec(
            num_scalar_prefetch=2,
            grid=(total // GROUP,),
            in_specs=[pl.BlockSpec((GROUP, 2 * width), lambda g, info, off: (g, 0)), small, small, col, col, row, whole, whole],
            out_specs=[whole, whole, pl.BlockSpec((3, part, TILE), lambda g, info, off: (0, 0, 0))],
            scratch_shapes=[
                buf, buf, pltpu.VMEM((part, TILE), F32), pltpu.VMEM((part, TILE), F32), pltpu.VMEM((TILE, part), F32), pltpu.SemaphoreType.DMA((2,))],
        ),
        out_shape=[out, out, jax.ShapeDtypeStruct((3, part, TILE), BF16)],
        compiler_params=pltpu.CompilerParams(dimension_semantics=("arbitrary",), vmem_limit_bytes=67043328),
        cost_estimate=pl.CostEstimate(flops=4 * GROUP * total * width, bytes_accessed=4 * total * width, transcendentals=0),
        name="pack_late",
    )(info, offsets, rows, pos, gates, wg, wu, wd, xn, dp)


def load_rows(first, xn_hbm, dp_hbm, xn, xt, dp, sem):
    n = xn.shape[0] // TILE

    def copies(t):
        return [pltpu.make_async_copy(src.at[at_tile(first + t)], dst.at[at_tile(t)], sem.at[k, t]) for k, (src, dst) in enumerate(((xn_hbm, xn), (dp_hbm, dp)))]

    def end(t):
        wait_all(copies)(t)
        xt[:, at_tile(t)] = xn[at_tile(t), :].T

    each(0, n, start_all(copies))
    each(0, n, end)


def block_grads(xn, xt, dp, acts, d_gate, d_up, wg, wu, wd, put):
    rows, width = xn.shape
    n_tile = rows // TILE
    unroll = 2 if n_tile % 2 == 0 else 1

    def forward(trip):
        for k in range(unroll):
            t = at_tile(trip * unroll + k)
            act, d_gate[t, :], d_up[t, :] = hidden_rows(xn[t, :], dp[t, :], wg, wu, wd)
            acts[:, t] = act.T

    each(0, n_tile // unroll, forward)
    wide = min(2 * TILE, width)
    for c in range(0, width, wide):
        cut = slice(c, c + wide)
        put(0, cut, dot(xt[cut, :], d_gate[...], ((1,), (0,))))
        put(1, cut, dot(xt[cut, :], d_up[...], ((1,), (0,))))
    for c in range(0, width, wide):
        cut = slice(c, c + wide)
        put(2, cut, dot(acts[...], dp[:, cut], ((1,), (0,))))


def first_kernel(n_y, n_z, n_ep, order, xn_hbm, xt_hbm, dp_hbm, pt_hbm, wg_ref, wu_ref, wd_ref, late_in, gg_ref, gu_ref, gd_ref, late_out, xn, xt, dp, pt, acts, d_gate, d_up, stage_a, stage_b, sem, send_sem, recv_sem):
    step = pl.program_id(0)
    copies = Copies(send_sem, recv_sem)
    before, rings = (Rings(n_y, n_z, n_ep, (None, late), None, copies) for late in (late_in, late_out))
    ends = [(piece, PIECES[piece][3][2]) for piece in LATE]

    def here(out):
        made = []
        for n, (piece, axis) in enumerate(ends):
            for k, core in enumerate((rings.core, 1 - rings.core)):
                block = (rings if out else before).region(piece, 2, rings.at[axis], None, core)
                staged, done = (stage_a, stage_b)[n].at[k], sem.at[4 + 2 * n + k]
                made.append(pltpu.make_async_copy(staged, block, done) if out else pltpu.make_async_copy(block, staged, done))
        return made

    @pl.when(step == 0)
    def _():
        enter([rings.neighbour(axis, by) for _, axis in ends for by in (1, -1)] + [rings.partner])
        for piece, _ in ends:
            rings.begin(piece, 2, before)
        first = pl.ds(0, xn.shape[0])
        loads = [pltpu.make_async_copy(src, dst, sem.at[k]) for k, (src, dst) in enumerate(((xn_hbm.at[first], xn), (xt_hbm, xt), (dp_hbm.at[first], dp), (pt_hbm, pt)))]
        loads += here(False)
        for copy in loads:
            copy.start()
        for copy in loads:
            copy.wait()
        for copy in here(True):
            copy.start()

    for k, hops in enumerate(order[:-1]):
        if hops:
            @pl.when(step == k)
            def _():
                for hop in hops:
                    rings.arrived(*hop)

    wg, wu, wd = wg_ref[...], wu_ref[...], wd_ref[...]
    rows, width = xn.shape
    for r in range(0, rows, TILE):
        t = slice(r, r + TILE)
        acts[t, :], d_gate[t, :], d_up[t, :] = hidden_rows(xn[t, :], dp[t, :], wg, wu, wd)
    wide = min(2 * TILE, width)
    for c in range(0, width, wide):
        cut = slice(c, c + wide)
        gg_ref[0, cut, :] = dot(xt[cut, :], d_gate[...], ((1,), (0,)))
        gu_ref[0, cut, :] = dot(xt[cut, :], d_up[...], ((1,), (0,)))
        gd_ref[0, cut, :] = dot(pt[cut, :], acts[...], ((1,), (0,)))

    @pl.when(step == pl.num_programs(0) - 1)
    def _():
        for hop in order[-1]:
            rings.arrived(*hop)
        for copy in here(True):
            copy.wait()
        rings.finish()


def late_order(sizes, tile_bytes, n_step):
    order = [[] for _ in range(n_step + 1)]
    for piece in LATE:
        axes = PIECES[piece][3]
        size = tile_bytes * sizes[axes[0]] * sizes[axes[1]]
        n_hop = sizes[axes[2]] // 2
        for hop in range(1, n_hop + 1):
            when = hop * (size / LINK_RATE + HOP_US) - (size / LINK_RATE / 2 if hop == n_hop else 0.0)
            step = min(int(when / STEP_US) + 1, n_step)
            order[step] += [(piece, 2, sign, hop) for sign in (1, -1)]
    return order


def first_grads(xn, xt, dp, pt, wg, wu, wd, late, n_block, n_y, n_z, n_ep):
    width = wg.shape[0]
    rows = FIRST_ROWS
    wide = late.shape[-1]
    order = late_order({"x": n_ep // 2, "y": n_y, "z": n_z}, 8 * wide * 2, n_block)
    n_sem = 2 * sum(len(hops) for hops in order)
    hbm = pl.BlockSpec(memory_space=pl.ANY)
    col = pl.BlockSpec((width, TILE), lambda j: (0, j))
    row = pl.BlockSpec((TILE, width), lambda j: (j, 0))
    col_part = pl.BlockSpec((1, width, TILE), lambda j: (j, 0, 0))
    return pl.pallas_call(
        functools.partial(first_kernel, n_y, n_z, n_ep, order),
        grid=(n_block,),
        in_specs=[hbm, hbm, hbm, hbm, col, col, row, hbm],
        out_specs=[col_part, col_part, col_part, hbm],
        out_shape=[jax.ShapeDtypeStruct((n_block, width, TILE), F32)] * 3 + [jax.ShapeDtypeStruct(late.shape, BF16)],
        scratch_shapes=[
            pltpu.VMEM((rows, width), BF16), pltpu.VMEM((width, rows), BF16), pltpu.VMEM((rows, width), BF16), pltpu.VMEM((width, rows), BF16),
            pltpu.VMEM((rows, TILE), BF16), pltpu.VMEM((rows, TILE), BF16), pltpu.VMEM((rows, TILE), BF16),
            *(pltpu.VMEM((2, *sides, 8, wide), BF16) for sides in ((n_y, n_ep // 2), (n_z, n_ep // 2))), pltpu.SemaphoreType.DMA((4 + 2 * len(LATE),)), pltpu.SemaphoreType.DMA((n_sem,)), pltpu.SemaphoreType.DMA((n_sem,))],
        compiler_params=pltpu.CompilerParams(collective_id=2, has_side_effects=True, dimension_semantics=("arbitrary",), vmem_limit_bytes=56 * 2**20),
        cost_estimate=pl.CostEstimate(flops=12 * rows * width * TILE * n_block, bytes_accessed=18 * width * TILE * n_block, transcendentals=0),
        name="first_grads",
    )(xn, xt, dp, pt, wg, wu, wd, late)


def last_kernel(info_ref, xn_hbm, dp_hbm, wg_ref, wu_ref, wd_ref, pg_ref, pu_ref, pd_ref, gg_ref, gu_ref, gd_ref, xn, xt, dp, act_t, d_gate, d_up, acc_g, acc_u, acc_d, tile_x, tile_p, sem):
    rows, width = xn.shape
    first, usual = FIRST_ROWS // TILE, USUAL_ROWS // TILE
    accs = (acc_g, acc_u, acc_d)

    @pl.when(pl.program_id(0) == 0)
    def _():
        for acc in accs:
            acc[...] = jnp.zeros_like(acc)
        load_rows(first, xn_hbm, dp_hbm, xn, xt, dp, sem)

    wg, wu, wd = wg_ref[...], wu_ref[...], wd_ref[...]

    @pl.when(info_ref[0] > usual)
    def _():
        for acc in accs:
            acc[...] = jnp.zeros_like(acc)

        def more(t):
            copies = [pltpu.make_async_copy(xn_hbm.at[at_tile(t)], tile_x, sem.at[0, 0]), pltpu.make_async_copy(dp_hbm.at[at_tile(t)], tile_p, sem.at[1, 0])]
            for copy in copies:
                copy.start()
            for copy in copies:
                copy.wait()
            act, d_gate[:TILE, :], d_up[:TILE, :] = hidden_rows(tile_x[...], tile_p[...], wg, wu, wd)
            act_t[:, :TILE] = act.T

            def part(c):
                cut = at_tile(c)
                acc_g[cut, :] += dot(tile_x[:, cut], d_gate[:TILE, :], ((0,), (0,)))
                acc_u[cut, :] += dot(tile_x[:, cut], d_up[:TILE, :], ((0,), (0,)))
                acc_d[:, cut] += dot(act_t[:, :TILE], tile_p[:, cut], ((1,), (0,)))

            each(0, width // TILE, part)

        each(usual, info_ref[0], more)

    def put(k, cut, value):
        if k < 2:
            (gg_ref, gu_ref)[k][cut, :] = (value + (pg_ref, pu_ref)[k][0, cut, :] + accs[k][cut, :]).astype(BF16)
        else:
            gd_ref[:, cut] = (value + pd_ref[0, cut, :].T + acc_d[:, cut]).astype(BF16)

    block_grads(xn, xt, dp, act_t, d_gate, d_up, wg, wu, wd, put)


def last_grads(info, xn, dp, wg, wu, wd, parts):
    width, ff = wg.shape
    rows = USUAL_ROWS - FIRST_ROWS
    n_block = parts[0].shape[0]
    hbm = pl.BlockSpec(memory_space=pl.ANY)
    col = pl.BlockSpec((width, TILE), lambda j, info: (0, j))
    row = pl.BlockSpec((TILE, width), lambda j, info: (j, 0))
    col_part = pl.BlockSpec((1, width, TILE), lambda j, info: (j, 0, 0))
    return pl.pallas_call(
        last_kernel,
        grid_spec=pltpu.PrefetchScalarGridSpec(
            num_scalar_prefetch=1,
            grid=(n_block,),
            in_specs=[hbm, hbm, col, col, row, col_part, col_part, col_part],
            out_specs=[col, col, row],
            scratch_shapes=[
                pltpu.VMEM((rows, width), BF16), pltpu.VMEM((width, rows), BF16), pltpu.VMEM((rows, width), BF16),
                pltpu.VMEM((TILE, rows), BF16), pltpu.VMEM((rows, TILE), BF16), pltpu.VMEM((rows, TILE), BF16),
                pltpu.VMEM((width, TILE), F32), pltpu.VMEM((width, TILE), F32), pltpu.VMEM((TILE, width), F32),
                pltpu.VMEM((TILE, width), BF16), pltpu.VMEM((TILE, width), BF16), pltpu.SemaphoreType.DMA((2, rows // TILE))],
        ),
        out_shape=[jax.ShapeDtypeStruct((width, ff), BF16)] * 2 + [jax.ShapeDtypeStruct((ff, width), BF16)],
        compiler_params=pltpu.CompilerParams(dimension_semantics=("arbitrary",), vmem_limit_bytes=63 * 2**20),
        cost_estimate=pl.CostEstimate(flops=12 * rows * width * TILE * n_block, bytes_accessed=24 * width * TILE * n_block, transcendentals=0),
        name="last_grads",
    )(info, xn, dp, wg, wu, wd, *parts)


def place_kernel(slices_ref, gg_in, gu_in, gd_in, gg_ref, gu_ref, gd_ref):
    part = slices_ref.shape[1]
    for q in range(slices_ref.shape[0] // 3):
        rows = slice(q * part, (q + 1) * part)
        gg_ref[rows, :] = slices_ref[3 * q]
        gu_ref[rows, :] = slices_ref[3 * q + 1]
        for k in range(0, part, TILE):
            gd_ref[:, q * part + k:q * part + k + TILE] = slices_ref[3 * q + 2, k:k + TILE, :]


def place_slices(slices, grads, first, n_quarter):
    width, ff = grads[0].shape
    part = width // n_quarter
    hbm = pl.BlockSpec(memory_space=pl.ANY)
    col = pl.BlockSpec((width, TILE), lambda i: (0, first + i))
    row = pl.BlockSpec((TILE, width), lambda i: (first + i, 0))
    return pl.pallas_call(
        place_kernel,
        grid=(slices.shape[0] // (3 * n_quarter),),
        in_specs=[pl.BlockSpec((3 * n_quarter, part, TILE), lambda i: (i, 0, 0)), hbm, hbm, hbm],
        out_specs=[col, col, row],
        out_shape=[jax.ShapeDtypeStruct(g.shape, g.dtype) for g in grads],
        input_output_aliases={1: 0, 2: 1, 3: 2},
        compiler_params=pltpu.CompilerParams(dimension_semantics=("arbitrary",)),
        cost_estimate=pl.CostEstimate(flops=0, bytes_accessed=4 * slices.size, transcendentals=0),
        name="place_slices",
    )(slices, *grads)


def solution(mesh):
    n_ep = mesh.shape["ep"]
    n_dp = mesh.shape["dp"]
    n_y = 4 if n_dp == 32 else 2
    n_z = n_dp // n_y
    n_dev = n_dp * n_ep
    all_axes = ("dp", "ep")

    def local_step(hidden, grad_out, expert_ids, norm_gain, w_router, w_gate, w_up, w_down):
        n_tok, width = hidden.shape
        n_exp = w_router.shape[1]
        capacity = 4 * n_tok // n_exp
        total_tok = n_tok * n_dev
        dest_rows, slot_owner, loads = route_tables(expert_ids, n_exp, capacity)
        choice_hot = (expert_ids[:, :, None] == jnp.arange(n_exp, dtype=jnp.int32)).astype(F32)

        x_f32 = hidden.astype(F32)
        inv_rms = lax.rsqrt(jnp.mean(x_f32 * x_f32, axis=-1, keepdims=True) + EPS)
        x_hat = x_f32 * inv_rms
        x_norm = (x_hat * norm_gain).astype(BF16)
        xn_f32 = x_norm.astype(F32)
        router_probs = jax.nn.softmax(jnp.dot(xn_f32, w_router, preferred_element_type=F32), axis=-1)
        gate_vals = jnp.sum(router_probs[:, None, :] * choice_hot, axis=-1)

        meta = jnp.concatenate([gate_vals.T.reshape(1, -1), expert_ids.T.astype(F32).reshape(1, -1)], axis=1)
        meta = jnp.pad(meta, ((0, 0), (0, LANES - meta.shape[1])))
        dy_f32 = grad_out.astype(F32)
        d_picked = (dy_f32[:, None, :] * gate_vals[:, :, None]).astype(BF16).reshape(n_tok * 2, width)
        send = jnp.concatenate([
            jnp.take(x_norm, slot_owner // 2, axis=0, mode="fill", fill_value=0),
            jnp.take(d_picked, slot_owner, axis=0, mode="fill", fill_value=0)], axis=1)
        wg, wu, wd = w_gate[0], w_up[0], w_down[0]
        tok = jnp.concatenate([router_probs, inv_rms, gate_vals, dest_rows.reshape(n_tok, 2).astype(F32), expert_ids.astype(F32)], axis=1)
        tok = jnp.pad(tok, ((0, 0), (0, LANES - tok.shape[1])))
        early, late, meta_all, out_hidden, grad_hidden, sums = gather_rows(
            jnp.concatenate([x_norm, grad_out], axis=1), send.reshape(n_exp, capacity, 2 * width), meta[None], hidden, tok,
            norm_gain[None], w_router.T, wg, wu, wd, n_y, n_z, n_ep, 2 * TILE)
        meta_all = meta_all.reshape(n_dev, LANES)
        ids_all = meta_all[:, 2 * n_tok:4 * n_tok].astype(jnp.int32).reshape(n_dev, 2, n_tok)
        gates_all = meta_all[:, :2 * n_tok].reshape(n_dev, 2, n_tok)
        sums = sums[:, 0]
        share = width // n_exp
        grad_router = sums[:, :width].T
        grad_gain = sums[:, width:width + share].reshape(-1)
        prob_sum = sums[0, width + share:width + share + n_exp]
        all_loads = jnp.sum((ids_all[..., None] == jnp.arange(n_exp, dtype=jnp.int32)).astype(F32), axis=(0, 1, 2))
        load_frac = all_loads / (2 * total_tok)
        aux_loss = AUX_COEF * n_exp * jnp.sum(load_frac * prob_sum / total_tok)

        me = lax.axis_index("ep")
        mine = ids_all == me
        member = jnp.any(mine, axis=1)
        gate_me = jnp.sum(jnp.where(mine, gates_all, 0.0), axis=1)
        half = n_tok // 2

        def listed(cut, start):
            named = member[:, cut].reshape(-1, GROUP)
            rank = jnp.cumsum(named.astype(jnp.int32), axis=1)
            ends = start + jnp.cumsum(rank[:, -1])
            offsets = jnp.concatenate([jnp.full((1,), start, jnp.int32), ends])
            pos = jnp.where(named, offsets[:-1, None] + rank - 1, -(2**24))[:, None]
            return offsets, pos, gate_me[:, cut].reshape(-1, 1, GROUP)

        n_block = w_gate.shape[2] // TILE
        own = n_block - n_dp // QUARTERS
        place = lax.axis_index("dp")
        offsets, pos, gate = listed(slice(0, half), jnp.int32(0))
        n_early = offsets[-1]
        late_offsets, late_pos, late_gate = listed(slice(half, n_tok), jnp.maximum(n_early, FIRST_ROWS))
        early_tiles, all_tiles = ((n + TILE - 1) // TILE for n in (n_early, late_offsets[-1]))
        info = jnp.stack([all_tiles, own + place // QUARTERS, place % QUARTERS, early_tiles]).astype(jnp.int32)
        most = capacity * n_dev
        xn, dp, xt, pt = pack_early(early_tiles[None].astype(jnp.int32), early, offsets, pos, gate, most)
        *parts, late = first_grads(xn, xt, dp, pt, wg, wu, wd, late, own, n_y, n_z, n_ep)
        xn, dp, slices = pack_late(info, late.reshape(-1, 2 * width), late_offsets, late_pos, late_gate, wg, wu, wd, xn, dp, most + FIRST_ROWS, QUARTERS)
        slices_all = lax.all_gather(slices, "dp", axis=0, tiled=True)
        grads = last_grads(info, xn, dp, wg, wu, wd, parts)
        g_gate, g_up, g_down = (g[None] for g in place_slices(slices_all, grads, own, QUARTERS))
        return out_hidden, aux_loss, grad_hidden, grad_gain, grad_router, g_gate, g_up, g_down

    tok_spec = P(all_axes, None)
    w_spec = P("ep", None, None)
    return jax.shard_map(local_step, mesh=mesh, in_specs=(tok_spec, tok_spec, tok_spec, P(), P(), w_spec, w_spec, w_spec), out_specs=(tok_spec, P(), tok_spec, P(), P(), w_spec, w_spec, w_spec), check_vma=False)
```

```python
import functools
import jax
import jax.numpy as jnp
from jax import lax
from jax.experimental import pallas as pl
from jax.experimental.pallas import tpu as pltpu
from jax.sharding import PartitionSpec as P

EPS = 1e-6
AUX_COEF = 0.001
LANES = 128
GROUP = 256
MOST_PER_GROUP = 128
ALIGN = 16
TILE = 256
USUAL_ROWS = 2304
QUARTERS = 4
F32 = jnp.float32
BF16 = jnp.bfloat16


def route_tables(expert_ids, n_exp, capacity):
    flat_ids = expert_ids.reshape(-1)
    n_choice = flat_ids.shape[0]
    one_hot = (flat_ids[:, None] == jnp.arange(n_exp, dtype=jnp.int32)[None, :]).astype(jnp.int32)
    running = jnp.cumsum(one_hot, axis=0) - 1
    dest_rows = flat_ids * capacity + jnp.sum(running * one_hot, axis=1)
    slot_owner = jnp.full((n_exp * capacity,), n_choice, jnp.int32).at[dest_rows].set(jnp.arange(n_choice, dtype=jnp.int32))
    return dest_rows, slot_owner, jnp.sum(one_hot, axis=0)


def peers(n_y, n_z, n_ep):
    dp, ep = lax.axis_index("dp"), lax.axis_index("ep")
    y, z = lax.rem(dp, n_y), lax.div(dp, n_y)
    along_ep = [{"dp": dp, "ep": lax.rem(ep + k, n_ep)} for k in range(1, n_ep)]
    along_y = [{"dp": z * n_y + lax.rem(y + k, n_y), "ep": ep} for k in range(1, n_y)]
    along_z = [{"dp": lax.rem(z + k, n_z) * n_y + y, "ep": ep} for k in range(1, n_z)]
    return dp, ep, y, z, along_ep, along_y, along_z


def enter(all_peers):
    barrier = pltpu.get_barrier_semaphore()
    for peer in all_peers:
        pl.semaphore_signal(barrier, inc=1, device_id=peer, device_id_type=pl.DeviceIdType.MESH)
    pl.semaphore_wait(barrier, len(all_peers))


def exchange(targets, make):
    copies = [make(k, target) for k, target in enumerate(targets)]
    for copy in copies:
        copy.start()
    for copy in copies:
        copy.wait()


def remote(src, dst, send_sem, recv_sem, target):
    return pltpu.make_async_remote_copy(src_ref=src, dst_ref=dst, send_sem=send_sem, recv_sem=recv_sem, device_id=target, device_id_type=pl.DeviceIdType.MESH)


def dot(a, b, dims):
    return lax.dot_general(a, b, (dims, ((), ())), preferred_element_type=F32)


def expert_math(hg, hu, da):
    gate = hg.astype(BF16).astype(F32)
    up = hu.astype(BF16).astype(F32)
    d_act = da.astype(BF16).astype(F32)
    sig = jax.nn.sigmoid(gate)
    silu = gate * sig
    act = (silu * up).astype(BF16)
    d_up = (d_act * silu).astype(BF16)
    d_gate = (d_act * up * sig * (1.0 + gate * (1.0 - sig))).astype(BF16)
    return act, d_gate, d_up


LINK_RATE, HOP_US, FFN_US, FFN_FROM_US = 25e3, 4.0, 3.5, 20.0
PIECES = (
    (0, 0, "zxy"), (0, 1, "zyx"), (1, 0, "xyz"), (1, 1, "yzx"))


def due(left):
    steps = [(piece, phase) for piece in range(len(PIECES)) for phase in (1, 2)]
    return [(piece, phase) for piece, phase in steps if (piece, phase) not in left and left.get((piece, phase - 1)) == 0]


def plan(sizes, tile_bytes, n_ffn):
    free, arrive, order, left = {}, [], [], {}
    tasks = [("ffn", 0.0, FFN_US)] * n_ffn + [("back", 0.0, 0.5), ("final", 12.0, 6.0)] + [(f"sum{k}", 5.0, 0.5) for k in range(4)]
    now, next_at = 8.0, FFN_FROM_US

    def issue(hop, when):
        piece, phase, sign, step = hop
        _, half, axes = PIECES[piece]
        size = tile_bytes // (1 if half is None else 2)
        for axis in axes[:phase]:
            size *= sizes[axis]
        size //= 2 if step == sizes[axes[phase]] // 2 else 1
        link = (axes[phase], sign)
        free[link] = max(when, free.get(link, 0.0)) + size / LINK_RATE
        arrive.append((free[link] + HOP_US, hop))

    def begin(piece, phase, when):
        left[piece, phase] = 2 * (sizes[PIECES[piece][2][phase]] // 2)
        for sign in (1, -1):
            issue((piece, phase, sign, 1), when)

    for piece in range(len(PIECES)):
        begin(piece, 0, now)
    while arrive or tasks:
        arrive.sort()
        when, hop = arrive[0] if arrive else (1e9, None)
        if tasks and max(now, next_at) + 0.6 * tasks[0][2] < max(now, when) + (0.0 if arrive else 1e9):
            name, _, lasts = tasks.pop(0)
            order.append(name)
            now = max(now, next_at) + lasts
            next_at = now + (tasks[0][1] if tasks else 0.0)
            continue
        arrive.pop(0)
        now = max(now, when)
        order.append(hop)
        piece, phase, sign, step = hop
        if step < sizes[PIECES[piece][2][phase]] // 2:
            issue((piece, phase, sign, step + 1), now)
        left[piece, phase] -= 1
        for other in due(left):
            begin(*other, now)
    return order, now


class Copies:
    def __init__(self, send_sem, recv_sem):
        self.sems, self.made = (send_sem, recv_sem), {}

    def start(self, name, ends):
        k = len(self.made)
        self.made[name] = lambda: remote(*ends()[:2], self.sems[0].at[k], self.sems[1].at[k], ends()[2])
        self.made[name]().start()

    def wait_recv(self, name):
        self.made[name]().wait_recv()


def gather_kernel(n_y, n_z, n_ep, order, rows_in, send_in, meta_in, x_ref, tok_ref, gain_ref, router_ref, wg_ref, wu_ref, wd_ref, rows_out, meta_res, y_ref, gh_ref, sum_ref,
                  got, result, back_out, meta_out, parts, got_ep, got_y, got_z, total, o_acc, d_acc, send_sem, recv_sem, own_sem):
    step = pl.program_id(0)
    n_x = n_ep // 2
    dp, ep = lax.axis_index("dp"), lax.axis_index("ep")
    at = {"x": lax.div(ep, 2), "y": lax.rem(dp, n_y), "z": lax.div(dp, n_y)}
    core = lax.rem(ep, 2)
    sizes = {"x": n_x, "y": n_y, "z": n_z}
    width = wg_ref.shape[0]
    wide = rows_in.shape[2]

    def shifted(axis, by):
        return lax.rem(at[axis] + by + 2 * sizes[axis], sizes[axis])

    def neighbour(axis, by):
        place = {**at, axis: shifted(axis, by)}
        return {"dp": place["z"] * n_y + place["y"], "ep": place["x"] * 2 + core}

    partner = {"dp": dp, "ep": at["x"] * 2 + (1 - core)}
    along_ep = [{"dp": dp, "ep": lax.rem(ep + k, n_ep)} for k in range(1, n_ep)]
    along_y = [{"dp": at["z"] * n_y + lax.rem(at["y"] + k, n_y), "ep": ep} for k in range(1, n_y)]
    along_z = [{"dp": lax.rem(at["z"] + k, n_z) * n_y + at["y"], "ep": ep} for k in range(1, n_z)]
    copies = Copies(send_sem, recv_sem)

    def columns(piece, half):
        low, high = 0, wide
        for part in (PIECES[piece][1], half):
            if part is not None:
                middle = (low + high) // 2
                low, high = ((low, middle), (middle, high))[part]
        return pl.ds(low, high - low)

    def region(piece, phase, index, half):
        tile, _, axes = PIECES[piece]
        pick = {axis: slice(None) if k < phase else index if k == phase else at[axis] for k, axis in enumerate(axes)}
        return rows_out.at[pick["z"], pick["y"], pick["x"], core, tile, :, columns(piece, half)]

    def send(piece, phase, sign, hop):
        axis = PIECES[piece][2][phase]
        half = None if hop < sizes[axis] // 2 else (0 if sign == 1 else 1)

        def ends():
            dst = region(piece, phase, shifted(axis, -sign * (hop - 1)), half)
            src = rows_in.at[PIECES[piece][0], :, columns(piece, half)] if (phase, hop) == (0, 1) else dst
            return src, dst, neighbour(axis, sign)

        copies.start((piece, phase, sign, hop), ends)

    def to_partner(name, block):
        copies.start(("pair", *name), lambda: (block(), block(), partner))

    left = {}

    def arrived(piece, phase, sign, hop):
        axes = PIECES[piece][2]
        copies.wait_recv((piece, phase, sign, hop))
        last = sizes[axes[phase]] // 2
        if hop < last:
            send(piece, phase, sign, hop + 1)
        if phase == 2:
            half = None if hop < last else (0 if sign == 1 else 1)
            to_partner((piece, phase, sign, hop), lambda: region(piece, phase, shifted(axes[phase], -sign * hop), half))
        left[piece, phase] = left.get((piece, phase), 2 * last) - 1
        if not left[piece, phase] and phase == 1:
            to_partner((piece, phase), lambda: region(piece, 2, at[axes[2]], None))
        for other, later in due(left):
            left[other, later] = 2 * (sizes[PIECES[other][2][later]] // 2)
            for way in (1, -1):
                send(other, later, way, 1)

    def exchange_results(name, src, dst):
        for k, target in enumerate(along_ep):
            copies.start((name, k), lambda target=target: (src.at[target["ep"]], dst.at[ep], target))

    def spread(name, targets, block):
        for k, target in enumerate(targets):
            copies.start((name, k), lambda target=target: (block(), block(), target))

    def all_in(name, n):
        for k in range(n):
            copies.wait_recv((name, k))

    def own_copies():
        return [
            pltpu.make_async_copy(rows_in.at[pl.ds(0, 2)], rows_out.at[at["z"], at["y"], at["x"], core], own_sem.at[0]),
            pltpu.make_async_copy(send_in.at[ep], got.at[ep], own_sem.at[1]),
            pltpu.make_async_copy(meta_in, meta_out.at[pl.ds(dp * n_ep + ep, 1)], own_sem.at[2])]

    def prologue():
        enter(along_ep + [neighbour("y", 1), neighbour("y", -1), neighbour("z", 1), neighbour("z", -1)] + along_y + along_z)
        mine = own_copies()
        for copy in mine:
            copy.start()
        for piece in range(len(PIECES)):
            left[piece, 0] = 2 * (sizes[PIECES[piece][2][0]] // 2)
            for sign in (1, -1):
                send(piece, 0, sign, 1)
        exchange_results("dispatch", send_in, got)
        for copy in mine:
            copy.wait()
        spread("meta_ep", along_ep, lambda: meta_out.at[pl.ds(dp * n_ep + ep, 1)])

    def ready():
        all_in("dispatch", n_ep - 1)
        all_in("meta_ep", n_ep - 1)
        spread("meta_y", along_y, lambda: meta_out.at[pl.ds(dp * n_ep, n_ep)])

    def finish_tokens():
        all_in("back", n_ep - 1)
        all_in("meta_z", n_z - 1)
        n_tok = x_ref.shape[0]
        n_slot = got.shape[0] * got.shape[1]
        tok = tok_ref[...]
        probs, inv = tok[:, :n_ep], tok[:, n_ep:n_ep + 1]
        gates, slots, experts = ([tok[:, n_ep + k:n_ep + k + 1] for k in (first, first + 1)] for first in (1, 3, 5))
        slot_id = lax.broadcasted_iota(jnp.int32, (n_tok, n_slot), 1).astype(F32)
        expert_id = lax.broadcasted_iota(jnp.int32, (n_tok, n_ep), 1).astype(F32)
        picks = [(slot_id == slot).astype(F32).astype(BF16) for slot in slots]
        hots = [(expert_id == expert).astype(F32) for expert in experts]
        back = back_out[...].reshape(n_slot, wide)
        picked = [dot(pick, back[:, :width], ((1,), (0,))) for pick in picks]
        d_picks = [dot(pick, back[:, width:], ((1,), (0,))) for pick in picks]
        x = x_ref[...].astype(F32)
        x_hat = x * inv
        xn = rows_in[:, :, :width].reshape(n_tok, width).astype(F32)
        dy = rows_in[:, :, width:].reshape(n_tok, width).astype(F32)
        ids = meta_out[...]
        lane = lax.broadcasted_iota(jnp.int32, (1, 1, LANES), 2)
        is_id = jnp.logical_and(lane >= 2 * n_tok, lane < 4 * n_tok)
        expert_lane = lax.broadcasted_iota(jnp.int32, (1, n_ep), 1)
        load_frac = jnp.zeros((1, n_ep), F32)
        for e in range(n_ep):
            named = jnp.sum(jnp.where(jnp.logical_and(is_id, ids == float(e)), 1.0, 0.0), axis=0)
            load_frac += jnp.where(expert_lane == e, jnp.sum(named, axis=1, keepdims=True), 0.0)
        total_tok = n_tok * ids.shape[0]
        load_frac = load_frac / (2 * total_tok)
        d_probs = (AUX_COEF * n_ep / total_tok) * load_frac
        for hot, pick in zip(hots, picked):
            d_probs = d_probs + hot * jnp.sum(dy * pick, axis=1, keepdims=True)
        d_logits = probs * (d_probs - jnp.sum(probs * d_probs, axis=1, keepdims=True))
        d_xn = d_picks[0] + d_picks[1]
        for e in range(n_ep):
            d_xn = d_xn + d_logits[:, e:e + 1] * router_ref[e:e + 1, :]
        d_xn = d_xn.astype(BF16).astype(F32)
        d_gain = jnp.sum(d_xn * x_hat, axis=0, keepdims=True)
        d_probs_sum = jnp.sum(tok, axis=0, keepdims=True)
        share = width // n_ep
        for e in range(n_ep):
            parts[e, :, :width] = jnp.sum(d_logits[:, e:e + 1] * xn, axis=0, keepdims=True)
            parts[e, :, width:width + share] = d_gain[:, e * share:(e + 1) * share]
            parts[e, :, width + share:] = d_probs_sum
        y_ref[...] = (x + (gates[0] * picked[0] + gates[1] * picked[1])).astype(BF16)
        scaled = d_xn * gain_ref[...]
        gh_ref[...] = (inv * (scaled - x_hat * jnp.mean(scaled * x_hat, axis=1, keepdims=True)) + dy).astype(BF16)
        got_ep[ep] = parts[ep]
        exchange_results("sum0", parts, got_ep)

    def added(ref, n):
        value = ref[0]
        for k in range(1, n):
            value = value + ref[k]
        return value

    def sum_up(stage):
        if stage == 0:
            all_in("sum0", n_ep - 1)
            got_y[at["y"]] = added(got_ep, n_ep)
            spread("sum1", along_y, lambda: got_y.at[at["y"]])
        if stage == 1:
            all_in("sum1", n_y - 1)
            got_z[at["z"]] = added(got_y, n_y)
            spread("sum2", along_z, lambda: got_z.at[at["z"]])
        if stage == 2:
            all_in("sum2", n_z - 1)
            total[ep] = added(got_z, n_z)
            spread("sum3", along_ep, lambda: total.at[ep])
        if stage == 3:
            all_in("sum3", n_ep - 1)
            sum_ref[...] = total[...]

    runs, current = [], []
    for entry in order:
        if entry == "ffn":
            runs.append(current)
            current = []
        else:
            current.append(entry)
    runs.append(current)
    n_ffn = len(runs) - 1

    @pl.when(step == 0)
    def _():
        prologue()
        for hop in runs[0]:
            arrived(*hop)
        ready()
        o_acc[...] = jnp.zeros_like(o_acc)
        d_acc[...] = jnp.zeros_like(d_acc)

    @pl.when(step < n_ffn)
    def _():
        n_row = got.shape[0] * got.shape[1]
        half = wg_ref.shape[1] // 2
        xn = got[:, :, :width].reshape(n_row, width)
        dy = got[:, :, width:].reshape(n_row, width)
        cuts = [slice(0, half), slice(half, 2 * half)]
        mid = [expert_math(dot(xn, wg_ref[:, c], ((1,), (0,))), dot(xn, wu_ref[:, c], ((1,), (0,))), dot(dy, wd_ref[c, :], ((1,), (1,)))) for c in cuts]
        act, d_gate, d_up = (jnp.concatenate(parts, axis=1) for parts in zip(*mid))
        o_acc[...] += dot(act, wd_ref[...], ((1,), (0,)))
        d_acc[...] += dot(d_gate, wg_ref[...], ((1,), (1,))) + dot(d_up, wu_ref[...], ((1,), (1,)))

    @pl.when(step == n_ffn - 1)
    def _():
        result[:, :, :width] = o_acc[...].astype(BF16).reshape(*result.shape[:2], width)
        result[:, :, width:] = d_acc[...].astype(BF16).reshape(*result.shape[:2], width)

    for k in range(1, n_ffn):
        @pl.when(step == k - 1)
        def _():
            if k == 2:
                all_in("meta_y", n_y - 1)
                spread("meta_z", along_z, lambda: meta_out.at[pl.ds(at["z"] * n_y * n_ep, n_y * n_ep)])
            for hop in runs[k]:
                arrived(*hop)

    @pl.when(step == n_ffn)
    def _():
        for entry in runs[n_ffn]:
            if entry == "back":
                back_out[ep] = result[ep]
                exchange_results("back", result, back_out)
            elif entry == "final":
                finish_tokens()
            elif entry[:3] == "sum":
                sum_up(int(entry[3:]))
            else:
                arrived(*entry)
        meta_res[...] = meta_out[...]
        for name in copies.made:
            if name[0] == "pair":
                copies.wait_recv(name)
        for copy in copies.made.values():
            copy().wait_send()


def gather_rows(rows, send, meta, x, tok, gain, router, wg, wu, wd, n_y, n_z, n_ep, block):
    n_tok, wide = rows.shape
    n_dev = n_y * n_z * n_ep
    capacity = send.shape[1]
    width, ff = wg.shape
    n_ffn = ff // block
    tiles = n_tok // 8
    order, _ = plan({"x": n_ep // 2, "y": n_y, "z": n_z}, 8 * wide * 2, n_ffn)
    hops = [e for e in order if not isinstance(e, str)]
    n_sem = len(hops) + sum(1 for e in hops if e[1] == 2) + len(PIECES)
    n_sem += 5 * (n_ep - 1) + 2 * (n_y - 1) + 2 * (n_z - 1)
    vmem, hbm = pl.BlockSpec(memory_space=pltpu.VMEM), pl.BlockSpec(memory_space=pl.ANY)
    col = pl.BlockSpec((width, block), lambda j: (0, jnp.minimum(j, n_ffn - 1)))
    row = pl.BlockSpec((block, width), lambda j: (jnp.minimum(j, n_ffn - 1), 0))
    slots = pltpu.VMEM((n_ep, capacity, wide), BF16)
    long = width + width // n_ep + LANES
    out, meta_all, y, gh, sums = pl.pallas_call(
        functools.partial(gather_kernel, n_y, n_z, n_ep, order),
        grid=(n_ffn + 1,),
        in_specs=[vmem] * 7 + [col, col, row],
        out_specs=[hbm] + [vmem] * 4,
        out_shape=[
            jax.ShapeDtypeStruct((n_z, n_y, n_ep // 2, 2, 2, 8, wide), BF16),
            jax.ShapeDtypeStruct((n_dev, 1, LANES), F32),
            jax.ShapeDtypeStruct((n_tok, width), BF16),
            jax.ShapeDtypeStruct((n_tok, width), BF16),
            jax.ShapeDtypeStruct((n_ep, 1, long), F32)],
        scratch_shapes=[
            slots, slots, slots, pltpu.VMEM((n_dev, 1, LANES), F32),
            *(pltpu.VMEM((n, 1, long), F32) for n in (n_ep, n_ep, n_y, n_z, n_ep)),
            pltpu.VMEM((n_ep * capacity, width), F32), pltpu.VMEM((n_ep * capacity, width), F32),
            pltpu.SemaphoreType.DMA((n_sem,)), pltpu.SemaphoreType.DMA((n_sem,)), pltpu.SemaphoreType.DMA((3,))],
        compiler_params=pltpu.CompilerParams(collective_id=1, has_side_effects=True, dimension_semantics=("arbitrary",), vmem_limit_bytes=56 * 2**20),
        cost_estimate=pl.CostEstimate(flops=12 * n_ep * capacity * width * ff, bytes_accessed=6 * width * ff, transcendentals=0),
        name="gather_rows",
    )(rows.reshape(tiles, 8, wide), send, meta, x, tok, gain, router, wg, wu, wd)
    return out.reshape(n_dev * 16, wide), meta_all, y, gh, sums


def pack_kernel(n_quarter, info_ref, off_ref, near_ref, far_ref, pos_ref, gate_ref, wg_ref, wu_ref, wd_ref, xn_out, dp_out, slice_ref, xn_buf, dp_buf, acc_g, acc_u, acc_d, sem):
    g = pl.program_id(0)
    n_group = pl.num_programs(0)
    width = xn_buf.shape[1]
    tile = MOST_PER_GROUP + ALIGN
    off = off_ref[g]
    base = pl.multiple_of(lax.div(off, ALIGN) * ALIGN, ALIGN)
    hit = lax.broadcasted_iota(jnp.int32, (tile, GROUP), 0) + base == pos_ref[0]
    pick = hit.astype(F32).astype(BF16)
    gate = jnp.sum(jnp.where(hit, gate_ref[0], 0.0), axis=1, keepdims=True)
    head, rest = pl.ds(base, ALIGN), pl.ds(pl.multiple_of(base + ALIGN, ALIGN), tile - ALIGN)
    wide = min(2 * TILE, width)
    half = near_ref.shape[0]
    keep = lax.broadcasted_iota(jnp.int32, (ALIGN, wide), 0) + base < off
    for buf, low, scale in ((xn_buf, 0, None), (dp_buf, width, gate)):
        for c in range(0, width, wide):
            cut = slice(c, c + wide)
            columns = slice(low + c, low + c + wide)
            new = dot(pick[:, :half], near_ref[:, columns], ((1,), (0,))) + dot(pick[:, half:], far_ref[:, columns], ((1,), (0,)))
            new = (new if scale is None else new * scale).astype(BF16)
            buf[head, cut] = jnp.where(keep, buf[head, cut].astype(F32), new[:ALIGN].astype(F32)).astype(BF16)
            buf[rest, cut] = new[ALIGN:]

    @pl.when(g == n_group - 1)
    def _():
        usual = USUAL_ROWS // TILE
        zeros = jnp.zeros((TILE, width), BF16)
        tail = pl.ds(pl.multiple_of(base + tile, ALIGN), TILE)
        xn_buf[tail, :] = zeros
        dp_buf[tail, :] = zeros
        used = info_ref[0]

        def at(t):
            return pl.ds(pl.multiple_of(t * TILE, TILE), TILE)

        def clear(t, carry):
            xn_buf[at(t), :] = zeros
            dp_buf[at(t), :] = zeros
            return carry

        lax.fori_loop(used, usual, clear, 0)

        part = width // n_quarter
        low = pl.multiple_of(info_ref[2] * part, part)
        quarter = pl.ds(low, part)
        wg, wu, wd = wg_ref[...], wu_ref[...], wd_ref[...]
        for acc in (acc_g, acc_u, acc_d):
            acc[...] = jnp.zeros_like(acc)

        def hidden_rows(x, p):
            return expert_math(dot(x, wg, ((1,), (0,))), dot(x, wu, ((1,), (0,))), dot(p, wd, ((1,), (1,))))

        def copies(t):
            return [pltpu.make_async_copy(buf.at[at(t)], out.at[at(t)], sem.at[k]) for k, (buf, out) in enumerate(((xn_buf, xn_out), (dp_buf, dp_out)))]

        def begin(t, carry):
            for copy in copies(t):
                copy.start()
            return carry

        def end(t, carry):
            for copy in copies(t):
                copy.wait()
            return carry

        def add(t, carry):
            act, dg, du = hidden_rows(xn_buf[at(t), :], dp_buf[at(t), :])
            acc_g[...] += dot(xn_buf[at(t), quarter], dg, ((0,), (0,)))
            acc_u[...] += dot(xn_buf[at(t), quarter], du, ((0,), (0,)))
            acc_d[...] += dot(act, dp_buf[at(t), quarter], ((0,), (0,)))

            @pl.when(t == 1)
            def _():
                lax.fori_loop(0, jnp.maximum(used, usual), begin, 0)

            return carry

        lax.fori_loop(0, jnp.maximum(used, 2), add, 0)
        slice_ref[0] = acc_g[...].astype(BF16)
        slice_ref[1] = acc_u[...].astype(BF16)
        for k in range(0, part, TILE):
            slice_ref[2, k:k + TILE, :] = acc_d[:, k:k + TILE].astype(BF16)
        lax.fori_loop(0, jnp.maximum(used, usual), end, 0)


def pack_rows(info, near, far, offsets, pos, gates, wg, wu, wd, most, n_quarter):
    total, width = 2 * near.shape[0], near.shape[1] // 2
    n_group = total // GROUP
    half = pl.BlockSpec((GROUP // 2, 2 * width), lambda g, info, off: (g, 0))
    usual, part = USUAL_ROWS, width // n_quarter
    small = pl.BlockSpec((1, 1, GROUP), lambda g, info, off: (g, 0, 0))
    col = pl.BlockSpec((width, TILE), lambda g, info, off: (0, info[1]))
    row = pl.BlockSpec((TILE, width), lambda g, info, off: (info[1], 0))
    whole = pl.BlockSpec(memory_space=pl.ANY)
    buf = pltpu.VMEM((max(most, usual) + 2 * TILE + ALIGN, width), BF16)
    out = jax.ShapeDtypeStruct((max(most, usual), width), BF16)
    return pl.pallas_call(
        functools.partial(pack_kernel, n_quarter),
        grid_spec=pltpu.PrefetchScalarGridSpec(
            num_scalar_prefetch=2,
            grid=(n_group,),
            in_specs=[half, half, small, small, col, col, row],
            out_specs=[whole, whole, pl.BlockSpec((3, part, TILE), lambda g, info, off: (0, 0, 0))],
            scratch_shapes=[
                buf, buf, pltpu.VMEM((part, TILE), F32), pltpu.VMEM((part, TILE), F32), pltpu.VMEM((TILE, part), F32), pltpu.SemaphoreType.DMA((2,))],
        ),
        out_shape=[out, out, jax.ShapeDtypeStruct((3, part, TILE), BF16)],
        compiler_params=pltpu.CompilerParams(dimension_semantics=("arbitrary",), vmem_limit_bytes=63 * 2**20),
        cost_estimate=pl.CostEstimate(flops=4 * GROUP * total * width, bytes_accessed=4 * total * width, transcendentals=0),
        name="pack_rows",
    )(info, offsets, near, far, pos, gates, wg, wu, wd)


def grads_kernel(info_ref, xn_hbm, dp_hbm, wg_ref, wu_ref, wd_ref, gg_ref, gu_ref, gd_ref, xn, xt, dp, act_t, d_gate, d_up, acc_g, acc_u, acc_d, tile_x, tile_p, sem):
    rows, width = xn.shape
    tiles = [slice(r, r + TILE) for r in range(0, rows, TILE)]

    @pl.when(pl.program_id(0) == 0)
    def _():
        def copies(t):
            at = pl.ds(pl.multiple_of(t * TILE, TILE), TILE)
            return [pltpu.make_async_copy(src.at[at], dst.at[at], sem.at[k, t]) for k, (src, dst) in enumerate(((xn_hbm, xn), (dp_hbm, dp)))]

        def begin(t, carry):
            for copy in copies(t):
                copy.start()
            return carry

        def end(t, carry):
            for copy in copies(t):
                copy.wait()
            at = pl.ds(pl.multiple_of(t * TILE, TILE), TILE)
            xt[:, at] = xn[at, :].T
            return carry

        lax.fori_loop(0, len(tiles), begin, 0)
        for acc in (acc_g, acc_u, acc_d):
            acc[...] = jnp.zeros_like(acc)
        lax.fori_loop(0, len(tiles), end, 0)

    wg, wu, wd = wg_ref[...], wu_ref[...], wd_ref[...]

    def hidden_rows(x, p):
        return expert_math(dot(x, wg, ((1,), (0,))), dot(x, wu, ((1,), (0,))), dot(p, wd, ((1,), (1,))))

    @pl.when(info_ref[0] > rows // TILE)
    def _():
        for acc in (acc_g, acc_u, acc_d):
            acc[...] = jnp.zeros_like(acc)

        def more(t, carry):
            at = pl.ds(pl.multiple_of(t * TILE, TILE), TILE)
            copies = [pltpu.make_async_copy(xn_hbm.at[at], tile_x, sem.at[0, 0]), pltpu.make_async_copy(dp_hbm.at[at], tile_p, sem.at[1, 0])]
            for copy in copies:
                copy.start()
            for copy in copies:
                copy.wait()
            act, d_gate[:TILE, :], d_up[:TILE, :] = hidden_rows(tile_x[...], tile_p[...])
            act_t[:, :TILE] = act.T

            def part(c, carry):
                cut = pl.ds(pl.multiple_of(c * TILE, TILE), TILE)
                acc_g[cut, :] += dot(tile_x[:, cut], d_gate[:TILE, :], ((0,), (0,)))
                acc_u[cut, :] += dot(tile_x[:, cut], d_up[:TILE, :], ((0,), (0,)))
                acc_d[:, cut] += dot(act_t[:, :TILE], tile_p[:, cut], ((1,), (0,)))
                return carry

            lax.fori_loop(0, width // TILE, part, 0)
            return carry

        lax.fori_loop(rows // TILE, info_ref[0], more, 0)

    for t in tiles:
        act, d_gate[t, :], d_up[t, :] = hidden_rows(xn[t, :], dp[t, :])
        act_t[:, t] = act.T

    wide = min(2 * TILE, width)
    for c in range(0, width, wide):
        cut = slice(c, c + wide)
        gg_ref[cut, :] = (dot(xt[cut, :], d_gate[...], ((1,), (0,))) + acc_g[cut, :]).astype(BF16)
        gu_ref[cut, :] = (dot(xt[cut, :], d_up[...], ((1,), (0,))) + acc_u[cut, :]).astype(BF16)
    for c in range(0, width, wide):
        cut = slice(c, c + wide)
        gd_ref[:, cut] = (dot(act_t[...], dp[:, cut], ((1,), (0,))) + acc_d[:, cut]).astype(BF16)


def expert_grads(info, xn, dp, wg, wu, wd, n_block):
    width, ff = wg.shape
    rows = USUAL_ROWS
    hbm = pl.BlockSpec(memory_space=pl.ANY)
    col = pl.BlockSpec((width, TILE), lambda j, info: (0, j))
    row = pl.BlockSpec((TILE, width), lambda j, info: (j, 0))
    return pl.pallas_call(
        grads_kernel,
        grid_spec=pltpu.PrefetchScalarGridSpec(
            num_scalar_prefetch=1,
            grid=(n_block,),
            in_specs=[hbm, hbm, col, col, row],
            out_specs=[col, col, row],
            scratch_shapes=[
                pltpu.VMEM((rows, width), BF16), pltpu.VMEM((width, rows), BF16), pltpu.VMEM((rows, width), BF16),
                pltpu.VMEM((TILE, rows), BF16), pltpu.VMEM((rows, TILE), BF16), pltpu.VMEM((rows, TILE), BF16),
                pltpu.VMEM((width, TILE), F32), pltpu.VMEM((width, TILE), F32), pltpu.VMEM((TILE, width), F32),
                pltpu.VMEM((TILE, width), BF16), pltpu.VMEM((TILE, width), BF16), pltpu.SemaphoreType.DMA((2, rows // TILE))],
        ),
        out_shape=[jax.ShapeDtypeStruct((width, ff), BF16)] * 2 + [jax.ShapeDtypeStruct((ff, width), BF16)],
        compiler_params=pltpu.CompilerParams(dimension_semantics=("arbitrary",), vmem_limit_bytes=63 * 2**20),
        cost_estimate=pl.CostEstimate(flops=12 * rows * width * TILE * n_block, bytes_accessed=12 * width * TILE * n_block, transcendentals=0),
        name="expert_grads",
    )(info, xn, dp, wg, wu, wd)


def place_kernel(slices_ref, gg_in, gu_in, gd_in, gg_ref, gu_ref, gd_ref):
    part = slices_ref.shape[1]
    for q in range(slices_ref.shape[0] // 3):
        rows = slice(q * part, (q + 1) * part)
        gg_ref[rows, :] = slices_ref[3 * q]
        gu_ref[rows, :] = slices_ref[3 * q + 1]
        for k in range(0, part, TILE):
            gd_ref[:, q * part + k:q * part + k + TILE] = slices_ref[3 * q + 2, k:k + TILE, :]


def place_slices(slices, grads, first, n_quarter):
    width, ff = grads[0].shape
    part = width // n_quarter
    hbm = pl.BlockSpec(memory_space=pl.ANY)
    col = pl.BlockSpec((width, TILE), lambda i: (0, first + i))
    row = pl.BlockSpec((TILE, width), lambda i: (first + i, 0))
    return pl.pallas_call(
        place_kernel,
        grid=(slices.shape[0] // (3 * n_quarter),),
        in_specs=[pl.BlockSpec((3 * n_quarter, part, TILE), lambda i: (i, 0, 0)), hbm, hbm, hbm],
        out_specs=[col, col, row],
        out_shape=[jax.ShapeDtypeStruct(g.shape, g.dtype) for g in grads],
        input_output_aliases={1: 0, 2: 1, 3: 2},
        compiler_params=pltpu.CompilerParams(dimension_semantics=("arbitrary",)),
        cost_estimate=pl.CostEstimate(flops=0, bytes_accessed=4 * slices.size, transcendentals=0),
        name="place_slices",
    )(slices, *grads)


def solution(mesh):
    n_ep = mesh.shape["ep"]
    n_dp = mesh.shape["dp"]
    n_y = 4 if n_dp == 32 else 2
    n_z = n_dp // n_y
    n_dev = n_dp * n_ep
    all_axes = ("dp", "ep")

    def local_step(hidden, grad_out, expert_ids, norm_gain, w_router, w_gate, w_up, w_down):
        n_tok, width = hidden.shape
        n_exp = w_router.shape[1]
        capacity = 4 * n_tok // n_exp
        total_tok = n_tok * n_dev
        dest_rows, slot_owner, loads = route_tables(expert_ids, n_exp, capacity)
        choice_hot = (expert_ids[:, :, None] == jnp.arange(n_exp, dtype=jnp.int32)).astype(F32)

        x_f32 = hidden.astype(F32)
        inv_rms = lax.rsqrt(jnp.mean(x_f32 * x_f32, axis=-1, keepdims=True) + EPS)
        x_hat = x_f32 * inv_rms
        x_norm = (x_hat * norm_gain).astype(BF16)
        xn_f32 = x_norm.astype(F32)
        router_probs = jax.nn.softmax(jnp.dot(xn_f32, w_router, preferred_element_type=F32), axis=-1)
        gate_vals = jnp.sum(router_probs[:, None, :] * choice_hot, axis=-1)

        meta = jnp.concatenate([gate_vals.T.reshape(1, -1), expert_ids.T.astype(F32).reshape(1, -1)], axis=1)
        meta = jnp.pad(meta, ((0, 0), (0, LANES - meta.shape[1])))
        dy_f32 = grad_out.astype(F32)
        d_picked = (dy_f32[:, None, :] * gate_vals[:, :, None]).astype(BF16).reshape(n_tok * 2, width)
        send = jnp.concatenate([
            jnp.take(x_norm, slot_owner // 2, axis=0, mode="fill", fill_value=0),
            jnp.take(d_picked, slot_owner, axis=0, mode="fill", fill_value=0)], axis=1)
        wg, wu, wd = w_gate[0], w_up[0], w_down[0]
        tok = jnp.concatenate([router_probs, inv_rms, gate_vals, dest_rows.reshape(n_tok, 2).astype(F32), expert_ids.astype(F32)], axis=1)
        tok = jnp.pad(tok, ((0, 0), (0, LANES - tok.shape[1])))
        rows = jnp.concatenate([x_norm, grad_out], axis=1)
        half = n_tok // 2
        far = lax.all_gather(rows[half:], all_axes, axis=0, tiled=True)
        near, meta_all, out_hidden, grad_hidden, sums = gather_rows(
            rows, send.reshape(n_exp, capacity, 2 * width), meta[None], hidden, tok,
            norm_gain[None], w_router.T, wg, wu, wd, n_y, n_z, n_ep, 2 * TILE)
        meta_all = meta_all.reshape(n_dev, LANES)
        ids_all = meta_all[:, 2 * n_tok:4 * n_tok].astype(jnp.int32).reshape(n_dev, 2, n_tok)
        gates_all = meta_all[:, :2 * n_tok].reshape(n_dev, 2, n_tok)
        sums = sums[:, 0]
        share = width // n_exp
        grad_router = sums[:, :width].T
        grad_gain = sums[:, width:width + share].reshape(-1)
        prob_sum = sums[0, width + share:width + share + n_exp]
        all_loads = jnp.sum((ids_all[..., None] == jnp.arange(n_exp, dtype=jnp.int32)).astype(F32), axis=(0, 1, 2))
        load_frac = all_loads / (2 * total_tok)
        aux_loss = AUX_COEF * n_exp * jnp.sum(load_frac * prob_sum / total_tok)

        me = lax.axis_index("ep")
        mine = ids_all == me

        def by_group(a):
            return jnp.concatenate([a[:, :half].reshape(-1, GROUP // 2), a[:, half:].reshape(-1, GROUP // 2)], axis=1)

        member = by_group(jnp.any(mine, axis=1))
        gate_me = by_group(jnp.sum(jnp.where(mine, gates_all, 0.0), axis=1))[:, None]
        rank = jnp.cumsum(member.astype(jnp.int32), axis=1)
        counts = rank[:, -1]
        ends = jnp.cumsum(counts)
        offsets = jnp.concatenate([jnp.zeros((1,), jnp.int32), ends])
        pos = jnp.where(member, offsets[:-1, None] + rank - 1, -(2**24))[:, None]
        n_block = w_gate.shape[2] // TILE
        own = n_block - n_dp // QUARTERS
        place = lax.axis_index("dp")
        info = jnp.stack([(offsets[-1] + TILE - 1) // TILE, own + place // QUARTERS, place % QUARTERS]).astype(jnp.int32)
        xn, dp, slices = pack_rows(info, near, far, offsets, pos, gate_me, wg, wu, wd, capacity * n_dev, QUARTERS)
        slices_all = lax.all_gather(slices, "dp", axis=0, tiled=True)
        grads = expert_grads(info, xn, dp, wg, wu, wd, own)
        g_gate, g_up, g_down = (g[None] for g in place_slices(slices_all, grads, own, QUARTERS))
        return out_hidden, aux_loss, grad_hidden, grad_gain, grad_router, g_gate, g_up, g_down

    tok_spec = P(all_axes, None)
    w_spec = P("ep", None, None)
    return jax.shard_map(local_step, mesh=mesh, in_specs=(tok_spec, tok_spec, tok_spec, P(), P(), w_spec, w_spec, w_spec), out_specs=(tok_spec, P(), tok_spec, P(), P(), w_spec, w_spec, w_spec), check_vma=False)
```

```python
import functools
import jax
import jax.numpy as jnp
from jax import lax
from jax.experimental import pallas as pl
from jax.experimental.pallas import tpu as pltpu
from jax.sharding import PartitionSpec as P

EPS = 1e-6
AUX_COEF = 0.001
LANES = 128
GROUP = 256
MOST_PER_GROUP = 128
ALIGN = 16
TILE = 256
USUAL_ROWS = 2304
QUARTERS = 4
F32 = jnp.float32
BF16 = jnp.bfloat16


def route_tables(expert_ids, n_exp, capacity):
    flat_ids = expert_ids.reshape(-1)
    n_choice = flat_ids.shape[0]
    one_hot = (flat_ids[:, None] == jnp.arange(n_exp, dtype=jnp.int32)[None, :]).astype(jnp.int32)
    running = jnp.cumsum(one_hot, axis=0) - 1
    dest_rows = flat_ids * capacity + jnp.sum(running * one_hot, axis=1)
    slot_owner = jnp.full((n_exp * capacity,), n_choice, jnp.int32).at[dest_rows].set(jnp.arange(n_choice, dtype=jnp.int32))
    return dest_rows, slot_owner, jnp.sum(one_hot, axis=0)


def peers(n_y, n_z, n_ep):
    dp, ep = lax.axis_index("dp"), lax.axis_index("ep")
    y, z = lax.rem(dp, n_y), lax.div(dp, n_y)
    along_ep = [{"dp": dp, "ep": lax.rem(ep + k, n_ep)} for k in range(1, n_ep)]
    along_y = [{"dp": z * n_y + lax.rem(y + k, n_y), "ep": ep} for k in range(1, n_y)]
    along_z = [{"dp": lax.rem(z + k, n_z) * n_y + y, "ep": ep} for k in range(1, n_z)]
    return dp, ep, y, z, along_ep, along_y, along_z


def enter(all_peers):
    barrier = pltpu.get_barrier_semaphore()
    for peer in all_peers:
        pl.semaphore_signal(barrier, inc=1, device_id=peer, device_id_type=pl.DeviceIdType.MESH)
    pl.semaphore_wait(barrier, len(all_peers))


def exchange(targets, make):
    copies = [make(k, target) for k, target in enumerate(targets)]
    for copy in copies:
        copy.start()
    for copy in copies:
        copy.wait()


def remote(src, dst, send_sem, recv_sem, target):
    return pltpu.make_async_remote_copy(src_ref=src, dst_ref=dst, send_sem=send_sem, recv_sem=recv_sem, device_id=target, device_id_type=pl.DeviceIdType.MESH)


def dot(a, b, dims):
    return lax.dot_general(a, b, (dims, ((), ())), preferred_element_type=F32)


def expert_math(hg, hu, da):
    gate = hg.astype(BF16).astype(F32)
    up = hu.astype(BF16).astype(F32)
    d_act = da.astype(BF16).astype(F32)
    sig = jax.nn.sigmoid(gate)
    silu = gate * sig
    act = (silu * up).astype(BF16)
    d_up = (d_act * silu).astype(BF16)
    d_gate = (d_act * up * sig * (1.0 + gate * (1.0 - sig))).astype(BF16)
    return act, d_gate, d_up


LINK_RATE, HOP_US, FFN_US, FFN_FROM_US = 25e3, 4.0, 3.5, 20.0
PIECES = (
    (0, 0, "zxy"), (0, 1, "zyx"), (1, 0, "xyz"), (1, 1, "yzx"))


def due(left):
    steps = [(piece, phase) for piece in range(len(PIECES)) for phase in (1, 2) if phase == 1 or "local" in left]
    return [(piece, phase) for piece, phase in steps if (piece, phase) not in left and left.get((piece, phase - 1)) == 0]


def plan(sizes, tile_bytes, n_ffn):
    free, arrive, order, left = {}, [], [], {}
    tasks = [("ffn", 0.0, FFN_US)] * n_ffn + [("back", 0.0, 0.5), ("final", 12.0, 6.0)] + [(f"sum{k}", 5.0, 0.5) for k in range(4)]
    now, next_at = 8.0, FFN_FROM_US

    def issue(hop, when):
        piece, phase, sign, step = hop
        _, half, axes = PIECES[piece]
        size = tile_bytes // (1 if half is None else 2)
        for axis in axes[:phase]:
            size *= sizes[axis]
        size //= 2 if step == sizes[axes[phase]] // 2 else 1
        link = (axes[phase], sign)
        free[link] = max(when, free.get(link, 0.0)) + size / LINK_RATE
        arrive.append((free[link] + HOP_US, hop))

    def begin(piece, phase, when):
        left[piece, phase] = 2 * (sizes[PIECES[piece][2][phase]] // 2)
        for sign in (1, -1):
            issue((piece, phase, sign, 1), when)

    for piece in range(len(PIECES)):
        begin(piece, 0, now)
    while arrive or tasks:
        arrive.sort()
        when, hop = arrive[0] if arrive else (1e9, None)
        if tasks and max(now, next_at) + 0.6 * tasks[0][2] < max(now, when) + (0.0 if arrive else 1e9):
            name, _, lasts = tasks.pop(0)
            order.append(name)
            now = max(now, next_at) + lasts
            next_at = now + (tasks[0][1] if tasks else 0.0)
            if not tasks:
                left["local"] = 0
                for other in due(left):
                    begin(*other, now)
            continue
        arrive.pop(0)
        now = max(now, when)
        order.append(hop)
        piece, phase, sign, step = hop
        if step < sizes[PIECES[piece][2][phase]] // 2:
            issue((piece, phase, sign, step + 1), now)
        left[piece, phase] -= 1
        for other in due(left):
            begin(*other, now)
    return order, now


class Copies:
    def __init__(self, send_sem, recv_sem):
        self.sems, self.made = (send_sem, recv_sem), {}

    def start(self, name, ends):
        k = len(self.made)
        self.made[name] = lambda: remote(*ends()[:2], self.sems[0].at[k], self.sems[1].at[k], ends()[2])
        self.made[name]().start()

    def wait_recv(self, name):
        self.made[name]().wait_recv()


def gather_kernel(n_y, n_z, n_ep, order, rows_in, send_in, meta_in, x_ref, tok_ref, gain_ref, router_ref, wg_ref, wu_ref, wd_ref, rows_out, meta_res, y_ref, gh_ref, sum_ref,
                  got, result, back_out, meta_out, parts, got_ep, got_y, got_z, total, o_acc, d_acc, send_sem, recv_sem, own_sem):
    step = pl.program_id(0)
    n_x = n_ep // 2
    dp, ep = lax.axis_index("dp"), lax.axis_index("ep")
    at = {"x": lax.div(ep, 2), "y": lax.rem(dp, n_y), "z": lax.div(dp, n_y)}
    core = lax.rem(ep, 2)
    sizes = {"x": n_x, "y": n_y, "z": n_z}
    width = wg_ref.shape[0]
    wide = rows_in.shape[2]

    def shifted(axis, by):
        return lax.rem(at[axis] + by + 2 * sizes[axis], sizes[axis])

    def neighbour(axis, by):
        place = {**at, axis: shifted(axis, by)}
        return {"dp": place["z"] * n_y + place["y"], "ep": place["x"] * 2 + core}

    partner = {"dp": dp, "ep": at["x"] * 2 + (1 - core)}
    along_ep = [{"dp": dp, "ep": lax.rem(ep + k, n_ep)} for k in range(1, n_ep)]
    along_y = [{"dp": at["z"] * n_y + lax.rem(at["y"] + k, n_y), "ep": ep} for k in range(1, n_y)]
    along_z = [{"dp": lax.rem(at["z"] + k, n_z) * n_y + at["y"], "ep": ep} for k in range(1, n_z)]
    copies = Copies(send_sem, recv_sem)

    def columns(piece, half):
        low, high = 0, wide
        for part in (PIECES[piece][1], half):
            if part is not None:
                middle = (low + high) // 2
                low, high = ((low, middle), (middle, high))[part]
        return pl.ds(low, high - low)

    def region(piece, phase, index, half):
        tile, _, axes = PIECES[piece]
        pick = {axis: slice(None) if k < phase else index if k == phase else at[axis] for k, axis in enumerate(axes)}
        return rows_out.at[pick["z"], pick["y"], pick["x"], core, tile, :, columns(piece, half)]

    def send(piece, phase, sign, hop):
        axis = PIECES[piece][2][phase]
        half = None if hop < sizes[axis] // 2 else (0 if sign == 1 else 1)

        def ends():
            dst = region(piece, phase, shifted(axis, -sign * (hop - 1)), half)
            src = rows_in.at[PIECES[piece][0], :, columns(piece, half)] if (phase, hop) == (0, 1) else dst
            return src, dst, neighbour(axis, sign)

        copies.start((piece, phase, sign, hop), ends)

    def to_partner(name, block):
        copies.start(("pair", *name), lambda: (block(), block(), partner))

    left = {}

    def arrived(piece, phase, sign, hop):
        axes = PIECES[piece][2]
        copies.wait_recv((piece, phase, sign, hop))
        last = sizes[axes[phase]] // 2
        if hop < last:
            send(piece, phase, sign, hop + 1)
        if phase == 2:
            half = None if hop < last else (0 if sign == 1 else 1)
            to_partner((piece, phase, sign, hop), lambda: region(piece, phase, shifted(axes[phase], -sign * hop), half))
        left[piece, phase] = left.get((piece, phase), 2 * last) - 1
        if not left[piece, phase] and phase == 1:
            to_partner((piece, phase), lambda: region(piece, 2, at[axes[2]], None))
        begin_due()

    def begin_due():
        for other, later in due(left):
            left[other, later] = 2 * (sizes[PIECES[other][2][later]] // 2)
            for way in (1, -1):
                send(other, later, way, 1)

    def exchange_results(name, src, dst):
        for k, target in enumerate(along_ep):
            copies.start((name, k), lambda target=target: (src.at[target["ep"]], dst.at[ep], target))

    def spread(name, targets, block):
        for k, target in enumerate(targets):
            copies.start((name, k), lambda target=target: (block(), block(), target))

    def all_in(name, n):
        for k in range(n):
            copies.wait_recv((name, k))

    def own_copies():
        return [
            pltpu.make_async_copy(rows_in.at[pl.ds(0, 2)], rows_out.at[at["z"], at["y"], at["x"], core], own_sem.at[0]),
            pltpu.make_async_copy(send_in.at[ep], got.at[ep], own_sem.at[1]),
            pltpu.make_async_copy(meta_in, meta_out.at[pl.ds(dp * n_ep + ep, 1)], own_sem.at[2])]

    def prologue():
        enter(along_ep + [neighbour("y", 1), neighbour("y", -1), neighbour("z", 1), neighbour("z", -1)] + along_y + along_z)
        mine = own_copies()
        for copy in mine:
            copy.start()
        for piece in range(len(PIECES)):
            left[piece, 0] = 2 * (sizes[PIECES[piece][2][0]] // 2)
            for sign in (1, -1):
                send(piece, 0, sign, 1)
        exchange_results("dispatch", send_in, got)
        for copy in mine:
            copy.wait()
        spread("meta_ep", along_ep, lambda: meta_out.at[pl.ds(dp * n_ep + ep, 1)])

    def ready():
        all_in("dispatch", n_ep - 1)
        all_in("meta_ep", n_ep - 1)
        spread("meta_y", along_y, lambda: meta_out.at[pl.ds(dp * n_ep, n_ep)])

    def finish_tokens():
        all_in("back", n_ep - 1)
        all_in("meta_z", n_z - 1)
        n_tok = x_ref.shape[0]
        n_slot = got.shape[0] * got.shape[1]
        tok = tok_ref[...]
        probs, inv = tok[:, :n_ep], tok[:, n_ep:n_ep + 1]
        gates, slots, experts = ([tok[:, n_ep + k:n_ep + k + 1] for k in (first, first + 1)] for first in (1, 3, 5))
        slot_id = lax.broadcasted_iota(jnp.int32, (n_tok, n_slot), 1).astype(F32)
        expert_id = lax.broadcasted_iota(jnp.int32, (n_tok, n_ep), 1).astype(F32)
        picks = [(slot_id == slot).astype(F32).astype(BF16) for slot in slots]
        hots = [(expert_id == expert).astype(F32) for expert in experts]
        back = back_out[...].reshape(n_slot, wide)
        picked = [dot(pick, back[:, :width], ((1,), (0,))) for pick in picks]
        d_picks = [dot(pick, back[:, width:], ((1,), (0,))) for pick in picks]
        x = x_ref[...].astype(F32)
        x_hat = x * inv
        xn = rows_in[:, :, :width].reshape(n_tok, width).astype(F32)
        dy = rows_in[:, :, width:].reshape(n_tok, width).astype(F32)
        ids = meta_out[...]
        lane = lax.broadcasted_iota(jnp.int32, (1, 1, LANES), 2)
        is_id = jnp.logical_and(lane >= 2 * n_tok, lane < 4 * n_tok)
        expert_lane = lax.broadcasted_iota(jnp.int32, (1, n_ep), 1)
        load_frac = jnp.zeros((1, n_ep), F32)
        for e in range(n_ep):
            named = jnp.sum(jnp.where(jnp.logical_and(is_id, ids == float(e)), 1.0, 0.0), axis=0)
            load_frac += jnp.where(expert_lane == e, jnp.sum(named, axis=1, keepdims=True), 0.0)
        total_tok = n_tok * ids.shape[0]
        load_frac = load_frac / (2 * total_tok)
        d_probs = (AUX_COEF * n_ep / total_tok) * load_frac
        for hot, pick in zip(hots, picked):
            d_probs = d_probs + hot * jnp.sum(dy * pick, axis=1, keepdims=True)
        d_logits = probs * (d_probs - jnp.sum(probs * d_probs, axis=1, keepdims=True))
        d_xn = d_picks[0] + d_picks[1]
        for e in range(n_ep):
            d_xn = d_xn + d_logits[:, e:e + 1] * router_ref[e:e + 1, :]
        d_xn = d_xn.astype(BF16).astype(F32)
        d_gain = jnp.sum(d_xn * x_hat, axis=0, keepdims=True)
        d_probs_sum = jnp.sum(tok, axis=0, keepdims=True)
        share = width // n_ep
        for e in range(n_ep):
            parts[e, :, :width] = jnp.sum(d_logits[:, e:e + 1] * xn, axis=0, keepdims=True)
            parts[e, :, width:width + share] = d_gain[:, e * share:(e + 1) * share]
            parts[e, :, width + share:] = d_probs_sum
        y_ref[...] = (x + (gates[0] * picked[0] + gates[1] * picked[1])).astype(BF16)
        scaled = d_xn * gain_ref[...]
        gh_ref[...] = (inv * (scaled - x_hat * jnp.mean(scaled * x_hat, axis=1, keepdims=True)) + dy).astype(BF16)
        got_ep[ep] = parts[ep]
        exchange_results("sum0", parts, got_ep)

    def added(ref, n):
        value = ref[0]
        for k in range(1, n):
            value = value + ref[k]
        return value

    def sum_up(stage):
        if stage == 0:
            all_in("sum0", n_ep - 1)
            got_y[at["y"]] = added(got_ep, n_ep)
            spread("sum1", along_y, lambda: got_y.at[at["y"]])
        if stage == 1:
            all_in("sum1", n_y - 1)
            got_z[at["z"]] = added(got_y, n_y)
            spread("sum2", along_z, lambda: got_z.at[at["z"]])
        if stage == 2:
            all_in("sum2", n_z - 1)
            total[ep] = added(got_z, n_z)
            spread("sum3", along_ep, lambda: total.at[ep])
        if stage == 3:
            all_in("sum3", n_ep - 1)
            sum_ref[...] = total[...]
            left["local"] = 0
            begin_due()

    runs, current = [], []
    for entry in order:
        if entry == "ffn":
            runs.append(current)
            current = []
        else:
            current.append(entry)
    runs.append(current)
    n_ffn = len(runs) - 1

    @pl.when(step == 0)
    def _():
        prologue()
        for hop in runs[0]:
            arrived(*hop)
        ready()
        o_acc[...] = jnp.zeros_like(o_acc)
        d_acc[...] = jnp.zeros_like(d_acc)

    @pl.when(step < n_ffn)
    def _():
        n_row = got.shape[0] * got.shape[1]
        half = wg_ref.shape[1] // 2
        xn = got[:, :, :width].reshape(n_row, width)
        dy = got[:, :, width:].reshape(n_row, width)
        cuts = [slice(0, half), slice(half, 2 * half)]
        mid = [expert_math(dot(xn, wg_ref[:, c], ((1,), (0,))), dot(xn, wu_ref[:, c], ((1,), (0,))), dot(dy, wd_ref[c, :], ((1,), (1,)))) for c in cuts]
        act, d_gate, d_up = (jnp.concatenate(parts, axis=1) for parts in zip(*mid))
        o_acc[...] += dot(act, wd_ref[...], ((1,), (0,)))
        d_acc[...] += dot(d_gate, wg_ref[...], ((1,), (1,))) + dot(d_up, wu_ref[...], ((1,), (1,)))

    @pl.when(step == n_ffn - 1)
    def _():
        result[:, :, :width] = o_acc[...].astype(BF16).reshape(*result.shape[:2], width)
        result[:, :, width:] = d_acc[...].astype(BF16).reshape(*result.shape[:2], width)

    for k in range(1, n_ffn):
        @pl.when(step == k - 1)
        def _():
            if k == 2:
                all_in("meta_y", n_y - 1)
                spread("meta_z", along_z, lambda: meta_out.at[pl.ds(at["z"] * n_y * n_ep, n_y * n_ep)])
            for hop in runs[k]:
                arrived(*hop)

    @pl.when(step == n_ffn)
    def _():
        for entry in runs[n_ffn]:
            if entry == "back":
                back_out[ep] = result[ep]
                exchange_results("back", result, back_out)
            elif entry == "final":
                finish_tokens()
            elif entry[:3] == "sum":
                sum_up(int(entry[3:]))
            else:
                arrived(*entry)
        meta_res[...] = meta_out[...]
        for name in copies.made:
            if name[0] == "pair":
                copies.wait_recv(name)
        for copy in copies.made.values():
            copy().wait_send()


def gather_rows(rows, send, meta, x, tok, gain, router, wg, wu, wd, n_y, n_z, n_ep, block):
    n_tok, wide = rows.shape
    n_dev = n_y * n_z * n_ep
    capacity = send.shape[1]
    width, ff = wg.shape
    n_ffn = ff // block
    tiles = n_tok // 8
    order, _ = plan({"x": n_ep // 2, "y": n_y, "z": n_z}, 8 * wide * 2, n_ffn)
    hops = [e for e in order if not isinstance(e, str)]
    n_sem = len(hops) + sum(1 for e in hops if e[1] == 2) + len(PIECES)
    n_sem += 5 * (n_ep - 1) + 2 * (n_y - 1) + 2 * (n_z - 1)
    vmem, hbm = pl.BlockSpec(memory_space=pltpu.VMEM), pl.BlockSpec(memory_space=pl.ANY)
    col = pl.BlockSpec((width, block), lambda j: (0, jnp.minimum(j, n_ffn - 1)))
    row = pl.BlockSpec((block, width), lambda j: (jnp.minimum(j, n_ffn - 1), 0))
    slots = pltpu.VMEM((n_ep, capacity, wide), BF16)
    long = width + width // n_ep + LANES
    out, meta_all, y, gh, sums = pl.pallas_call(
        functools.partial(gather_kernel, n_y, n_z, n_ep, order),
        grid=(n_ffn + 1,),
        in_specs=[vmem] * 7 + [col, col, row],
        out_specs=[hbm] + [vmem] * 4,
        out_shape=[
            jax.ShapeDtypeStruct((n_z, n_y, n_ep // 2, 2, 2, 8, wide), BF16),
            jax.ShapeDtypeStruct((n_dev, 1, LANES), F32),
            jax.ShapeDtypeStruct((n_tok, width), BF16),
            jax.ShapeDtypeStruct((n_tok, width), BF16),
            jax.ShapeDtypeStruct((n_ep, 1, long), F32)],
        scratch_shapes=[
            slots, slots, slots, pltpu.VMEM((n_dev, 1, LANES), F32),
            *(pltpu.VMEM((n, 1, long), F32) for n in (n_ep, n_ep, n_y, n_z, n_ep)),
            pltpu.VMEM((n_ep * capacity, width), F32), pltpu.VMEM((n_ep * capacity, width), F32),
            pltpu.SemaphoreType.DMA((n_sem,)), pltpu.SemaphoreType.DMA((n_sem,)), pltpu.SemaphoreType.DMA((3,))],
        compiler_params=pltpu.CompilerParams(collective_id=1, has_side_effects=True, dimension_semantics=("arbitrary",), vmem_limit_bytes=56 * 2**20),
        cost_estimate=pl.CostEstimate(flops=12 * n_ep * capacity * width * ff, bytes_accessed=6 * width * ff, transcendentals=0),
        name="gather_rows",
    )(rows.reshape(tiles, 8, wide), send, meta, x, tok, gain, router, wg, wu, wd)
    return out.reshape(n_dev * 16, wide), meta_all, y, gh, sums


def pack_kernel(n_quarter, info_ref, off_ref, near_ref, far_ref, pos_ref, gate_ref, wg_ref, wu_ref, wd_ref, xn_out, dp_out, slice_ref, xn_buf, dp_buf, acc_g, acc_u, acc_d, sem):
    g = pl.program_id(0)
    n_group = pl.num_programs(0)
    width = xn_buf.shape[1]
    tile = MOST_PER_GROUP + ALIGN
    off = off_ref[g]
    base = pl.multiple_of(lax.div(off, ALIGN) * ALIGN, ALIGN)
    hit = lax.broadcasted_iota(jnp.int32, (tile, GROUP), 0) + base == pos_ref[0]
    pick = hit.astype(F32).astype(BF16)
    gate = jnp.sum(jnp.where(hit, gate_ref[0], 0.0), axis=1, keepdims=True)
    head, rest = pl.ds(base, ALIGN), pl.ds(pl.multiple_of(base + ALIGN, ALIGN), tile - ALIGN)
    wide = min(2 * TILE, width)
    half = near_ref.shape[0]
    keep = lax.broadcasted_iota(jnp.int32, (ALIGN, wide), 0) + base < off
    for buf, low, scale in ((xn_buf, 0, None), (dp_buf, width, gate)):
        for c in range(0, width, wide):
            cut = slice(c, c + wide)
            columns = slice(low + c, low + c + wide)
            new = dot(pick[:, :half], near_ref[:, columns], ((1,), (0,))) + dot(pick[:, half:], far_ref[:, columns], ((1,), (0,)))
            new = (new if scale is None else new * scale).astype(BF16)
            buf[head, cut] = jnp.where(keep, buf[head, cut].astype(F32), new[:ALIGN].astype(F32)).astype(BF16)
            buf[rest, cut] = new[ALIGN:]

    @pl.when(g == n_group - 1)
    def _():
        usual = USUAL_ROWS // TILE
        zeros = jnp.zeros((TILE, width), BF16)
        tail = pl.ds(pl.multiple_of(base + tile, ALIGN), TILE)
        xn_buf[tail, :] = zeros
        dp_buf[tail, :] = zeros
        used = info_ref[0]

        def at(t):
            return pl.ds(pl.multiple_of(t * TILE, TILE), TILE)

        def clear(t, carry):
            xn_buf[at(t), :] = zeros
            dp_buf[at(t), :] = zeros
            return carry

        lax.fori_loop(used, usual, clear, 0)

        part = width // n_quarter
        low = pl.multiple_of(info_ref[2] * part, part)
        quarter = pl.ds(low, part)
        wg, wu, wd = wg_ref[...], wu_ref[...], wd_ref[...]
        for acc in (acc_g, acc_u, acc_d):
            acc[...] = jnp.zeros_like(acc)

        def hidden_rows(x, p):
            return expert_math(dot(x, wg, ((1,), (0,))), dot(x, wu, ((1,), (0,))), dot(p, wd, ((1,), (1,))))

        def copies(t):
            return [pltpu.make_async_copy(buf.at[at(t)], out.at[at(t)], sem.at[k]) for k, (buf, out) in enumerate(((xn_buf, xn_out), (dp_buf, dp_out)))]

        def begin(t, carry):
            for copy in copies(t):
                copy.start()
            return carry

        def end(t, carry):
            for copy in copies(t):
                copy.wait()
            return carry

        def add(t, carry):
            act, dg, du = hidden_rows(xn_buf[at(t), :], dp_buf[at(t), :])
            acc_g[...] += dot(xn_buf[at(t), quarter], dg, ((0,), (0,)))
            acc_u[...] += dot(xn_buf[at(t), quarter], du, ((0,), (0,)))
            acc_d[...] += dot(act, dp_buf[at(t), quarter], ((0,), (0,)))

            @pl.when(t == 1)
            def _():
                lax.fori_loop(0, jnp.maximum(used, usual), begin, 0)

            return carry

        lax.fori_loop(0, jnp.maximum(used, 2), add, 0)
        slice_ref[0] = acc_g[...].astype(BF16)
        slice_ref[1] = acc_u[...].astype(BF16)
        for k in range(0, part, TILE):
            slice_ref[2, k:k + TILE, :] = acc_d[:, k:k + TILE].astype(BF16)
        lax.fori_loop(0, jnp.maximum(used, usual), end, 0)


def pack_rows(info, near, far, offsets, pos, gates, wg, wu, wd, most, n_quarter):
    total, width = 2 * near.shape[0], near.shape[1] // 2
    n_group = total // GROUP
    half = pl.BlockSpec((GROUP // 2, 2 * width), lambda g, info, off: (g, 0))
    usual, part = USUAL_ROWS, width // n_quarter
    small = pl.BlockSpec((1, 1, GROUP), lambda g, info, off: (g, 0, 0))
    col = pl.BlockSpec((width, TILE), lambda g, info, off: (0, info[1]))
    row = pl.BlockSpec((TILE, width), lambda g, info, off: (info[1], 0))
    whole = pl.BlockSpec(memory_space=pl.ANY)
    buf = pltpu.VMEM((max(most, usual) + 2 * TILE + ALIGN, width), BF16)
    out = jax.ShapeDtypeStruct((max(most, usual), width), BF16)
    return pl.pallas_call(
        functools.partial(pack_kernel, n_quarter),
        grid_spec=pltpu.PrefetchScalarGridSpec(
            num_scalar_prefetch=2,
            grid=(n_group,),
            in_specs=[half, half, small, small, col, col, row],
            out_specs=[whole, whole, pl.BlockSpec((3, part, TILE), lambda g, info, off: (0, 0, 0))],
            scratch_shapes=[
                buf, buf, pltpu.VMEM((part, TILE), F32), pltpu.VMEM((part, TILE), F32), pltpu.VMEM((TILE, part), F32), pltpu.SemaphoreType.DMA((2,))],
        ),
        out_shape=[out, out, jax.ShapeDtypeStruct((3, part, TILE), BF16)],
        compiler_params=pltpu.CompilerParams(dimension_semantics=("arbitrary",), vmem_limit_bytes=63 * 2**20),
        cost_estimate=pl.CostEstimate(flops=4 * GROUP * total * width, bytes_accessed=4 * total * width, transcendentals=0),
        name="pack_rows",
    )(info, offsets, near, far, pos, gates, wg, wu, wd)


def grads_kernel(info_ref, xn_hbm, dp_hbm, wg_ref, wu_ref, wd_ref, gg_ref, gu_ref, gd_ref, xn, xt, dp, act_t, d_gate, d_up, acc_g, acc_u, acc_d, tile_x, tile_p, sem):
    rows, width = xn.shape
    tiles = [slice(r, r + TILE) for r in range(0, rows, TILE)]

    @pl.when(pl.program_id(0) == 0)
    def _():
        def copies(t):
            at = pl.ds(pl.multiple_of(t * TILE, TILE), TILE)
            return [pltpu.make_async_copy(src.at[at], dst.at[at], sem.at[k, t]) for k, (src, dst) in enumerate(((xn_hbm, xn), (dp_hbm, dp)))]

        def begin(t, carry):
            for copy in copies(t):
                copy.start()
            return carry

        def end(t, carry):
            for copy in copies(t):
                copy.wait()
            at = pl.ds(pl.multiple_of(t * TILE, TILE), TILE)
            xt[:, at] = xn[at, :].T
            return carry

        lax.fori_loop(0, len(tiles), begin, 0)
        for acc in (acc_g, acc_u, acc_d):
            acc[...] = jnp.zeros_like(acc)
        lax.fori_loop(0, len(tiles), end, 0)

    wg, wu, wd = wg_ref[...], wu_ref[...], wd_ref[...]

    def hidden_rows(x, p):
        return expert_math(dot(x, wg, ((1,), (0,))), dot(x, wu, ((1,), (0,))), dot(p, wd, ((1,), (1,))))

    @pl.when(info_ref[0] > rows // TILE)
    def _():
        for acc in (acc_g, acc_u, acc_d):
            acc[...] = jnp.zeros_like(acc)

        def more(t, carry):
            at = pl.ds(pl.multiple_of(t * TILE, TILE), TILE)
            copies = [pltpu.make_async_copy(xn_hbm.at[at], tile_x, sem.at[0, 0]), pltpu.make_async_copy(dp_hbm.at[at], tile_p, sem.at[1, 0])]
            for copy in copies:
                copy.start()
            for copy in copies:
                copy.wait()
            act, d_gate[:TILE, :], d_up[:TILE, :] = hidden_rows(tile_x[...], tile_p[...])
            act_t[:, :TILE] = act.T

            def part(c, carry):
                cut = pl.ds(pl.multiple_of(c * TILE, TILE), TILE)
                acc_g[cut, :] += dot(tile_x[:, cut], d_gate[:TILE, :], ((0,), (0,)))
                acc_u[cut, :] += dot(tile_x[:, cut], d_up[:TILE, :], ((0,), (0,)))
                acc_d[:, cut] += dot(act_t[:, :TILE], tile_p[:, cut], ((1,), (0,)))
                return carry

            lax.fori_loop(0, width // TILE, part, 0)
            return carry

        lax.fori_loop(rows // TILE, info_ref[0], more, 0)

    for t in tiles:
        act, d_gate[t, :], d_up[t, :] = hidden_rows(xn[t, :], dp[t, :])
        act_t[:, t] = act.T

    wide = min(2 * TILE, width)
    for c in range(0, width, wide):
        cut = slice(c, c + wide)
        gg_ref[cut, :] = (dot(xt[cut, :], d_gate[...], ((1,), (0,))) + acc_g[cut, :]).astype(BF16)
        gu_ref[cut, :] = (dot(xt[cut, :], d_up[...], ((1,), (0,))) + acc_u[cut, :]).astype(BF16)
    for c in range(0, width, wide):
        cut = slice(c, c + wide)
        gd_ref[:, cut] = (dot(act_t[...], dp[:, cut], ((1,), (0,))) + acc_d[:, cut]).astype(BF16)


def expert_grads(info, xn, dp, wg, wu, wd, n_block):
    width, ff = wg.shape
    rows = USUAL_ROWS
    hbm = pl.BlockSpec(memory_space=pl.ANY)
    col = pl.BlockSpec((width, TILE), lambda j, info: (0, j))
    row = pl.BlockSpec((TILE, width), lambda j, info: (j, 0))
    return pl.pallas_call(
        grads_kernel,
        grid_spec=pltpu.PrefetchScalarGridSpec(
            num_scalar_prefetch=1,
            grid=(n_block,),
            in_specs=[hbm, hbm, col, col, row],
            out_specs=[col, col, row],
            scratch_shapes=[
                pltpu.VMEM((rows, width), BF16), pltpu.VMEM((width, rows), BF16), pltpu.VMEM((rows, width), BF16),
                pltpu.VMEM((TILE, rows), BF16), pltpu.VMEM((rows, TILE), BF16), pltpu.VMEM((rows, TILE), BF16),
                pltpu.VMEM((width, TILE), F32), pltpu.VMEM((width, TILE), F32), pltpu.VMEM((TILE, width), F32),
                pltpu.VMEM((TILE, width), BF16), pltpu.VMEM((TILE, width), BF16), pltpu.SemaphoreType.DMA((2, rows // TILE))],
        ),
        out_shape=[jax.ShapeDtypeStruct((width, ff), BF16)] * 2 + [jax.ShapeDtypeStruct((ff, width), BF16)],
        compiler_params=pltpu.CompilerParams(dimension_semantics=("arbitrary",), vmem_limit_bytes=63 * 2**20),
        cost_estimate=pl.CostEstimate(flops=12 * rows * width * TILE * n_block, bytes_accessed=12 * width * TILE * n_block, transcendentals=0),
        name="expert_grads",
    )(info, xn, dp, wg, wu, wd)


def place_kernel(slices_ref, gg_in, gu_in, gd_in, gg_ref, gu_ref, gd_ref):
    part = slices_ref.shape[1]
    for q in range(slices_ref.shape[0] // 3):
        rows = slice(q * part, (q + 1) * part)
        gg_ref[rows, :] = slices_ref[3 * q]
        gu_ref[rows, :] = slices_ref[3 * q + 1]
        for k in range(0, part, TILE):
            gd_ref[:, q * part + k:q * part + k + TILE] = slices_ref[3 * q + 2, k:k + TILE, :]


def place_slices(slices, grads, first, n_quarter):
    width, ff = grads[0].shape
    part = width // n_quarter
    hbm = pl.BlockSpec(memory_space=pl.ANY)
    col = pl.BlockSpec((width, TILE), lambda i: (0, first + i))
    row = pl.BlockSpec((TILE, width), lambda i: (first + i, 0))
    return pl.pallas_call(
        place_kernel,
        grid=(slices.shape[0] // (3 * n_quarter),),
        in_specs=[pl.BlockSpec((3 * n_quarter, part, TILE), lambda i: (i, 0, 0)), hbm, hbm, hbm],
        out_specs=[col, col, row],
        out_shape=[jax.ShapeDtypeStruct(g.shape, g.dtype) for g in grads],
        input_output_aliases={1: 0, 2: 1, 3: 2},
        compiler_params=pltpu.CompilerParams(dimension_semantics=("arbitrary",)),
        cost_estimate=pl.CostEstimate(flops=0, bytes_accessed=4 * slices.size, transcendentals=0),
        name="place_slices",
    )(slices, *grads)


def solution(mesh):
    n_ep = mesh.shape["ep"]
    n_dp = mesh.shape["dp"]
    n_y = 4 if n_dp == 32 else 2
    n_z = n_dp // n_y
    n_dev = n_dp * n_ep
    all_axes = ("dp", "ep")

    def local_step(hidden, grad_out, expert_ids, norm_gain, w_router, w_gate, w_up, w_down):
        n_tok, width = hidden.shape
        n_exp = w_router.shape[1]
        capacity = 4 * n_tok // n_exp
        total_tok = n_tok * n_dev
        dest_rows, slot_owner, loads = route_tables(expert_ids, n_exp, capacity)
        choice_hot = (expert_ids[:, :, None] == jnp.arange(n_exp, dtype=jnp.int32)).astype(F32)

        x_f32 = hidden.astype(F32)
        inv_rms = lax.rsqrt(jnp.mean(x_f32 * x_f32, axis=-1, keepdims=True) + EPS)
        x_hat = x_f32 * inv_rms
        x_norm = (x_hat * norm_gain).astype(BF16)
        xn_f32 = x_norm.astype(F32)
        router_probs = jax.nn.softmax(jnp.dot(xn_f32, w_router, preferred_element_type=F32), axis=-1)
        gate_vals = jnp.sum(router_probs[:, None, :] * choice_hot, axis=-1)

        meta = jnp.concatenate([gate_vals.T.reshape(1, -1), expert_ids.T.astype(F32).reshape(1, -1)], axis=1)
        meta = jnp.pad(meta, ((0, 0), (0, LANES - meta.shape[1])))
        dy_f32 = grad_out.astype(F32)
        d_picked = (dy_f32[:, None, :] * gate_vals[:, :, None]).astype(BF16).reshape(n_tok * 2, width)
        send = jnp.concatenate([
            jnp.take(x_norm, slot_owner // 2, axis=0, mode="fill", fill_value=0),
            jnp.take(d_picked, slot_owner, axis=0, mode="fill", fill_value=0)], axis=1)
        wg, wu, wd = w_gate[0], w_up[0], w_down[0]
        tok = jnp.concatenate([router_probs, inv_rms, gate_vals, dest_rows.reshape(n_tok, 2).astype(F32), expert_ids.astype(F32)], axis=1)
        tok = jnp.pad(tok, ((0, 0), (0, LANES - tok.shape[1])))
        rows = jnp.concatenate([x_norm, grad_out], axis=1)
        half = n_tok // 2
        far = lax.all_gather(rows[half:], all_axes, axis=0, tiled=True)
        near, meta_all, out_hidden, grad_hidden, sums = gather_rows(
            rows, send.reshape(n_exp, capacity, 2 * width), meta[None], hidden, tok,
            norm_gain[None], w_router.T, wg, wu, wd, n_y, n_z, n_ep, 2 * TILE)
        meta_all = meta_all.reshape(n_dev, LANES)
        ids_all = meta_all[:, 2 * n_tok:4 * n_tok].astype(jnp.int32).reshape(n_dev, 2, n_tok)
        gates_all = meta_all[:, :2 * n_tok].reshape(n_dev, 2, n_tok)
        sums = sums[:, 0]
        share = width // n_exp
        grad_router = sums[:, :width].T
        grad_gain = sums[:, width:width + share].reshape(-1)
        prob_sum = sums[0, width + share:width + share + n_exp]
        all_loads = jnp.sum((ids_all[..., None] == jnp.arange(n_exp, dtype=jnp.int32)).astype(F32), axis=(0, 1, 2))
        load_frac = all_loads / (2 * total_tok)
        aux_loss = AUX_COEF * n_exp * jnp.sum(load_frac * prob_sum / total_tok)

        me = lax.axis_index("ep")
        mine = ids_all == me

        def by_group(a):
            return jnp.concatenate([a[:, :half].reshape(-1, GROUP // 2), a[:, half:].reshape(-1, GROUP // 2)], axis=1)

        member = by_group(jnp.any(mine, axis=1))
        gate_me = by_group(jnp.sum(jnp.where(mine, gates_all, 0.0), axis=1))[:, None]
        rank = jnp.cumsum(member.astype(jnp.int32), axis=1)
        counts = rank[:, -1]
        ends = jnp.cumsum(counts)
        offsets = jnp.concatenate([jnp.zeros((1,), jnp.int32), ends])
        pos = jnp.where(member, offsets[:-1, None] + rank - 1, -(2**24))[:, None]
        n_block = w_gate.shape[2] // TILE
        own = n_block - n_dp // QUARTERS
        place = lax.axis_index("dp")
        info = jnp.stack([(offsets[-1] + TILE - 1) // TILE, own + place // QUARTERS, place % QUARTERS]).astype(jnp.int32)
        xn, dp, slices = pack_rows(info, near, far, offsets, pos, gate_me, wg, wu, wd, capacity * n_dev, QUARTERS)
        slices_all = lax.all_gather(slices, "dp", axis=0, tiled=True)
        grads = expert_grads(info, xn, dp, wg, wu, wd, own)
        g_gate, g_up, g_down = (g[None] for g in place_slices(slices_all, grads, own, QUARTERS))
        return out_hidden, aux_loss, grad_hidden, grad_gain, grad_router, g_gate, g_up, g_down

    tok_spec = P(all_axes, None)
    w_spec = P("ep", None, None)
    return jax.shard_map(local_step, mesh=mesh, in_specs=(tok_spec, tok_spec, tok_spec, P(), P(), w_spec, w_spec, w_spec), out_specs=(tok_spec, P(), tok_spec, P(), P(), w_spec, w_spec, w_spec), check_vma=False)
```
